32 devices in a mesh: row: 4 (over z), col: 8 (over y, x, core).
Axes of the slice: x: 2, y: 2, z: 4, core: 2. Of those that a mesh axis runs over, the one named last changes fastest.
Arguments:
- tokens_in: bfloat16 [8192, 1408], P(('row', 'col')), may hold values from -300 to 300
- ln1_gain: bfloat16 [1408], replicated, may hold values from 0.099609375 to 1.8984375
- ln1_bias: bfloat16 [1408], replicated, may hold values from -3 to 3
- qkv_weight: bfloat16 [1408, 4224], P('row', 'col'), may hold values from -0.8 to 0.8
- qkv_bias: bfloat16 [4224], P('col'), may hold values from -3 to 3
- proj_weight: bfloat16 [1408, 1408], P('col', 'row'), may hold values from -0.15625 to 0.15625
- proj_bias: bfloat16 [1408], replicated, may hold values from -3 to 3
- ln2_gain: bfloat16 [1408], replicated, may hold values from 0.099609375 to 1.8984375
- ln2_bias: bfloat16 [1408], replicated, may hold values from -3 to 3
- fc1_weight: bfloat16 [1408, 6144], P('row', 'col'), may hold values from -0.15625 to 0.15625
- fc1_bias: bfloat16 [6144], P('col'), may hold values from -3 to 3
- fc2_weight: bfloat16 [1408, 6144], P('row', 'col'), may hold values from -0.078125 to 0.078125
- fc2_bias: bfloat16 [1408], replicated, may hold values from -3 to 3
Outputs:
- tokens_out: bfloat16 [8192, 1408], P(('row', 'col'))
The draws below stay inside these ranges and needn't reach their ends.
All inputs are finite; a program needn't handle non-finite values.
Results may differ from the reference program's by a relative error of at most 0.01.
Values may be sent and summed in bfloat16 or wider, within the bound.
A program may use at most 64 MiB of HBM per device.

```python
import jax
import jax.numpy as jnp
from jax import lax

D = 1408
HEADS = 16
FF = 6144
LEN = 2048
TOKENS = 8192
N_ROW = 4
N_COL = 8


def draw_tokens_in(key, part):
    key_base = jax.random.fold_in(key, 11)
    columns = 1.0 + 2.0 * jnp.arange(D, dtype=jnp.float32) / (D - 1)
    base = jax.random.normal(key_base, (TOKENS, D), jnp.float32)
    return (base * columns).astype(jnp.bfloat16)


def draw_qkv_weight(key, part):
    noise = jax.random.normal(jax.random.fold_in(key, 21), (D, 3 * D), jnp.float32) * D ** (-0.5)
    return jnp.clip(noise, -0.8, 0.8).astype(jnp.bfloat16)


def shard_levels(stream_key, dims, cuts, low, largest):
    level, own = 1.0, jax.random.fold_in(stream_key, 6)
    for position, shards_of in cuts:
        draws = jnp.exp(jax.random.uniform(jax.random.fold_in(own, position), (shards_of,), jnp.float32, low / len(cuts), largest / len(cuts)))
        level = level * jnp.repeat(draws, dims[position] // shards_of).reshape([-1 if axis == position else 1 for axis in range(len(dims))])
    return level


def normal_values(own_key, dims, spread, reach, pieces=(), held_as=jnp.bfloat16):
    level = shard_levels(own_key, dims, pieces, -0.22, 0.18) if pieces else 1.0
    drawn = jax.random.normal(own_key, dims, jnp.float32) * spread * level
    return jnp.minimum(jnp.maximum(drawn, -reach), reach).astype(held_as)


def setup_inputs(seed: int = 0) -> dict:
    streams_of = jax.random.split(jax.random.key(seed), 14)
    return {
        "tokens_in": draw_tokens_in(jax.random.fold_in(streams_of[13], 71), 0),
        "ln1_gain": jnp.clip(1.0 + 0.18 * jax.random.normal(streams_of[1], (D,), jnp.float32), 0.099609375, 1.8984375).astype(jnp.bfloat16),
        "ln1_bias": normal_values(streams_of[2], (D,), 0.5, 3.0),
        "qkv_weight": draw_qkv_weight(jax.random.fold_in(streams_of[13], 71), 0),
        "qkv_bias": normal_values(streams_of[4], (3 * D,), 0.5, 3.0, ((0, 8),)),
        "proj_weight": normal_values(streams_of[5], (D, D), D ** -0.5, 0.15625, ((0, 8), (1, 4))),
        "proj_bias": normal_values(streams_of[6], (D,), 0.5, 3.0),
        "ln2_gain": jnp.clip(1.0 + 0.18 * jax.random.normal(streams_of[7], (D,), jnp.float32), 0.099609375, 1.8984375).astype(jnp.bfloat16),
        "ln2_bias": normal_values(streams_of[8], (D,), 0.5, 3.0),
        "fc1_weight": normal_values(streams_of[9], (D, FF), D ** -0.5, 0.15625, ((0, 4), (1, 8))),
        "fc1_bias": normal_values(streams_of[10], (FF,), 0.5, 3.0, ((0, 8),)),
        "fc2_weight": normal_values(streams_of[11], (D, FF), FF ** -0.5, 0.078125, ((0, 4), (1, 8))),
        "fc2_bias": normal_values(streams_of[12], (D,), 0.5, 3.0),
    }


def layer_norm(values, gain, bias):
    mean = lax.optimization_barrier(jnp.mean(values, axis=-1, keepdims=True))
    centred = values - mean
    var = lax.optimization_barrier(jnp.mean(centred * centred, axis=-1, keepdims=True))
    return centred * lax.rsqrt(var + 1e-06) * gain.astype(jnp.float32) + bias.astype(jnp.float32)

def attend(qkv, heads):
    length = qkv.shape[0]
    head_size = qkv.shape[1] // (3 * heads)
    parts = qkv.reshape(length, heads, 3, head_size).astype(jnp.float32)
    query = parts[:, :, 0]
    keys = parts[:, :, 1]
    values = parts[:, :, 2]
    block = min(512, length)
    blocks = query.reshape(length // block, block, heads, head_size)
    scale = 1.0 / head_size ** 0.5

    def one_block(qblock):
        scores = jnp.einsum('qhe,khe->hqk', qblock, keys) * scale
        top = lax.optimization_barrier(jnp.max(scores, axis=-1, keepdims=True))
        expo = jnp.exp(scores - top)
        probs = (expo / lax.optimization_barrier(jnp.sum(expo, axis=-1, keepdims=True))).astype(jnp.bfloat16)
        mixed = jnp.einsum('hqk,khe->qhe', probs.astype(jnp.float32), values)
        return mixed.astype(jnp.bfloat16).reshape(block, heads * head_size)
    return lax.map(one_block, blocks).reshape(length, heads * head_size)

def grouped_sum(left, right, groups):
    width = left.shape[1] // groups
    lefts = left.reshape(left.shape[0], groups, width).transpose(1, 0, 2)
    rights = right.reshape(groups, width, right.shape[1])

    def add_group(total, pair):
        part = jnp.dot(pair[0], pair[1], preferred_element_type=jnp.float32).astype(jnp.bfloat16)
        part = lax.optimization_barrier(part)
        return (total + part.astype(jnp.float32), None)
    start = jnp.zeros((left.shape[0], right.shape[1]), jnp.float32)
    total, _ = lax.scan(add_group, start, (lefts, rights))
    return total

def reference(tokens_in, ln1_gain, ln1_bias, qkv_weight, qkv_bias, proj_weight, proj_bias, ln2_gain, ln2_bias, fc1_weight, fc1_bias, fc2_weight, fc2_bias):
    inputs = tokens_in.astype(jnp.float32)
    ln1 = layer_norm(inputs, ln1_gain, ln1_bias).astype(jnp.bfloat16)
    qkv = jnp.dot(ln1, qkv_weight, preferred_element_type=jnp.float32) + qkv_bias.astype(jnp.float32)
    qkv = qkv.astype(jnp.bfloat16)
    clips = qkv.reshape(N_ROW, LEN, 3 * D)
    attn = lax.map(lambda clip: attend(clip, HEADS), clips).reshape(TOKENS, D)
    resid = inputs + grouped_sum(attn, proj_weight, N_COL) + proj_bias.astype(jnp.float32)
    ln2 = layer_norm(resid, ln2_gain, ln2_bias).astype(jnp.bfloat16)
    hidden = jnp.dot(ln2, fc1_weight, preferred_element_type=jnp.float32) + fc1_bias.astype(jnp.float32)
    hidden = jax.nn.gelu(hidden, approximate=False).astype(jnp.bfloat16)
    result = resid + grouped_sum(hidden, fc2_weight.T, N_COL) + fc2_bias.astype(jnp.float32)
    return result.astype(jnp.bfloat16)
```

```python
import functools

import jax
import jax.numpy as jnp
from jax import lax
from jax.experimental import pallas as pl
from jax.experimental.pallas import tpu as pltpu
from jax.sharding import PartitionSpec as P

HEADS = 16
LANES = 128
MESH = pl.DeviceIdType.MESH


def greet(peers):
    barrier = pltpu.get_barrier_semaphore()
    for peer in peers:
        pl.semaphore_signal(barrier, inc=1, device_id={"col": peer}, device_id_type=MESH)
    pl.semaphore_wait(barrier, len(peers))


def neighbours():
    me = lax.axis_index("col")
    core, x, y = me % 2, (me // 2) % 2, me // 4
    place = lambda y, x, core: y * 4 + x * 2 + core
    return (
        me,
        place(y, x, 1 - core),
        place(y, 1 - x, core),
        place(1 - y, x, core),
        place(1 - y, 1 - x, core),
    )


def gather_kernel(x_ref, o_ref, send, recv, local_sem):
    rows = x_ref.shape[0]
    half = rows // 2
    me, mate, xn, yn, dn = neighbours()
    greet((mate, xn, yn))

    def part(block, h):
        return o_ref.at[pl.ds(pl.multiple_of(block * rows + h * half, half), half)]

    def copy(i, src, block, h, to):
        return pltpu.make_async_remote_copy(
            src_ref=src, dst_ref=part(block, h), send_sem=send.at[i], recv_sem=recv.at[i],
            device_id={"col": to}, device_id_type=MESH,
        )

    def own(h):
        return x_ref.at[pl.ds(h * half, half)]

    def arrived(i, block, h):
        copy(i, own(0), block, h, mate).wait_recv()

    started = []

    def go(c):
        c.start()
        started.append(c)

    go(copy(0, own(0), me, 0, xn))
    go(copy(1, own(1), me, 1, yn))
    go(copy(2, own(1), me, 1, xn))
    go(copy(3, own(0), me, 0, yn))
    go(copy(6, own(0), me, 0, mate))
    go(copy(7, own(1), me, 1, mate))
    here = pltpu.make_async_copy(
        x_ref, o_ref.at[pl.ds(pl.multiple_of(me * rows, rows), rows)], local_sem
    )
    here.start()
    arrived(0, xn, 0)
    go(copy(4, part(xn, 0), xn, 0, yn))
    go(copy(8, part(xn, 0), xn, 0, mate))
    arrived(1, yn, 1)
    go(copy(5, part(yn, 1), yn, 1, xn))
    go(copy(9, part(yn, 1), yn, 1, mate))
    arrived(2, xn, 1)
    go(copy(10, part(xn, 1), xn, 1, mate))
    arrived(3, yn, 0)
    go(copy(11, part(yn, 0), yn, 0, mate))
    arrived(4, dn, 0)
    go(copy(12, part(dn, 0), dn, 0, mate))
    arrived(5, dn, 1)
    go(copy(13, part(dn, 1), dn, 1, mate))
    across = lambda block: block + mate - me
    for i, block, h in (
        (6, me, 0), (7, me, 1), (8, xn, 0), (9, yn, 1),
        (10, xn, 1), (11, yn, 0), (12, dn, 0), (13, dn, 1),
    ):
        arrived(i, across(block), h)
    for c in started:
        c.wait_send()
    here.wait()


def gather_col(x, collective_id):
    n = lax.axis_size("col")
    rows, width = x.shape
    if n != 8 or rows % 32:
        return lax.all_gather(x, "col", axis=0, tiled=True)
    return pl.pallas_call(
        gather_kernel,
        out_shape=jax.ShapeDtypeStruct((n * rows, width), x.dtype),
        in_specs=[pl.BlockSpec(memory_space=pltpu.VMEM)],
        out_specs=pl.BlockSpec(memory_space=pltpu.VMEM),
        scratch_shapes=[
            pltpu.SemaphoreType.DMA((14,)),
            pltpu.SemaphoreType.DMA((14,)),
            pltpu.SemaphoreType.DMA,
        ],
        compiler_params=pltpu.CompilerParams(
            collective_id=collective_id, has_side_effects=True, vmem_limit_bytes=24 << 20
        ),
        cost_estimate=pl.CostEstimate(
            flops=10**10, bytes_accessed=2 * n * rows * width, transcendentals=0
        ),
        name="gather_col",
    )(x)


def scatter_kernel(x_ref, o_ref, mated, sums, relay, landed, send, recv):
    rows = o_ref.shape[0]
    half = rows // 2
    me, mate, xn, yn, dn = neighbours()
    greet((mate, xn, yn))
    shift = mate - me
    targets = (dn, xn, yn, me)

    def copy(i, src, dst, to):
        return pltpu.make_async_remote_copy(
            src_ref=src, dst_ref=dst, send_sem=send.at[i], recv_sem=recv.at[i],
            device_id={"col": to}, device_id_type=MESH,
        )

    def block(j):
        return pl.ds(pl.multiple_of(j * rows, rows), rows)

    started = []

    def go(c):
        c.start()
        started.append(c)

    for k, target in enumerate(targets):
        go(copy(k, x_ref.at[block(target + shift)], mated.at[k], mate))

    def mine(k, h):
        rows_h = pl.ds(pl.multiple_of(targets[k] * rows + h * half, half), half)
        return x_ref[rows_h, :].astype(jnp.float32) + mated[k, pl.ds(h * half, half), :].astype(
            jnp.float32
        )

    def put(k, h, value):
        sums[k, pl.ds(h * half, half), :] = value.astype(jnp.bfloat16)

    def of(ref, k, h):
        return ref.at[k, pl.ds(h * half, half)]

    started[0].wait_recv()
    put(0, 0, mine(0, 0))
    go(copy(4, of(sums, 0, 0), relay.at[0], xn))
    put(0, 1, mine(0, 1))
    go(copy(5, of(sums, 0, 1), relay.at[1], yn))
    started[1].wait_recv()
    put(1, 0, mine(1, 0))
    go(copy(6, of(sums, 1, 0), of(landed, 0, 0), xn))
    started[2].wait_recv()
    put(2, 1, mine(2, 1))
    go(copy(7, of(sums, 2, 1), of(landed, 1, 1), yn))
    started[4].wait_recv()
    put(2, 0, mine(2, 0) + relay[0].astype(jnp.float32))
    go(copy(8, of(sums, 2, 0), of(landed, 1, 0), yn))
    started[5].wait_recv()
    put(1, 1, mine(1, 1) + relay[1].astype(jnp.float32))
    go(copy(9, of(sums, 1, 1), of(landed, 0, 1), xn))
    started[3].wait_recv()
    for i in (6, 7, 8, 9):
        started[i].wait_recv()
    for h in (0, 1):
        lines = pl.ds(h * half, half)
        o_ref[lines, :] = (
            mine(3, h)
            + landed[0, lines, :].astype(jnp.float32)
            + landed[1, lines, :].astype(jnp.float32)
        )
    for c in started:
        c.wait_send()


def scatter_col(x, collective_id):
    n = lax.axis_size("col")
    rows, width = x.shape[0] // n, x.shape[1]
    if n != 8 or rows % 32:
        return lax.psum_scatter(x, "col", scatter_dimension=0, tiled=True).astype(jnp.float32)
    return pl.pallas_call(
        scatter_kernel,
        out_shape=jax.ShapeDtypeStruct((rows, width), jnp.float32),
        in_specs=[pl.BlockSpec(memory_space=pltpu.VMEM)],
        out_specs=pl.BlockSpec(memory_space=pltpu.VMEM),
        scratch_shapes=[
            pltpu.VMEM((4, rows, width), x.dtype),
            pltpu.VMEM((3, rows, width), x.dtype),
            pltpu.VMEM((2, rows // 2, width), x.dtype),
            pltpu.VMEM((2, rows, width), x.dtype),
            pltpu.SemaphoreType.DMA((10,)),
            pltpu.SemaphoreType.DMA((10,)),
        ],
        compiler_params=pltpu.CompilerParams(
            collective_id=collective_id, has_side_effects=True, vmem_limit_bytes=32 << 20
        ),
        cost_estimate=pl.CostEstimate(
            flops=10**10, bytes_accessed=2 * n * rows * width, transcendentals=0
        ),
        name="scatter_col",
    )(x)


def gather_row(weight, axis):
    n = lax.axis_size("row")
    me = lax.axis_index("row")
    depth = weight.shape[axis]
    shape = list(weight.shape)
    shape[axis] *= n
    whole = jnp.zeros(shape, weight.dtype)
    for step in range(n):
        block = weight
        if step:
            block = lax.ppermute(weight, "row", [((i + step) % n, i) for i in range(n)])
        whole = lax.dynamic_update_slice_in_dim(whole, block, ((me + step) % n) * depth, axis)
    return whole


def cube_gather_col(x):
    n = lax.axis_size("col")
    if n != 8:
        return lax.all_gather(x, "col", axis=0, tiled=True)
    me = lax.axis_index("col")
    x = x[None]
    for bit, after in ((2, 1), (4, 2), (1, 4)):
        other = lax.ppermute(x, "col", [(i, i ^ bit) for i in range(n)])
        low = (me // bit) % 2 == 0
        first, second = jnp.where(low, x, other), jnp.where(low, other, x)
        x = jnp.concatenate([first, second], axis=0) if bit != 1 else jnp.stack([first, second], 1)
    return x.reshape(-1, x.shape[-1])


def norm_local(values, gain, bias):
    mean = jnp.mean(values, axis=-1, keepdims=True)
    centred = values - mean
    var = jnp.mean(centred * centred, axis=-1, keepdims=True)
    return centred * lax.rsqrt(var + 1e-06) * gain.astype(jnp.float32) + bias.astype(jnp.float32)


def attend_kernel(heads, size, padded, q_ref, kv_ref, o_ref):
    outs = []
    for head in range(heads):
        base = head * 3 * padded
        query = q_ref[:, base : base + padded]
        keys = kv_ref[:, base + padded : base + 2 * padded]
        values = kv_ref[:, base + 2 * padded : base + 3 * padded]
        scores = lax.dot_general(
            query, keys, (((1,), (1,)), ((), ())), preferred_element_type=jnp.float32
        )
        top = jnp.max(scores, axis=-1, keepdims=True)
        expo = jnp.exp2(scores - top).astype(jnp.bfloat16)
        mixed = jnp.dot(expo, values, preferred_element_type=jnp.float32)
        outs.append(mixed[:, :size] / mixed[:, size : size + 1])
    o_ref[...] = jnp.concatenate(outs, axis=1).astype(o_ref.dtype)


def attend(qkv, heads, size, padded):
    length, width = qkv.shape
    block = min(256, length)
    return pl.pallas_call(
        functools.partial(attend_kernel, heads, size, padded),
        grid=(length // block,),
        in_specs=[
            pl.BlockSpec((block, width), lambda i: (i, 0)),
            pl.BlockSpec((length, width), lambda i: (0, 0)),
        ],
        out_specs=pl.BlockSpec((block, heads * size), lambda i: (i, 0)),
        out_shape=jax.ShapeDtypeStruct((length, heads * size), jnp.bfloat16),
        compiler_params=pltpu.CompilerParams(vmem_limit_bytes=40 << 20),
        cost_estimate=pl.CostEstimate(
            flops=4 * heads * length * length * padded * 8,
            bytes_accessed=4 * length * width,
            transcendentals=heads * length * length,
        ),
        name="attend",
    )(qkv, qkv)


def project_back(left, right):
    return lax.dot_general(
        left, right, (((1,), (1,)), ((), ())), preferred_element_type=jnp.float32
    )


def fast_plan(heads, own_rows, features, qkv_width, proj_rows, hidden):
    if lax.axis_size("col") != 8 or lax.axis_size("row") != 4:
        return None
    quarter = features // 4
    size = qkv_width // (3 * heads)
    whole = qkv_width // LANES * LANES
    rest = qkv_width - whole
    ok = (
        own_rows % 32 == 0 and features % LANES == 0 and quarter % 32 == 0
        and hidden % LANES == 0 and 0 < rest and proj_rows == heads * size
        and proj_rows % 16 == 0 and size < LANES and whole // size == 3 * heads - 1
    )
    if not ok:
        return None
    first = 2 * quarter // LANES * LANES
    last = -(-quarter // LANES) * LANES
    middle = features - first - last
    if middle <= 0 or features - last > 3 * quarter:
        return None
    return dict(
        heads=heads, size=size, rows=own_rows, features=features, quarter=quarter, whole=whole,
        rest=rest, proj_rows=proj_rows, slot=-(-proj_rows // LANES) * LANES, hidden=hidden,
        pieces=(first, middle, last),
    )


def layer_kernel(
    plan, tok, vec, wq, wp, w1, w2, o_ref,
    x1, x2, qmain, qrest, qwide, qrow, qkv, ctx, ctx_out, pfull, f1, f2, resid, hid, part,
    mated, sums, relay, landed,
    zsend, zrecv, gsend, grecv, psend, precv, asend, arecv, ssend, srecv,
):
    heads, size, rows = plan["heads"], plan["size"], plan["rows"]
    features, quarter = plan["features"], plan["quarter"]
    whole, rest, slot, prows = plan["whole"], plan["rest"], plan["slot"], plan["proj_rows"]
    hidden, pieces = plan["hidden"], plan["pieces"]
    half = rows // 2
    groups = 3 * heads
    f32, bf16 = jnp.float32, jnp.bfloat16

    row = lax.axis_index("row")
    me, mate, xn, yn, dn = neighbours()
    shift = mate - me
    pair = row // 2
    near = row + 1 - 2 * (row % 2)
    other = 2 - pair
    far = 3 - 3 * pair
    middle = jnp.logical_or(row == 1, row == 2)
    end = jnp.logical_or(row == 0, row == 3)
    lo = 2 * pair
    hi = 2 - lo

    def flipped(mask):
        bits = [(me % 2 + mask % 2) % 2, (me // 2 % 2 + mask // 2 % 2) % 2, (me // 4 + mask // 4) % 2]
        return bits[0] + 2 * bits[1] + 4 * bits[2]

    barrier = pltpu.get_barrier_semaphore()
    for step in range(1, 8):
        pl.semaphore_signal(
            barrier, inc=1, device_id={"col": flipped(step)}, device_id_type=MESH
        )
    for step in range(1, 4):
        pl.semaphore_signal(
            barrier, inc=1, device_id={"row": (row + step) % 4}, device_id_type=MESH
        )

    def remote(src, dst, ssem, rsem, **to):
        return pltpu.make_async_remote_copy(
            src_ref=src, dst_ref=dst, send_sem=ssem, recv_sem=rsem,
            device_id=to, device_id_type=MESH,
        )

    def lines(b, n=rows):
        return pl.ds(pl.multiple_of(b * n, n), n)

    def place(w, b):
        if w == 0:
            return qmain.at[lines(b, quarter)]
        if w == 1:
            return qrest.at[b]
        if w == 2:
            return pfull.at[b, lines(me, slot)].at[pl.ds(0, prows)]
        return (f1 if w == 3 else f2).at[lines(b, quarter)]

    def source(w):
        if w == 0:
            return wq.at[:, pl.ds(0, whole)]
        return (None, qrest.at[row], wp, w1, w2)[w]

    def own_copy(w, s):
        return remote(
            source(w), place(w, row), zsend.at[w * 4 + s], zrecv.at[w * 4 + row],
            row=near if s == 0 else other,
        )

    def forward_copy(w, s, b):
        return remote(
            place(w, b), place(w, b), zsend.at[w * 4 + s], zrecv.at[w * 4 + b], row=near
        )

    def z_wait(w, b):
        remote(
            place(w, b), place(w, b), zsend.at[w * 4], zrecv.at[w * 4 + b], row=near
        ).wait_recv()

    def z_forward(w, s, b):
        z_wait(w, b)
        forward_copy(w, s, b).start()

    for j in range(quarter // 32):
        qrest[row, :, j * rest : (j + 1) * rest] = wq[32 * j : 32 * (j + 1), whole:]
    pl.semaphore_wait(barrier, 10)
    for w in (0, 2):
        for s in (0, 1):
            own_copy(w, s).start()

    def norm(values, g, b):
        mean = jnp.mean(values, axis=-1, keepdims=True)
        centred = values - mean
        var = jnp.mean(centred * centred, axis=-1, keepdims=True)
        return centred * lax.rsqrt(var + 1e-06) * vec[g : g + 1, :] + vec[b : b + 1, :]

    chunk = 32

    def norm1(i, c):
        at = pl.ds(pl.multiple_of(i * chunk, chunk), chunk)
        to = pl.ds(pl.multiple_of(me * rows + i * chunk, chunk), chunk)
        x1[to, :] = norm(tok[at, :].astype(f32), 0, 1).astype(bf16)
        return c

    lax.fori_loop(0, rows // chunk, norm1, 0)
    for s in (0, 1):
        own_copy(1, s).start()

    class Gather:
        def __init__(self, x, gi):
            self.x, self.gi = x, gi

        def copy(self, i, block, h, to):
            at = self.x.at[pl.ds(pl.multiple_of(block * rows + h * half, half), half)]
            return remote(at, at, gsend.at[self.gi, i], grecv.at[self.gi, i], col=to)

        def arrived(self, i, block, h):
            self.copy(i, block, h, mate).wait_recv()

        def start(self):
            for i, h, to in ((0, 0, xn), (1, 1, yn), (2, 1, xn), (3, 0, yn), (6, 0, mate), (7, 1, mate)):
                self.copy(i, me, h, to).start()

        def event0(self):
            self.arrived(0, xn, 0)
            self.copy(4, xn, 0, yn).start()
            self.copy(8, xn, 0, mate).start()
            self.arrived(1, yn, 1)
            self.copy(5, yn, 1, xn).start()
            self.copy(9, yn, 1, mate).start()

        def event1(self):
            self.arrived(2, xn, 1)
            self.copy(10, xn, 1, mate).start()
            self.arrived(3, yn, 0)
            self.copy(11, yn, 0, mate).start()

        def event2(self):
            self.arrived(4, dn, 0)
            self.copy(12, dn, 0, mate).start()
            self.arrived(5, dn, 1)
            self.copy(13, dn, 1, mate).start()

        def mate0(self):
            self.arrived(6, mate, 0)
            self.arrived(7, mate, 1)

        def mate1(self):
            for i, block, h in ((8, xn, 0), (10, xn, 1), (9, yn, 1), (11, yn, 0)):
                self.arrived(i, block + shift, h)

        def mate2(self):
            for i, h in ((12, 0), (13, 1)):
                self.arrived(i, dn + shift, h)

        def finish(self):
            for i in range(14):
                self.copy(i, me, 0, mate).wait_send()

    first = Gather(x1, 0)
    first.start()
    for w in (3, 4):
        @pl.when(end)
        def _():
            own_copy(w, 0).start()

        own_copy(w, 1).start()

    qrow[...] = jnp.zeros_like(qrow)
    for g in range(groups):
        qrow[:, g * LANES : g * LANES + size] = vec[6:7, g * size : (g + 1) * size]
    lane = lax.broadcasted_iota(jnp.int32, (1, LANES), 1)
    for head in range(heads):
        at = slice((3 * head + 2) * LANES, (3 * head + 3) * LANES)
        qrow[:, at] = jnp.where(lane == size, 1.0, qrow[:, at])
    pfull[row, lines(me, slot), :] = jnp.concatenate(
        [wp[...], jnp.zeros((slot - prows, quarter), bf16)], axis=0
    )
    for b in range(4):
        for d in range(8):
            pfull[b, d * slot + prows : (d + 1) * slot, :] = jnp.zeros((slot - prows, quarter), bf16)
    f1[lines(row, quarter), :] = w1[...]
    f2[lines(row, quarter), :] = w2[...]
    qmain[lines(row, quarter), :] = wq[:, :whole]

    spare = jnp.zeros((quarter, LANES - size), bf16)
    few = jnp.zeros((32, LANES - size), bf16)

    def widen(b):
        base = b * quarter
        at = pl.ds(pl.multiple_of(base, 32), quarter)
        for g in range(groups - 1):
            qwide[at, g * LANES : (g + 1) * LANES] = jnp.concatenate(
                [qmain[at, g * size : (g + 1) * size], spare], axis=1
            )
        for j in range(quarter // 32):
            some = pl.ds(pl.multiple_of(base + 32 * j, 32), 32)
            qwide[some, (groups - 1) * LANES :] = jnp.concatenate(
                [qmain[some, (groups - 1) * size :], qrest[b, :, j * rest : (j + 1) * rest], few],
                axis=1,
            )

    def q_wait(b):
        z_wait(0, b)
        z_wait(1, b)

    widen(row)
    first.event0()

    @pl.when(middle)
    def _():
        q_wait(other)
        forward_copy(0, 2, other).start()
        forward_copy(1, 2, other).start()

    q_wait(near)
    widen(near)
    first.event1()

    @pl.when(middle)
    def _():
        q_wait(far)
        forward_copy(0, 3, far).start()
        forward_copy(1, 3, far).start()

    first.event2()
    first.mate0()
    z_wait(2, near)

    def pcopy(i, r, at, count, block, to):
        ref = pfull.at[pl.ds(at, count), lines(block, slot)].at[:, pl.ds(0, prows)]
        return remote(ref, ref, psend.at[r, i], precv.at[r, i], col=to)

    def p_start(r, at):
        pcopy(0, r, at, 2, me, xn).start()
        pcopy(1, r, at, 2, me, yn).start()
        pcopy(2, r, at, 2, me, mate).start()

    def p_forward(r, at):
        pcopy(0, r, at, 2, xn, xn).wait_recv()
        pcopy(3, r, at, 1, xn, yn).start()
        pcopy(5, r, at, 2, xn, mate).start()
        pcopy(1, r, at, 2, yn, yn).wait_recv()
        pcopy(4, r, at + 1, 1, yn, xn).start()
        pcopy(6, r, at, 2, yn, mate).start()

    def p_last(r, at):
        pcopy(3, r, at, 1, dn, yn).wait_recv()
        pcopy(7, r, at, 1, dn, mate).start()
        pcopy(4, r, at + 1, 1, dn, xn).wait_recv()
        pcopy(8, r, at + 1, 1, dn, mate).start()

    def p_mates(r, at):
        pcopy(2, r, at, 2, mate, mate).wait_recv()
        pcopy(5, r, at, 2, xn + shift, mate).wait_recv()
        pcopy(6, r, at, 2, yn + shift, mate).wait_recv()
        pcopy(7, r, at, 1, dn + shift, mate).wait_recv()
        pcopy(8, r, at + 1, 1, dn + shift, mate).wait_recv()

    def p_finish(r, at):
        for i in (0, 1, 2, 5, 6):
            pcopy(i, r, at, 2, me, mate).wait_send()
        for i in (3, 4, 7, 8):
            pcopy(i, r, at, 1, me, mate).wait_send()

    p_start(0, lo)

    @pl.when(middle)
    def _():
        z_forward(2, 2, other)
        z_forward(2, 3, far)
        own_copy(3, 0).start()

    @pl.when(end)
    def _():
        q_wait(other)
        q_wait(far)

    widen(other)
    widen(far)
    first.mate1()
    first.mate2()

    factor = 1.4426950408889634 / size**0.5

    def qkv_block(i, c):
        @pl.when(i == 5)
        def _():
            p_forward(0, lo)

        at = lines(flipped(i))
        product = jnp.dot(x1[at, :], qwide[...], preferred_element_type=f32) + qrow[...]
        for g in range(groups):
            cols = slice(g * LANES, (g + 1) * LANES)
            value = product[:, cols]
            qkv[at, cols] = (value * factor if g % 3 == 0 else value).astype(bf16)
        return c

    lax.fori_loop(0, 8, qkv_block, 0)

    @pl.when(end)
    def _():
        z_wait(2, other)
        z_wait(2, far)

    p_start(1, hi)

    def a_copy(m, to):
        return remote(
            ctx_out.at[m], ctx.at[:, lines(me, slot)], asend.at[m], arecv.at[m], col=to
        )

    def attend_block(i, c):
        @pl.when(i == 1)
        def _():
            p_last(0, lo)

        @pl.when(i == 4)
        def _():
            p_forward(1, hi)

        @pl.when(i == 7)
        def _():
            p_last(1, hi)

        mask = 7 - i
        block = flipped(mask)
        at = lines(block)
        outs = []
        for head in range(heads):
            base = head * 3 * LANES
            query = qkv[at, base : base + LANES]
            keys = qkv[:, base + LANES : base + 2 * LANES]
            values = qkv[:, base + 2 * LANES : base + 3 * LANES]
            scores = lax.dot_general(
                query, keys, (((1,), (1,)), ((), ())), preferred_element_type=f32
            )
            top = jnp.max(scores, axis=-1, keepdims=True)
            expo = jnp.exp2(scores - top).astype(bf16)
            mixed = jnp.dot(expo, values, preferred_element_type=f32)
            outs.append(mixed[:, :size] / mixed[:, size : size + 1])
        outs.append(jnp.zeros((rows, slot - heads * size), f32))
        ctx_out[mask] = jnp.concatenate(outs, axis=1).astype(bf16)

        @pl.when(i < 7)
        def _():
            a_copy(mask, block).start()

        return c

    lax.fori_loop(0, 8, attend_block, 0)

    @pl.when(middle)
    def _():
        z_forward(3, 2, other)
        z_forward(3, 3, far)
        own_copy(4, 0).start()

    ctx[:, lines(me, slot)] = ctx_out[0]
    p_mates(0, lo)
    p_mates(1, hi)
    for m in range(1, 8):
        remote(
            ctx_out.at[m], ctx.at[:, lines(flipped(m), slot)], asend.at[m], arecv.at[m], col=mate
        ).wait_recv()

    for b in range(4):
        resid[:, b * quarter : (b + 1) * quarter] = jnp.dot(
            ctx[...], pfull[b], preferred_element_type=f32
        )

    def norm2(i, c):
        at = pl.ds(pl.multiple_of(i * chunk, chunk), chunk)
        to = pl.ds(pl.multiple_of(me * rows + i * chunk, chunk), chunk)
        value = tok[at, :].astype(f32) + resid[at, :] + vec[4:5, :]
        resid[at, :] = value
        x2[to, :] = norm(value, 2, 3).astype(bf16)
        return c

    lax.fori_loop(0, rows // chunk, norm2, 0)
    second = Gather(x2, 1)
    second.start()
    z_wait(3, near)
    second.event0()

    @pl.when(end)
    def _():
        z_wait(3, other)
        z_wait(3, far)

    def fc1_block(i, c):
        @pl.when(i == 1)
        def _():
            second.mate0()

        @pl.when(i == 2)
        def _():
            second.event1()

        @pl.when(i == 3)
        def _():
            second.mate1()

        @pl.when(i == 6)
        def _():
            second.event2()

        @pl.when(jnp.logical_and(i == 6, middle))
        def _():
            z_forward(4, 2, other)
            z_forward(4, 3, far)

        @pl.when(i == 7)
        def _():
            second.mate2()

        at = lines(flipped(i))
        value = jnp.dot(x2[at, :], f1[...], preferred_element_type=f32) + vec[7:8, :hidden]
        hid[at, :] = (0.5 * value * (1.0 + lax.erf(value * 0.7071067811865476))).astype(bf16)
        return c

    lax.fori_loop(0, 8, fc1_block, 0)

    starts = (
        (features - pieces[0]) * pair,
        pieces[0] - (pieces[0] - pieces[2]) * pair,
        (features - pieces[2]) * (1 - pair),
    )
    targets = (dn, yn, xn, me)

    class Piece:
        def __init__(self, p):
            self.p, self.width = p, pieces[p]
            self.cols = pl.ds(pl.multiple_of(starts[p], LANES), pieces[p])

        def copy(self, i, src, dst, to):
            return remote(src, dst, ssend.at[self.p, i], srecv.at[self.p, i], col=to)

        def of(self, ref, k, h):
            return ref.at[k, pl.ds(h * half, half), self.cols]

        def to_mate(self, k):
            block = flipped(6 - 2 * k + 1)
            return self.copy(k, part.at[lines(block), self.cols], mated.at[k, :, self.cols], mate)

        def compute(self):
            weight = f2.at[self.cols]

            def body(t, c):
                k = t % 4
                block = flipped(6 - 2 * k + 1 - t // 4)
                at = lines(block)
                part[at, self.cols] = project_back(hid[at, :], weight[...]).astype(bf16)

                @pl.when(t < 4)
                def _():
                    self.to_mate(k).start()

                return c

            lax.fori_loop(0, 8, body, 0)

        def mine(self, k, h):
            at = pl.ds(pl.multiple_of(targets[k] * rows + h * half, half), half)
            return part[at, self.cols].astype(f32) + mated[
                k, h * half : (h + 1) * half, self.cols
            ].astype(f32)

        def put(self, k, h, value):
            sums[k, h * half : (h + 1) * half, self.cols] = value.astype(bf16)

        def relays(self, h):
            return relay.at[h, :, self.cols]

        def c(self, i):
            k, h, dst, to = {
                4: (0, 0, self.relays(0), xn),
                5: (0, 1, self.relays(1), yn),
                6: (2, 0, self.of(landed, 0, 0), xn),
                7: (1, 1, self.of(landed, 1, 1), yn),
                8: (1, 0, self.of(landed, 1, 0), yn),
                9: (2, 1, self.of(landed, 0, 1), xn),
            }[i]
            return self.copy(i, self.of(sums, k, h), dst, to)

        def open(self):
            self.to_mate(0).wait_recv()
            self.put(0, 0, self.mine(0, 0))
            self.c(4).start()
            self.put(0, 1, self.mine(0, 1))
            self.c(5).start()
            self.to_mate(1).wait_recv()
            self.put(1, 1, self.mine(1, 1))
            self.c(7).start()
            self.to_mate(2).wait_recv()
            self.put(2, 0, self.mine(2, 0))
            self.c(6).start()

        def pass_on(self):
            self.c(4).wait_recv()
            self.put(1, 0, self.mine(1, 0) + relay[0, :, self.cols].astype(f32))
            self.c(8).start()
            self.c(5).wait_recv()
            self.put(2, 1, self.mine(2, 1) + relay[1, :, self.cols].astype(f32))
            self.c(9).start()

        def close(self):
            self.to_mate(3).wait_recv()
            for i in (6, 7, 8, 9):
                self.c(i).wait_recv()
            for h in (0, 1):
                at = slice(h * half, (h + 1) * half)
                total = (
                    self.mine(3, h)
                    + landed[0, at, self.cols].astype(f32)
                    + landed[1, at, self.cols].astype(f32)
                )
                value = resid[at, self.cols] + total + vec[5:6, self.cols]
                o_ref[at, self.cols] = value.astype(o_ref.dtype)

        def finish(self):
            for k in range(4):
                self.to_mate(k).wait_send()
            for i in range(4, 10):
                self.c(i).wait_send()

    one, two, three = Piece(0), Piece(1), Piece(2)
    z_wait(4, near)
    one.compute()
    one.open()

    @pl.when(end)
    def _():
        z_wait(4, other)

    two.compute()
    one.pass_on()
    two.open()

    @pl.when(end)
    def _():
        z_wait(4, far)

    three.compute()
    two.pass_on()
    three.open()
    one.close()
    three.pass_on()
    two.close()
    three.close()

    for piece in (one, two, three):
        piece.finish()
    first.finish()
    second.finish()
    p_finish(0, lo)
    p_finish(1, hi)
    for m in range(1, 8):
        a_copy(m, mate).wait_send()
    for w in range(5):
        for s in (0, 1):
            own_copy(w, s).wait_send()

    @pl.when(middle)
    def _():
        for w in range(5):
            forward_copy(w, 2, other).wait_send()
            forward_copy(w, 3, far).wait_send()


def layer_call(plan, tok, vec, wq, wp, w1, w2):
    rows, features, quarter = plan["rows"], plan["features"], plan["quarter"]
    hidden, slot = plan["hidden"], plan["slot"]
    wide = 3 * plan["heads"] * LANES
    length = 8 * rows
    bf16, f32 = jnp.bfloat16, jnp.float32
    dma = pltpu.SemaphoreType.DMA
    return pl.pallas_call(
        functools.partial(layer_kernel, plan),
        out_shape=jax.ShapeDtypeStruct((rows, features), bf16),
        in_specs=[pl.BlockSpec(memory_space=pltpu.VMEM)] * 6,
        out_specs=pl.BlockSpec(memory_space=pltpu.VMEM),
        scratch_shapes=[
            pltpu.VMEM((length, features), bf16),
            pltpu.VMEM((length, features), bf16),
            pltpu.VMEM((features, plan["whole"]), bf16),
            pltpu.VMEM((4, 32, quarter // 32 * plan["rest"]), bf16),
            pltpu.VMEM((features, wide), bf16),
            pltpu.VMEM((1, wide), f32),
            pltpu.VMEM((length, wide), bf16),
            pltpu.VMEM((rows, 8 * slot), bf16),
            pltpu.VMEM((8, rows, slot), bf16),
            pltpu.VMEM((4, 8 * slot, quarter), bf16),
            pltpu.VMEM((features, hidden), bf16),
            pltpu.VMEM((features, hidden), bf16),
            pltpu.VMEM((rows, features), f32),
            pltpu.VMEM((length, hidden), bf16),
            pltpu.VMEM((length, features), bf16),
            pltpu.VMEM((4, rows, features), bf16),
            pltpu.VMEM((3, rows, features), bf16),
            pltpu.VMEM((2, rows // 2, features), bf16),
            pltpu.VMEM((2, rows, features), bf16),
            dma((20,)), dma((20,)),
            dma((2, 14)), dma((2, 14)),
            dma((2, 9)), dma((2, 9)),
            dma((8,)), dma((8,)),
            dma((3, 10)), dma((3, 10)),
        ],
        compiler_params=pltpu.CompilerParams(
            collective_id=3, has_side_effects=True, vmem_limit_bytes=60 * 1024 * 1024
        ),
        name="layer",
    )(tok, vec, wq, wp, w1, w2)


def local(
    tokens_in,
    ln1_gain,
    ln1_bias,
    qkv_weight,
    qkv_bias,
    proj_weight,
    proj_bias,
    ln2_gain,
    ln2_bias,
    fc1_weight,
    fc1_bias,
    fc2_weight,
    fc2_bias,
):
    local_heads = HEADS // lax.axis_size("col")
    own_rows, features = tokens_in.shape
    size = qkv_weight.shape[1] // (3 * local_heads)
    padded = -(-(size + 1) // LANES) * LANES
    plan = fast_plan(
        local_heads, own_rows, features, qkv_weight.shape[1], proj_weight.shape[0],
        fc1_weight.shape[1],
    )
    if plan is not None:
        wide = lambda v: jnp.pad(v.astype(jnp.float32), (0, features - v.shape[0]))
        vec = jnp.stack(
            [
                wide(v)
                for v in (
                    ln1_gain, ln1_bias, ln2_gain, ln2_bias, proj_bias, fc2_bias, qkv_bias, fc1_bias
                )
            ]
        )
        return layer_call(plan, tokens_in, vec, qkv_weight, proj_weight, fc1_weight, fc2_weight)
    inputs = tokens_in.astype(jnp.float32)
    qkv_full = gather_row(qkv_weight, 0)
    proj_full = gather_row(proj_weight, 1)
    fc1_full = gather_row(fc1_weight, 0)
    fc2_full = gather_row(fc2_weight, 0)
    fc1_shift = fc1_bias.astype(jnp.float32)

    spare = padded - size
    qkv_wide = jnp.pad(
        qkv_full.reshape(features, local_heads, 3, size), ((0, 0), (0, 0), (0, 0), (0, spare))
    ).reshape(features, local_heads * 3 * padded)
    shift = jnp.pad(
        qkv_bias.astype(jnp.float32).reshape(local_heads, 3, size), ((0, 0), (0, 0), (0, spare))
    )
    shift = shift.at[:, 2, size].set(1.0).reshape(-1)
    scale = jnp.ones((local_heads, 3, padded), jnp.float32)
    scale = scale.at[:, 0].set(1.4426950408889634 / size**0.5).reshape(-1)

    ln1 = norm_local(inputs, ln1_gain, ln1_bias).astype(jnp.bfloat16)
    product = jnp.dot(gather_col(ln1, 0), qkv_wide, preferred_element_type=jnp.float32)
    qkv = ((product + shift) * scale).astype(jnp.bfloat16)
    attn = attend(qkv, local_heads, size, padded)
    proj_whole = cube_gather_col(proj_full)
    own_heads = lax.all_to_all(attn, "col", split_axis=0, concat_axis=1, tiled=True)
    attn_sum = jnp.dot(own_heads, proj_whole, preferred_element_type=jnp.float32)
    resid = inputs + attn_sum + proj_bias.astype(jnp.float32)
    ln2 = norm_local(resid, ln2_gain, ln2_bias).astype(jnp.bfloat16)
    product = jnp.dot(gather_col(ln2, 1), fc1_full, preferred_element_type=jnp.float32) + fc1_shift
    hidden = jax.nn.gelu(product, approximate=False).astype(jnp.bfloat16)
    mlp_sum = scatter_col(project_back(hidden, fc2_full).astype(jnp.bfloat16), 2)
    result = resid + mlp_sum + fc2_bias.astype(jnp.float32)
    return result.astype(jnp.bfloat16)


def solution(mesh):
    in_specs = (
        P(("row", "col"), None),
        P(),
        P(),
        P("row", "col"),
        P("col"),
        P("col", "row"),
        P(),
        P(),
        P(),
        P("row", "col"),
        P("col"),
        P("row", "col"),
        P(),
    )
    out_specs = P(("row", "col"), None)
    return jax.shard_map(local, mesh=mesh, in_specs=in_specs, out_specs=out_specs, check_vma=False)
```

```python
import functools

import jax
import jax.numpy as jnp
from jax import lax
from jax.experimental import pallas as pl
from jax.experimental.pallas import tpu as pltpu
from jax.sharding import PartitionSpec as P

HEADS = 16
LANES = 128
MESH = pl.DeviceIdType.MESH


def greet(peers):
    barrier = pltpu.get_barrier_semaphore()
    for peer in peers:
        pl.semaphore_signal(barrier, inc=1, device_id={"col": peer}, device_id_type=MESH)
    pl.semaphore_wait(barrier, len(peers))


def neighbours():
    me = lax.axis_index("col")
    core, x, y = me % 2, (me // 2) % 2, me // 4
    place = lambda y, x, core: y * 4 + x * 2 + core
    return (
        me,
        place(y, x, 1 - core),
        place(y, 1 - x, core),
        place(1 - y, x, core),
        place(1 - y, 1 - x, core),
    )


def gather_kernel(x_ref, o_ref, send, recv, local_sem):
    rows = x_ref.shape[0]
    half = rows // 2
    me, mate, xn, yn, dn = neighbours()
    greet((mate, xn, yn))

    def part(block, h):
        return o_ref.at[pl.ds(pl.multiple_of(block * rows + h * half, half), half)]

    def copy(i, src, block, h, to):
        return pltpu.make_async_remote_copy(
            src_ref=src, dst_ref=part(block, h), send_sem=send.at[i], recv_sem=recv.at[i],
            device_id={"col": to}, device_id_type=MESH,
        )

    def own(h):
        return x_ref.at[pl.ds(h * half, half)]

    def arrived(i, block, h):
        copy(i, own(0), block, h, mate).wait_recv()

    started = []

    def go(c):
        c.start()
        started.append(c)

    go(copy(0, own(0), me, 0, xn))
    go(copy(1, own(1), me, 1, yn))
    go(copy(2, own(1), me, 1, xn))
    go(copy(3, own(0), me, 0, yn))
    go(copy(6, own(0), me, 0, mate))
    go(copy(7, own(1), me, 1, mate))
    here = pltpu.make_async_copy(
        x_ref, o_ref.at[pl.ds(pl.multiple_of(me * rows, rows), rows)], local_sem
    )
    here.start()
    arrived(0, xn, 0)
    go(copy(4, part(xn, 0), xn, 0, yn))
    go(copy(8, part(xn, 0), xn, 0, mate))
    arrived(1, yn, 1)
    go(copy(5, part(yn, 1), yn, 1, xn))
    go(copy(9, part(yn, 1), yn, 1, mate))
    arrived(2, xn, 1)
    go(copy(10, part(xn, 1), xn, 1, mate))
    arrived(3, yn, 0)
    go(copy(11, part(yn, 0), yn, 0, mate))
    arrived(4, dn, 0)
    go(copy(12, part(dn, 0), dn, 0, mate))
    arrived(5, dn, 1)
    go(copy(13, part(dn, 1), dn, 1, mate))
    across = lambda block: block + mate - me
    for i, block, h in (
        (6, me, 0), (7, me, 1), (8, xn, 0), (9, yn, 1),
        (10, xn, 1), (11, yn, 0), (12, dn, 0), (13, dn, 1),
    ):
        arrived(i, across(block), h)
    for c in started:
        c.wait_send()
    here.wait()


def gather_col(x, collective_id):
    n = lax.axis_size("col")
    rows, width = x.shape
    if n != 8 or rows % 32:
        return lax.all_gather(x, "col", axis=0, tiled=True)
    return pl.pallas_call(
        gather_kernel,
        out_shape=jax.ShapeDtypeStruct((n * rows, width), x.dtype),
        in_specs=[pl.BlockSpec(memory_space=pltpu.VMEM)],
        out_specs=pl.BlockSpec(memory_space=pltpu.VMEM),
        scratch_shapes=[
            pltpu.SemaphoreType.DMA((14,)),
            pltpu.SemaphoreType.DMA((14,)),
            pltpu.SemaphoreType.DMA,
        ],
        compiler_params=pltpu.CompilerParams(
            collective_id=collective_id, has_side_effects=True, vmem_limit_bytes=24 << 20
        ),
        cost_estimate=pl.CostEstimate(
            flops=10**10, bytes_accessed=2 * n * rows * width, transcendentals=0
        ),
        name="gather_col",
    )(x)


def scatter_kernel(x_ref, o_ref, mated, sums, relay, landed, send, recv):
    rows = o_ref.shape[0]
    half = rows // 2
    me, mate, xn, yn, dn = neighbours()
    greet((mate, xn, yn))
    shift = mate - me
    targets = (dn, xn, yn, me)

    def copy(i, src, dst, to):
        return pltpu.make_async_remote_copy(
            src_ref=src, dst_ref=dst, send_sem=send.at[i], recv_sem=recv.at[i],
            device_id={"col": to}, device_id_type=MESH,
        )

    def block(j):
        return pl.ds(pl.multiple_of(j * rows, rows), rows)

    started = []

    def go(c):
        c.start()
        started.append(c)

    for k, target in enumerate(targets):
        go(copy(k, x_ref.at[block(target + shift)], mated.at[k], mate))

    def mine(k, h):
        rows_h = pl.ds(pl.multiple_of(targets[k] * rows + h * half, half), half)
        return x_ref[rows_h, :].astype(jnp.float32) + mated[k, pl.ds(h * half, half), :].astype(
            jnp.float32
        )

    def put(k, h, value):
        sums[k, pl.ds(h * half, half), :] = value.astype(jnp.bfloat16)

    def of(ref, k, h):
        return ref.at[k, pl.ds(h * half, half)]

    started[0].wait_recv()
    put(0, 0, mine(0, 0))
    go(copy(4, of(sums, 0, 0), relay.at[0], xn))
    put(0, 1, mine(0, 1))
    go(copy(5, of(sums, 0, 1), relay.at[1], yn))
    started[1].wait_recv()
    put(1, 0, mine(1, 0))
    go(copy(6, of(sums, 1, 0), of(landed, 0, 0), xn))
    started[2].wait_recv()
    put(2, 1, mine(2, 1))
    go(copy(7, of(sums, 2, 1), of(landed, 1, 1), yn))
    started[4].wait_recv()
    put(2, 0, mine(2, 0) + relay[0].astype(jnp.float32))
    go(copy(8, of(sums, 2, 0), of(landed, 1, 0), yn))
    started[5].wait_recv()
    put(1, 1, mine(1, 1) + relay[1].astype(jnp.float32))
    go(copy(9, of(sums, 1, 1), of(landed, 0, 1), xn))
    started[3].wait_recv()
    for i in (6, 7, 8, 9):
        started[i].wait_recv()
    for h in (0, 1):
        lines = pl.ds(h * half, half)
        o_ref[lines, :] = (
            mine(3, h)
            + landed[0, lines, :].astype(jnp.float32)
            + landed[1, lines, :].astype(jnp.float32)
        )
    for c in started:
        c.wait_send()


def scatter_col(x, collective_id):
    n = lax.axis_size("col")
    rows, width = x.shape[0] // n, x.shape[1]
    if n != 8 or rows % 32:
        return lax.psum_scatter(x, "col", scatter_dimension=0, tiled=True).astype(jnp.float32)
    return pl.pallas_call(
        scatter_kernel,
        out_shape=jax.ShapeDtypeStruct((rows, width), jnp.float32),
        in_specs=[pl.BlockSpec(memory_space=pltpu.VMEM)],
        out_specs=pl.BlockSpec(memory_space=pltpu.VMEM),
        scratch_shapes=[
            pltpu.VMEM((4, rows, width), x.dtype),
            pltpu.VMEM((3, rows, width), x.dtype),
            pltpu.VMEM((2, rows // 2, width), x.dtype),
            pltpu.VMEM((2, rows, width), x.dtype),
            pltpu.SemaphoreType.DMA((10,)),
            pltpu.SemaphoreType.DMA((10,)),
        ],
        compiler_params=pltpu.CompilerParams(
            collective_id=collective_id, has_side_effects=True, vmem_limit_bytes=32 << 20
        ),
        cost_estimate=pl.CostEstimate(
            flops=10**10, bytes_accessed=2 * n * rows * width, transcendentals=0
        ),
        name="scatter_col",
    )(x)


def gather_row(weight, axis):
    n = lax.axis_size("row")
    me = lax.axis_index("row")
    depth = weight.shape[axis]
    shape = list(weight.shape)
    shape[axis] *= n
    whole = jnp.zeros(shape, weight.dtype)
    for step in range(n):
        block = weight
        if step:
            block = lax.ppermute(weight, "row", [((i + step) % n, i) for i in range(n)])
        whole = lax.dynamic_update_slice_in_dim(whole, block, ((me + step) % n) * depth, axis)
    return whole


def cube_gather_col(x):
    n = lax.axis_size("col")
    if n != 8:
        return lax.all_gather(x, "col", axis=0, tiled=True)
    me = lax.axis_index("col")
    x = x[None]
    for bit, after in ((2, 1), (4, 2), (1, 4)):
        other = lax.ppermute(x, "col", [(i, i ^ bit) for i in range(n)])
        low = (me // bit) % 2 == 0
        first, second = jnp.where(low, x, other), jnp.where(low, other, x)
        x = jnp.concatenate([first, second], axis=0) if bit != 1 else jnp.stack([first, second], 1)
    return x.reshape(-1, x.shape[-1])


def norm_local(values, gain, bias):
    mean = jnp.mean(values, axis=-1, keepdims=True)
    centred = values - mean
    var = jnp.mean(centred * centred, axis=-1, keepdims=True)
    return centred * lax.rsqrt(var + 1e-06) * gain.astype(jnp.float32) + bias.astype(jnp.float32)


def attend_kernel(heads, size, padded, q_ref, kv_ref, o_ref):
    outs = []
    for head in range(heads):
        base = head * 3 * padded
        query = q_ref[:, base : base + padded]
        keys = kv_ref[:, base + padded : base + 2 * padded]
        values = kv_ref[:, base + 2 * padded : base + 3 * padded]
        scores = lax.dot_general(
            query, keys, (((1,), (1,)), ((), ())), preferred_element_type=jnp.float32
        )
        top = jnp.max(scores, axis=-1, keepdims=True)
        expo = jnp.exp2(scores - top).astype(jnp.bfloat16)
        mixed = jnp.dot(expo, values, preferred_element_type=jnp.float32)
        outs.append(mixed[:, :size] / mixed[:, size : size + 1])
    o_ref[...] = jnp.concatenate(outs, axis=1).astype(o_ref.dtype)


def attend(qkv, heads, size, padded):
    length, width = qkv.shape
    block = min(256, length)
    return pl.pallas_call(
        functools.partial(attend_kernel, heads, size, padded),
        grid=(length // block,),
        in_specs=[
            pl.BlockSpec((block, width), lambda i: (i, 0)),
            pl.BlockSpec((length, width), lambda i: (0, 0)),
        ],
        out_specs=pl.BlockSpec((block, heads * size), lambda i: (i, 0)),
        out_shape=jax.ShapeDtypeStruct((length, heads * size), jnp.bfloat16),
        compiler_params=pltpu.CompilerParams(vmem_limit_bytes=40 << 20),
        cost_estimate=pl.CostEstimate(
            flops=4 * heads * length * length * padded * 8,
            bytes_accessed=4 * length * width,
            transcendentals=heads * length * length,
        ),
        name="attend",
    )(qkv, qkv)


def project_back(left, right):
    return lax.dot_general(
        left, right, (((1,), (1,)), ((), ())), preferred_element_type=jnp.float32
    )


def fast_plan(heads, own_rows, features, qkv_width, proj_rows, hidden):
    if lax.axis_size("col") != 8 or lax.axis_size("row") != 4:
        return None
    quarter = features // 4
    size = qkv_width // (3 * heads)
    whole = qkv_width // LANES * LANES
    rest = qkv_width - whole
    ok = (
        hidden == 3 * heads * LANES and own_rows % 32 == 0 and features % LANES == 0 and quarter % 32 == 0
        and hidden % LANES == 0 and 0 < rest and proj_rows == heads * size
        and proj_rows % 16 == 0 and 0 < proj_rows - LANES <= LANES // 2
        and 8 * proj_rows == features and size < LANES and whole // size == 3 * heads - 1
    )
    if not ok:
        return None
    first = 2 * quarter // LANES * LANES
    last = -(-quarter // LANES) * LANES
    middle = features - first - last
    if middle <= 0 or last <= LANES or features - last > 3 * quarter:
        return None
    return dict(
        heads=heads, size=size, rows=own_rows, features=features, quarter=quarter, whole=whole,
        rest=rest, proj_rows=proj_rows, hidden=hidden,
        pieces=(first, middle, last - LANES, LANES),
    )


def layer_kernel(
    plan, tok_in, g1, c1, qb, pb, g2, c2, d1, d2, wq_in, wp, w1, w2, o_ref,
    tok, wq, v1, v2, v3, v4, v5, v6, v7, v8,
    vec, x1, x2, qmain, qrest, qwide, qrow, qkv, ctx, heads_out, tails_out, heads_in, tails_in, pfull, f1, f2, resid,
    mated, sums, relay, landed,
    lsem, zsend, zrecv, gsend, grecv, psend, precv, asend, arecv, ssend, srecv,
):
    heads, size, rows = plan["heads"], plan["size"], plan["rows"]
    features, quarter = plan["features"], plan["quarter"]
    whole, rest, prows = plan["whole"], plan["rest"], plan["proj_rows"]
    hidden, pieces = plan["hidden"], plan["pieces"]
    half = rows // 2
    groups = 3 * heads
    f32, bf16 = jnp.float32, jnp.bfloat16
    hid, part = qkv, x1

    row = lax.axis_index("row")
    me, mate, xn, yn, dn = neighbours()
    shift = mate - me
    pair = row // 2
    near = row + 1 - 2 * (row % 2)
    other = 2 - pair
    far = 3 - 3 * pair
    middle = jnp.logical_or(row == 1, row == 2)
    end = jnp.logical_or(row == 0, row == 3)
    lo = 2 * pair
    hi = 2 - lo

    def flipped(mask):
        bits = [(me % 2 + mask % 2) % 2, (me // 2 % 2 + mask // 2 % 2) % 2, (me // 4 + mask // 4) % 2]
        return bits[0] + 2 * bits[1] + 4 * bits[2]

    barrier = pltpu.get_barrier_semaphore()
    for step in range(1, 8):
        pl.semaphore_signal(
            barrier, inc=1, device_id={"col": flipped(step)}, device_id_type=MESH
        )
    for step in range(1, 4):
        pl.semaphore_signal(
            barrier, inc=1, device_id={"row": (row + step) % 4}, device_id_type=MESH
        )

    def load(i, src, dst):
        return pltpu.make_async_copy(src, dst, lsem.at[i])

    def remote(src, dst, ssem, rsem, **to):
        return pltpu.make_async_remote_copy(
            src_ref=src, dst_ref=dst, send_sem=ssem, recv_sem=rsem,
            device_id=to, device_id_type=MESH,
        )

    def lines(b, n=rows):
        return pl.ds(pl.multiple_of(b * n, n), n)

    def cut(w, b):
        low = b // 2
        return (1 - low) * LANES if w == 5 else low * (quarter - LANES)

    def length_of(w):
        return quarter - LANES if w == 5 else LANES

    def place(w, b):
        if w == 0:
            return qmain.at[lines(b, quarter)]
        if w == 1:
            return qrest.at[b]
        if w == 2:
            return pfull.at[b, lines(me, prows)]
        if w == 3:
            return f1.at[lines(b, quarter)]
        if w == 4:
            return f2.at[lines(b, quarter)]
        return f2.at[pl.ds(pl.multiple_of(b * quarter + cut(w, b), 32), length_of(w))]

    def source(w):
        if w == 0:
            return place(0, row)
        return (None, qrest.at[row], wp, w1, w2)[w]

    def z_copy(w, s, b):
        return remote(
            place(w, b), place(w, b), zsend.at[w * 5 + s], zrecv.at[w * 4 + b],
            row=other if s in (1, 4) else near,
        )

    def own_copy(w, s):
        return remote(
            source(w), place(w, row), zsend.at[w * 5 + s], zrecv.at[w * 4 + row],
            row=other if s == 1 else near,
        )

    def z_wait(w, b):
        z_copy(w, 0, b).wait_recv()

    def z_forward(w, s):
        b = {2: other, 3: far, 4: near}[s]
        z_wait(w, b)
        z_copy(w, s, b).start()

    loads = [load(0, wq_in, wq), load(1, tok_in, tok)]
    for i, (src, dst) in enumerate(
        ((g1, v1), (c1, v2), (g2, v3), (c2, v4), (pb, v5), (d2, v6), (qb, v7), (d1, v8))
    ):
        loads.append(load(i + 2, src, dst))
    loads.append(load(10, wp, place(2, row)))
    loads.append(load(11, w1, place(3, row)))
    loads.append(load(12, w2, place(4, row)))
    for c in loads:
        c.start()
    loads[0].wait()
    turned = wq[...].astype(f32).T.astype(bf16)
    qmain[lines(row, quarter), :] = turned[:, :whole]
    for j in range(quarter // 32):
        qrest[row, :, j * rest : (j + 1) * rest] = turned[32 * j : 32 * (j + 1), whole:]
    for i, v in enumerate((v1, v2, v3, v4, v5, v6, v7, v8)):
        loads[i + 2].wait()
        vec[i : i + 1, : v.shape[0]] = v[...].astype(f32).reshape(1, -1)
    loads[1].wait()
    pl.semaphore_wait(barrier, 10)
    for w in (0, 1, 2):
        own_copy(w, 0).start()

    @pl.when(middle)
    def _():
        for w in (0, 1, 2):
            own_copy(w, 1).start()

    @pl.when(end)
    def _():
        for w in (3, 4):
            own_copy(w, 0).start()

    def norm(values, g, b):
        mean = jnp.mean(values, axis=-1, keepdims=True)
        centred = values - mean
        var = jnp.mean(centred * centred, axis=-1, keepdims=True)
        return centred * lax.rsqrt(var + 1e-06) * vec[g : g + 1, :] + vec[b : b + 1, :]

    chunk = 32

    def norm1(i, c):
        at = pl.ds(pl.multiple_of(i * chunk, chunk), chunk)
        to = pl.ds(pl.multiple_of(me * rows + i * chunk, chunk), chunk)
        x1[to, :] = norm(tok[at, :].astype(f32), 0, 1).astype(bf16)
        return c

    lax.fori_loop(0, rows // chunk, norm1, 0)

    class Gather:
        def __init__(self, x, gi):
            self.x, self.gi = x, gi

        def copy(self, i, block, h, to):
            at = self.x.at[pl.ds(pl.multiple_of(block * rows + h * half, half), half)]
            return remote(at, at, gsend.at[self.gi, i], grecv.at[self.gi, i], col=to)

        def arrived(self, i, block, h):
            self.copy(i, block, h, mate).wait_recv()

        def start(self):
            for i, h, to in ((0, 0, xn), (1, 1, yn), (2, 1, xn), (3, 0, yn), (6, 0, mate), (7, 1, mate)):
                self.copy(i, me, h, to).start()

        def event0(self):
            self.arrived(0, xn, 0)
            self.copy(4, xn, 0, yn).start()
            self.copy(8, xn, 0, mate).start()
            self.arrived(1, yn, 1)
            self.copy(5, yn, 1, xn).start()
            self.copy(9, yn, 1, mate).start()

        def event1(self):
            self.arrived(2, xn, 1)
            self.copy(10, xn, 1, mate).start()
            self.arrived(3, yn, 0)
            self.copy(11, yn, 0, mate).start()

        def event2(self):
            self.arrived(4, dn, 0)
            self.copy(12, dn, 0, mate).start()
            self.arrived(5, dn, 1)
            self.copy(13, dn, 1, mate).start()

        def mate0(self):
            self.arrived(6, mate, 0)
            self.arrived(7, mate, 1)

        def mate1(self):
            for i, block, h in ((8, xn, 0), (10, xn, 1), (9, yn, 1), (11, yn, 0)):
                self.arrived(i, block + shift, h)

        def mate2(self):
            for i, h in ((12, 0), (13, 1)):
                self.arrived(i, dn + shift, h)

        def finish(self):
            for i in range(14):
                self.copy(i, me, 0, mate).wait_send()

    first = Gather(x1, 0)
    first.start()
    qrow[...] = jnp.zeros_like(qrow)
    for g in range(groups):
        qrow[:, g * LANES : g * LANES + size] = vec[6:7, g * size : (g + 1) * size]
    lane = lax.broadcasted_iota(jnp.int32, (1, LANES), 1)
    for head in range(heads):
        at = slice((3 * head + 2) * LANES, (3 * head + 3) * LANES)
        qrow[:, at] = jnp.where(lane == size, 1.0, qrow[:, at])
    for c in loads[10:]:
        c.wait()

    spare = jnp.zeros((quarter, LANES - size), bf16)
    few = jnp.zeros((32, LANES - size), bf16)

    def widen(b):
        base = b * quarter
        at = pl.ds(pl.multiple_of(base, 32), quarter)
        for g in range(groups - 1):
            qwide[at, g * LANES : (g + 1) * LANES] = jnp.concatenate(
                [qmain[at, g * size : (g + 1) * size], spare], axis=1
            )
        for j in range(quarter // 32):
            some = pl.ds(pl.multiple_of(base + 32 * j, 32), 32)
            qwide[some, (groups - 1) * LANES :] = jnp.concatenate(
                [qmain[some, (groups - 1) * size :], qrest[b, :, j * rest : (j + 1) * rest], few],
                axis=1,
            )

    widen(row)

    def q_wait(b):
        z_wait(0, b)
        z_wait(1, b)

    @pl.when(middle)
    def _():
        for w in (0, 1):
            z_forward(w, 4)
        for w in (0, 1):
            z_forward(w, 2)

    first.event0()

    @pl.when(end)
    def _():
        q_wait(near)

    widen(near)

    @pl.when(middle)
    def _():
        z_forward(2, 4)
        own_copy(3, 1).start()
        for w in (0, 1):
            z_forward(w, 3)

    first.event1()

    def pcopy(i, r, at, count, block, to):
        ref = pfull.at[pl.ds(at, count), lines(block, prows)]
        return remote(ref, ref, psend.at[r, i], precv.at[r, i], col=to)

    def p_start(r, at):
        pcopy(0, r, at, 2, me, xn).start()
        pcopy(1, r, at, 2, me, yn).start()
        pcopy(2, r, at, 2, me, mate).start()

    def p_forward(r, at):
        pcopy(0, r, at, 2, xn, xn).wait_recv()
        pcopy(3, r, at, 1, xn, yn).start()
        pcopy(5, r, at, 2, xn, mate).start()
        pcopy(1, r, at, 2, yn, yn).wait_recv()
        pcopy(4, r, at + 1, 1, yn, xn).start()
        pcopy(6, r, at, 2, yn, mate).start()

    def p_last(r, at):
        pcopy(3, r, at, 1, dn, yn).wait_recv()
        pcopy(7, r, at, 1, dn, mate).start()
        pcopy(4, r, at + 1, 1, dn, xn).wait_recv()
        pcopy(8, r, at + 1, 1, dn, mate).start()

    def p_mates(r, at):
        pcopy(2, r, at, 2, mate, mate).wait_recv()
        pcopy(5, r, at, 2, xn + shift, mate).wait_recv()
        pcopy(6, r, at, 2, yn + shift, mate).wait_recv()
        pcopy(7, r, at, 1, dn + shift, mate).wait_recv()
        pcopy(8, r, at + 1, 1, dn + shift, mate).wait_recv()

    def p_finish(r, at):
        for i in (0, 1, 2, 5, 6):
            pcopy(i, r, at, 2, me, mate).wait_send()
        for i in (3, 4, 7, 8):
            pcopy(i, r, at, 1, me, mate).wait_send()


    @pl.when(end)
    def _():
        z_wait(2, near)

    p_start(0, lo)

    @pl.when(middle)
    def _():
        z_forward(2, 2)
        z_forward(2, 3)
        own_copy(3, 0).start()
        z_forward(3, 4)
        own_copy(4, 1).start()

    first.event2()
    first.mate0()

    @pl.when(end)
    def _():
        q_wait(other)
        q_wait(far)

    widen(other)
    widen(far)
    first.mate1()
    first.mate2()

    factor = 1.4426950408889634 / size**0.5

    def qkv_block(i, c):
        @pl.when(i == 6)
        def _():
            p_forward(0, lo)

        @pl.when(jnp.logical_and(i == 7, end))
        def _():
            z_wait(2, other)
            z_wait(2, far)

        @pl.when(i == 7)
        def _():
            p_start(1, hi)

        at = lines(flipped(i))
        product = jnp.dot(x1[at, :], qwide[...], preferred_element_type=f32) + qrow[...]
        for g in range(groups):
            cols = slice(g * LANES, (g + 1) * LANES)
            value = product[:, cols]
            qkv[at, cols] = (value * factor if g % 3 == 0 else value).astype(bf16)
        return c

    lax.fori_loop(0, 8, qkv_block, 0)

    rest_lanes = prows - LANES

    def a_copies(i, core, m, to):
        at = lines(core)
        tail = pl.ds(pl.multiple_of(core * half, half), half)
        return (
            remote(
                heads_out.at[i, at], heads_in.at[me], asend.at[0, m], arecv.at[0, m], col=to
            ),
            remote(
                tails_out.at[i, tail], tails_in.at[me], asend.at[1, m], arecv.at[1, m], col=to
            ),
        )

    def attend_block(i, c):
        @pl.when(i == 1)
        def _():
            p_last(0, lo)

        @pl.when(jnp.logical_and(i == 1, middle))
        def _():
            z_forward(3, 2)
            z_wait(4, near)
            for w in (5, 6):
                z_copy(w, 4, near).start()

        @pl.when(i == 3)
        def _():
            p_forward(1, hi)

        chip = flipped(6 - 2 * i) // 2
        at = lines(chip, 2 * rows)
        scores = []
        for head in range(heads):
            base = head * 3 * LANES
            scores.append(
                lax.dot_general(
                    qkv[at, base : base + LANES], qkv[:, base + LANES : base + 2 * LANES],
                    (((1,), (1,)), ((), ())), preferred_element_type=f32,
                )
            )
        expos = [
            jnp.exp2(x - jnp.max(x, axis=-1, keepdims=True)).astype(bf16) for x in scores
        ]
        outs = []
        for head in range(heads):
            base = (head * 3 + 2) * LANES
            mixed = jnp.dot(
                expos[head], qkv[:, base : base + LANES], preferred_element_type=f32
            )
            outs.append(mixed[:, :size] / mixed[:, size : size + 1])
        mixed = jnp.concatenate(outs, axis=1).astype(bf16)
        gap = jnp.zeros((half, LANES // 2 - rest_lanes), bf16)
        heads_out[i] = mixed[:, :LANES]
        for core in (0, 1):
            top, low = (
                mixed[core * rows + h * half : core * rows + (h + 1) * half, LANES:]
                for h in (0, 1)
            )
            tails_out[i, core * half : (core + 1) * half, :] = jnp.concatenate(
                [top, gap, low, gap], axis=1
            )
        for core in (0, 1):
            to = 2 * chip + core

            @pl.when(to != me)
            def _():
                for c in a_copies(i, core, 6 - 2 * i + (core + me) % 2, to):
                    c.start()

        return c

    lax.fori_loop(0, 4, attend_block, 0)
    @pl.when(middle)
    def _():
        z_forward(3, 3)
        own_copy(4, 0).start()

    p_last(1, hi)
    first.finish()
    heads_in[me] = heads_out[3, lines(me % 2), :]
    tails_in[me] = tails_out[3, lines(me % 2, half), :]
    p_mates(0, lo)
    p_mates(1, hi)
    for m in range(1, 8):
        for ref, out, n, which in (
            (heads_in, heads_out, rows, 0), (tails_in, tails_out, half, 1)
        ):
            arrived = remote(
                out.at[0, pl.ds(0, n)], ref.at[flipped(m)], asend.at[which, m],
                arecv.at[which, m], col=mate,
            )
            arrived.wait_recv()

    for d in range(8):
        base = d * prows
        ctx[:, base : base + LANES] = heads_in[d]
        for h in (0, 1):
            ctx[h * half : (h + 1) * half, base + LANES : base + prows] = tails_in[
                d, :, h * (LANES // 2) : h * (LANES // 2) + rest_lanes
            ]

    for b in range(4):
        resid[:, b * quarter : (b + 1) * quarter] = jnp.dot(
            ctx[...], pfull[b], preferred_element_type=f32
        )

    def norm2(i, c):
        at = pl.ds(pl.multiple_of(i * chunk, chunk), chunk)
        to = pl.ds(pl.multiple_of(me * rows + i * chunk, chunk), chunk)
        value = tok[at, :].astype(f32) + resid[at, :] + vec[4:5, :]
        resid[at, :] = value
        x2[to, :] = norm(value, 2, 3).astype(bf16)
        return c

    lax.fori_loop(0, rows // chunk, norm2, 0)
    second = Gather(x2, 1)
    second.start()
    second.event0()

    @pl.when(end)
    def _():
        z_wait(3, near)
        z_wait(3, other)
        z_wait(3, far)

    starts, done = [], 0
    for width in pieces:
        starts.append(done + (features - width - 2 * done) * pair)
        done += width
    targets = (dn, yn, xn, me)

    class Piece:
        def __init__(self, p):
            self.p, self.width = p, pieces[p]
            self.cols = pl.ds(pl.multiple_of(starts[p], LANES), pieces[p])

        def copy(self, i, src, dst, to):
            return remote(src, dst, ssend.at[self.p, i], srecv.at[self.p, i], col=to)

        def of(self, ref, k, h):
            return ref.at[k, pl.ds(h * half, half), self.cols]

        def to_mate(self, k):
            block = flipped(6 - 2 * k + 1)
            return self.copy(k, part.at[lines(block), self.cols], mated.at[k, :, self.cols], mate)

        def compute(self, stage):
            weight = f2.at[self.cols]

            def body(t, c):
                k = 2 - t % 2 if stage == 0 else 3 * (t % 2)
                block = flipped(6 - 2 * k + 1 - t // 2)
                at = lines(block)
                part[at, self.cols] = project_back(hid[at, :], weight[...]).astype(bf16)

                @pl.when(t < 2)
                def _():
                    self.to_mate(k).start()

                return c

            lax.fori_loop(0, 4, body, 0)

        def mine(self, k, h):
            at = pl.ds(pl.multiple_of(targets[k] * rows + h * half, half), half)
            return part[at, self.cols].astype(f32) + mated[
                k, h * half : (h + 1) * half, self.cols
            ].astype(f32)

        def put(self, k, h, value):
            sums[k, h * half : (h + 1) * half, self.cols] = value.astype(bf16)

        def relays(self, h):
            return relay.at[h, :, self.cols]

        def c(self, i):
            k, h, dst, to = {
                4: (0, 0, self.relays(0), xn),
                5: (0, 1, self.relays(1), yn),
                6: (2, 0, self.of(landed, 0, 0), xn),
                7: (1, 1, self.of(landed, 1, 1), yn),
                8: (1, 0, self.of(landed, 1, 0), yn),
                9: (2, 1, self.of(landed, 0, 1), xn),
            }[i]
            return self.copy(i, self.of(sums, k, h), dst, to)

        def open_direct(self):
            self.to_mate(2).wait_recv()
            self.put(2, 0, self.mine(2, 0))
            self.c(6).start()
            self.to_mate(1).wait_recv()
            self.put(1, 1, self.mine(1, 1))
            self.c(7).start()

        def open_relayed(self):
            self.to_mate(0).wait_recv()
            self.put(0, 0, self.mine(0, 0))
            self.c(4).start()
            self.put(0, 1, self.mine(0, 1))
            self.c(5).start()

        def pass_on(self):
            self.c(4).wait_recv()
            self.put(1, 0, self.mine(1, 0) + relay[0, :, self.cols].astype(f32))
            self.c(8).start()
            self.c(5).wait_recv()
            self.put(2, 1, self.mine(2, 1) + relay[1, :, self.cols].astype(f32))
            self.c(9).start()

        def close(self):
            self.to_mate(3).wait_recv()
            for i in (6, 7, 8, 9):
                self.c(i).wait_recv()
            for h in (0, 1):
                at = slice(h * half, (h + 1) * half)
                total = (
                    self.mine(3, h)
                    + landed[0, at, self.cols].astype(f32)
                    + landed[1, at, self.cols].astype(f32)
                )
                value = resid[at, self.cols] + total + vec[5:6, self.cols]
                o_ref[at, self.cols] = value.astype(o_ref.dtype)

        def finish(self):
            for k in range(4):
                self.to_mate(k).wait_send()
            for i in range(4, 10):
                self.c(i).wait_send()

    one, two, three, four = (Piece(p) for p in range(4))

    def fc1_block(i, c):
        @pl.when(i == 1)
        def _():
            second.mate0()

        @pl.when(i == 2)
        def _():
            second.event1()

        @pl.when(i == 3)
        def _():
            second.mate1()

        @pl.when(i == 6)
        def _():
            second.event2()

        @pl.when(jnp.logical_and(i == 2, middle))
        def _():
            z_forward(4, 2)

        @pl.when(jnp.logical_and(i == 5, middle))
        def _():
            z_forward(5, 3)
            z_forward(6, 3)

        @pl.when(i == 7)
        def _():
            second.mate2()

        at = lines(flipped(i))
        for c0 in range(0, hidden, 2 * LANES):
            cols = slice(c0, c0 + 2 * LANES)
            value = jnp.dot(x2[at, :], f1[:, cols], preferred_element_type=f32) + vec[7:8, cols]
            hid[at, cols] = (
                0.5 * value * (1.0 + lax.erf(value * 0.7071067811865476))
            ).astype(bf16)

        @pl.when(jnp.logical_and(i == 5, end))
        def _():
            z_wait(4, near)

        @pl.when(i == 5)
        def _():
            one.compute(0)
            one.open_direct()

        return c

    lax.fori_loop(0, 8, fc1_block, 0)

    one.compute(1)
    one.open_relayed()

    @pl.when(end)
    def _():
        z_wait(4, other)

    two.compute(0)
    two.open_direct()
    two.compute(1)
    two.open_relayed()
    one.pass_on()

    @pl.when(end)
    def _():
        z_wait(5, far)

    three.compute(0)
    three.open_direct()
    three.compute(1)
    three.open_relayed()
    two.pass_on()
    one.close()

    @pl.when(end)
    def _():
        z_wait(6, far)

    four.compute(0)
    four.open_direct()
    four.compute(1)
    four.open_relayed()
    three.pass_on()
    two.close()
    four.pass_on()
    three.close()
    four.close()

    for piece in (one, two, three, four):
        piece.finish()
    second.finish()
    p_finish(0, lo)
    p_finish(1, hi)
    for m in range(1, 8):
        for c in a_copies(0, 0, m, mate):
            c.wait_send()
    for w in range(5):
        own_copy(w, 0).wait_send()

    @pl.when(middle)
    def _():
        for w in range(5):
            own_copy(w, 1).wait_send()
            z_copy(w, 2, other).wait_send()
        for w in (0, 1, 2, 3, 5, 6):
            z_copy(w, 3, far).wait_send()
            z_copy(w, 4, near).wait_send()


def layer_call(plan, *arrays):
    rows, features, quarter = plan["rows"], plan["features"], plan["quarter"]
    hidden = plan["hidden"]
    wide = 3 * plan["heads"] * LANES
    length = 8 * rows
    bf16, f32 = jnp.bfloat16, jnp.float32
    dma = pltpu.SemaphoreType.DMA
    return pl.pallas_call(
        functools.partial(layer_kernel, plan),
        out_shape=jax.ShapeDtypeStruct((rows, features), f32),
        in_specs=[pl.BlockSpec(memory_space=pl.ANY)] * 13,
        out_specs=pl.BlockSpec(memory_space=pltpu.VMEM),
        scratch_shapes=[
            pltpu.VMEM((rows, features), bf16),
            pltpu.VMEM(arrays[9].shape, bf16),
            *(pltpu.VMEM(arrays[i].shape, bf16) for i in (1, 2, 5, 6, 4, 8, 3, 7)),
            pltpu.VMEM((8, features), f32),
            pltpu.VMEM((length, features), bf16),
            pltpu.VMEM((length, features), bf16),
            pltpu.VMEM((features, plan["whole"]), bf16),
            pltpu.VMEM((4, 32, quarter // 32 * plan["rest"]), bf16),
            pltpu.VMEM((features, wide), bf16),
            pltpu.VMEM((1, wide), f32),
            pltpu.VMEM((length, wide), bf16),
            pltpu.VMEM((rows, features), bf16),
            pltpu.VMEM((4, 2 * rows, LANES), bf16),
            pltpu.VMEM((4, rows, LANES), bf16),
            pltpu.VMEM((8, rows, LANES), bf16),
            pltpu.VMEM((8, rows // 2, LANES), bf16),
            pltpu.VMEM((4, features, quarter), bf16),
            pltpu.VMEM((features, hidden), bf16),
            pltpu.VMEM((features, hidden), bf16),
            pltpu.VMEM((rows, features), f32),
            pltpu.VMEM((4, rows, features), bf16),
            pltpu.VMEM((3, rows, features), bf16),
            pltpu.VMEM((2, rows // 2, features), bf16),
            pltpu.VMEM((2, rows, features), bf16),
            dma((13,)),
            dma((35,)), dma((28,)),
            dma((2, 14)), dma((2, 14)),
            dma((2, 9)), dma((2, 9)),
            dma((2, 8)), dma((2, 8)),
            dma((4, 10)), dma((4, 10)),
        ],
        compiler_params=pltpu.CompilerParams(
            collective_id=3, has_side_effects=True, vmem_limit_bytes=60 * 1024 * 1024
        ),
        name="layer",
    )(*arrays)


def local(
    tokens_in,
    ln1_gain,
    ln1_bias,
    qkv_weight,
    qkv_bias,
    proj_weight,
    proj_bias,
    ln2_gain,
    ln2_bias,
    fc1_weight,
    fc1_bias,
    fc2_weight,
    fc2_bias,
):
    local_heads = HEADS // lax.axis_size("col")
    own_rows, features = tokens_in.shape
    size = qkv_weight.shape[1] // (3 * local_heads)
    padded = -(-(size + 1) // LANES) * LANES
    plan = fast_plan(
        local_heads, own_rows, features, qkv_weight.shape[1], proj_weight.shape[0],
        fc1_weight.shape[1],
    )
    if plan is not None:
        return layer_call(
            plan, tokens_in, ln1_gain, ln1_bias, qkv_bias, proj_bias, ln2_gain, ln2_bias, fc1_bias,
            fc2_bias, qkv_weight.T, proj_weight, fc1_weight, fc2_weight,
        ).astype(jnp.bfloat16)
    inputs = tokens_in.astype(jnp.float32)
    qkv_full = gather_row(qkv_weight, 0)
    proj_full = gather_row(proj_weight, 1)
    fc1_full = gather_row(fc1_weight, 0)
    fc2_full = gather_row(fc2_weight, 0)
    fc1_shift = fc1_bias.astype(jnp.float32)

    spare = padded - size
    qkv_wide = jnp.pad(
        qkv_full.reshape(features, local_heads, 3, size), ((0, 0), (0, 0), (0, 0), (0, spare))
    ).reshape(features, local_heads * 3 * padded)
    shift = jnp.pad(
        qkv_bias.astype(jnp.float32).reshape(local_heads, 3, size), ((0, 0), (0, 0), (0, spare))
    )
    shift = shift.at[:, 2, size].set(1.0).reshape(-1)
    scale = jnp.ones((local_heads, 3, padded), jnp.float32)
    scale = scale.at[:, 0].set(1.4426950408889634 / size**0.5).reshape(-1)

    ln1 = norm_local(inputs, ln1_gain, ln1_bias).astype(jnp.bfloat16)
    product = jnp.dot(gather_col(ln1, 0), qkv_wide, preferred_element_type=jnp.float32)
    qkv = ((product + shift) * scale).astype(jnp.bfloat16)
    attn = attend(qkv, local_heads, size, padded)
    proj_whole = cube_gather_col(proj_full)
    own_heads = lax.all_to_all(attn, "col", split_axis=0, concat_axis=1, tiled=True)
    attn_sum = jnp.dot(own_heads, proj_whole, preferred_element_type=jnp.float32)
    resid = inputs + attn_sum + proj_bias.astype(jnp.float32)
    ln2 = norm_local(resid, ln2_gain, ln2_bias).astype(jnp.bfloat16)
    product = jnp.dot(gather_col(ln2, 1), fc1_full, preferred_element_type=jnp.float32) + fc1_shift
    hidden = jax.nn.gelu(product, approximate=False).astype(jnp.bfloat16)
    mlp_sum = scatter_col(project_back(hidden, fc2_full).astype(jnp.bfloat16), 2)
    result = resid + mlp_sum + fc2_bias.astype(jnp.float32)
    return result.astype(jnp.bfloat16)


def solution(mesh):
    in_specs = (
        P(("row", "col"), None),
        P(),
        P(),
        P("row", "col"),
        P("col"),
        P("col", "row"),
        P(),
        P(),
        P(),
        P("row", "col"),
        P("col"),
        P("row", "col"),
        P(),
    )
    out_specs = P(("row", "col"), None)
    return jax.shard_map(local, mesh=mesh, in_specs=in_specs, out_specs=out_specs, check_vma=False)
```

```python
import functools

import jax
import jax.numpy as jnp
from jax import lax
from jax.experimental import pallas as pl
from jax.experimental.pallas import tpu as pltpu
from jax.sharding import PartitionSpec as P

HEADS = 16
LANES = 128
MESH = pl.DeviceIdType.MESH


def greet(peers):
    barrier = pltpu.get_barrier_semaphore()
    for peer in peers:
        pl.semaphore_signal(barrier, inc=1, device_id={"col": peer}, device_id_type=MESH)
    pl.semaphore_wait(barrier, len(peers))


def neighbours():
    me = lax.axis_index("col")
    core, x, y = me % 2, (me // 2) % 2, me // 4
    place = lambda y, x, core: y * 4 + x * 2 + core
    return (
        me,
        place(y, x, 1 - core),
        place(y, 1 - x, core),
        place(1 - y, x, core),
        place(1 - y, 1 - x, core),
    )


def gather_kernel(x_ref, o_ref, send, recv, local_sem):
    rows = x_ref.shape[0]
    half = rows // 2
    me, mate, xn, yn, dn = neighbours()
    greet((mate, xn, yn))

    def part(block, h):
        return o_ref.at[pl.ds(pl.multiple_of(block * rows + h * half, half), half)]

    def copy(i, src, block, h, to):
        return pltpu.make_async_remote_copy(
            src_ref=src, dst_ref=part(block, h), send_sem=send.at[i], recv_sem=recv.at[i],
            device_id={"col": to}, device_id_type=MESH,
        )

    def own(h):
        return x_ref.at[pl.ds(h * half, half)]

    def arrived(i, block, h):
        copy(i, own(0), block, h, mate).wait_recv()

    started = []

    def go(c):
        c.start()
        started.append(c)

    go(copy(0, own(0), me, 0, xn))
    go(copy(1, own(1), me, 1, yn))
    go(copy(2, own(1), me, 1, xn))
    go(copy(3, own(0), me, 0, yn))
    go(copy(6, own(0), me, 0, mate))
    go(copy(7, own(1), me, 1, mate))
    here = pltpu.make_async_copy(
        x_ref, o_ref.at[pl.ds(pl.multiple_of(me * rows, rows), rows)], local_sem
    )
    here.start()
    arrived(0, xn, 0)
    go(copy(4, part(xn, 0), xn, 0, yn))
    go(copy(8, part(xn, 0), xn, 0, mate))
    arrived(1, yn, 1)
    go(copy(5, part(yn, 1), yn, 1, xn))
    go(copy(9, part(yn, 1), yn, 1, mate))
    arrived(2, xn, 1)
    go(copy(10, part(xn, 1), xn, 1, mate))
    arrived(3, yn, 0)
    go(copy(11, part(yn, 0), yn, 0, mate))
    arrived(4, dn, 0)
    go(copy(12, part(dn, 0), dn, 0, mate))
    arrived(5, dn, 1)
    go(copy(13, part(dn, 1), dn, 1, mate))
    across = lambda block: block + mate - me
    for i, block, h in (
        (6, me, 0), (7, me, 1), (8, xn, 0), (9, yn, 1),
        (10, xn, 1), (11, yn, 0), (12, dn, 0), (13, dn, 1),
    ):
        arrived(i, across(block), h)
    for c in started:
        c.wait_send()
    here.wait()


def gather_col(x, collective_id):
    n = lax.axis_size("col")
    rows, width = x.shape
    if n != 8 or rows % 32:
        return lax.all_gather(x, "col", axis=0, tiled=True)
    return pl.pallas_call(
        gather_kernel,
        out_shape=jax.ShapeDtypeStruct((n * rows, width), x.dtype),
        in_specs=[pl.BlockSpec(memory_space=pltpu.VMEM)],
        out_specs=pl.BlockSpec(memory_space=pltpu.VMEM),
        scratch_shapes=[
            pltpu.SemaphoreType.DMA((14,)),
            pltpu.SemaphoreType.DMA((14,)),
            pltpu.SemaphoreType.DMA,
        ],
        compiler_params=pltpu.CompilerParams(
            collective_id=collective_id, has_side_effects=True, vmem_limit_bytes=24 << 20
        ),
        cost_estimate=pl.CostEstimate(
            flops=10**10, bytes_accessed=2 * n * rows * width, transcendentals=0
        ),
        name="gather_col",
    )(x)


def scatter_kernel(x_ref, o_ref, mated, sums, relay, landed, send, recv):
    rows = o_ref.shape[0]
    half = rows // 2
    me, mate, xn, yn, dn = neighbours()
    greet((mate, xn, yn))
    shift = mate - me
    targets = (dn, xn, yn, me)

    def copy(i, src, dst, to):
        return pltpu.make_async_remote_copy(
            src_ref=src, dst_ref=dst, send_sem=send.at[i], recv_sem=recv.at[i],
            device_id={"col": to}, device_id_type=MESH,
        )

    def block(j):
        return pl.ds(pl.multiple_of(j * rows, rows), rows)

    started = []

    def go(c):
        c.start()
        started.append(c)

    for k, target in enumerate(targets):
        go(copy(k, x_ref.at[block(target + shift)], mated.at[k], mate))

    def mine(k, h):
        rows_h = pl.ds(pl.multiple_of(targets[k] * rows + h * half, half), half)
        return x_ref[rows_h, :].astype(jnp.float32) + mated[k, pl.ds(h * half, half), :].astype(
            jnp.float32
        )

    def put(k, h, value):
        sums[k, pl.ds(h * half, half), :] = value.astype(jnp.bfloat16)

    def of(ref, k, h):
        return ref.at[k, pl.ds(h * half, half)]

    started[0].wait_recv()
    put(0, 0, mine(0, 0))
    go(copy(4, of(sums, 0, 0), relay.at[0], xn))
    put(0, 1, mine(0, 1))
    go(copy(5, of(sums, 0, 1), relay.at[1], yn))
    started[1].wait_recv()
    put(1, 0, mine(1, 0))
    go(copy(6, of(sums, 1, 0), of(landed, 0, 0), xn))
    started[2].wait_recv()
    put(2, 1, mine(2, 1))
    go(copy(7, of(sums, 2, 1), of(landed, 1, 1), yn))
    started[4].wait_recv()
    put(2, 0, mine(2, 0) + relay[0].astype(jnp.float32))
    go(copy(8, of(sums, 2, 0), of(landed, 1, 0), yn))
    started[5].wait_recv()
    put(1, 1, mine(1, 1) + relay[1].astype(jnp.float32))
    go(copy(9, of(sums, 1, 1), of(landed, 0, 1), xn))
    started[3].wait_recv()
    for i in (6, 7, 8, 9):
        started[i].wait_recv()
    for h in (0, 1):
        lines = pl.ds(h * half, half)
        o_ref[lines, :] = (
            mine(3, h)
            + landed[0, lines, :].astype(jnp.float32)
            + landed[1, lines, :].astype(jnp.float32)
        )
    for c in started:
        c.wait_send()


def scatter_col(x, collective_id):
    n = lax.axis_size("col")
    rows, width = x.shape[0] // n, x.shape[1]
    if n != 8 or rows % 32:
        return lax.psum_scatter(x, "col", scatter_dimension=0, tiled=True).astype(jnp.float32)
    return pl.pallas_call(
        scatter_kernel,
        out_shape=jax.ShapeDtypeStruct((rows, width), jnp.float32),
        in_specs=[pl.BlockSpec(memory_space=pltpu.VMEM)],
        out_specs=pl.BlockSpec(memory_space=pltpu.VMEM),
        scratch_shapes=[
            pltpu.VMEM((4, rows, width), x.dtype),
            pltpu.VMEM((3, rows, width), x.dtype),
            pltpu.VMEM((2, rows // 2, width), x.dtype),
            pltpu.VMEM((2, rows, width), x.dtype),
            pltpu.SemaphoreType.DMA((10,)),
            pltpu.SemaphoreType.DMA((10,)),
        ],
        compiler_params=pltpu.CompilerParams(
            collective_id=collective_id, has_side_effects=True, vmem_limit_bytes=32 << 20
        ),
        cost_estimate=pl.CostEstimate(
            flops=10**10, bytes_accessed=2 * n * rows * width, transcendentals=0
        ),
        name="scatter_col",
    )(x)


def gather_row(weight, axis):
    n = lax.axis_size("row")
    me = lax.axis_index("row")
    depth = weight.shape[axis]
    shape = list(weight.shape)
    shape[axis] *= n
    whole = jnp.zeros(shape, weight.dtype)
    for step in range(n):
        block = weight
        if step:
            block = lax.ppermute(weight, "row", [((i + step) % n, i) for i in range(n)])
        whole = lax.dynamic_update_slice_in_dim(whole, block, ((me + step) % n) * depth, axis)
    return whole


def cube_gather_col(x):
    n = lax.axis_size("col")
    if n != 8:
        return lax.all_gather(x, "col", axis=0, tiled=True)
    me = lax.axis_index("col")
    x = x[None]
    for bit, after in ((2, 1), (4, 2), (1, 4)):
        other = lax.ppermute(x, "col", [(i, i ^ bit) for i in range(n)])
        low = (me // bit) % 2 == 0
        first, second = jnp.where(low, x, other), jnp.where(low, other, x)
        x = jnp.concatenate([first, second], axis=0) if bit != 1 else jnp.stack([first, second], 1)
    return x.reshape(-1, x.shape[-1])


def norm_local(values, gain, bias):
    mean = jnp.mean(values, axis=-1, keepdims=True)
    centred = values - mean
    var = jnp.mean(centred * centred, axis=-1, keepdims=True)
    return centred * lax.rsqrt(var + 1e-06) * gain.astype(jnp.float32) + bias.astype(jnp.float32)


def attend_kernel(heads, size, padded, q_ref, kv_ref, o_ref):
    outs = []
    for head in range(heads):
        base = head * 3 * padded
        query = q_ref[:, base : base + padded]
        keys = kv_ref[:, base + padded : base + 2 * padded]
        values = kv_ref[:, base + 2 * padded : base + 3 * padded]
        scores = lax.dot_general(
            query, keys, (((1,), (1,)), ((), ())), preferred_element_type=jnp.float32
        )
        top = jnp.max(scores, axis=-1, keepdims=True)
        expo = jnp.exp2(scores - top).astype(jnp.bfloat16)
        mixed = jnp.dot(expo, values, preferred_element_type=jnp.float32)
        outs.append(mixed[:, :size] / mixed[:, size : size + 1])
    o_ref[...] = jnp.concatenate(outs, axis=1).astype(o_ref.dtype)


def attend(qkv, heads, size, padded):
    length, width = qkv.shape
    block = min(256, length)
    return pl.pallas_call(
        functools.partial(attend_kernel, heads, size, padded),
        grid=(length // block,),
        in_specs=[
            pl.BlockSpec((block, width), lambda i: (i, 0)),
            pl.BlockSpec((length, width), lambda i: (0, 0)),
        ],
        out_specs=pl.BlockSpec((block, heads * size), lambda i: (i, 0)),
        out_shape=jax.ShapeDtypeStruct((length, heads * size), jnp.bfloat16),
        compiler_params=pltpu.CompilerParams(vmem_limit_bytes=40 << 20),
        cost_estimate=pl.CostEstimate(
            flops=4 * heads * length * length * padded * 8,
            bytes_accessed=4 * length * width,
            transcendentals=heads * length * length,
        ),
        name="attend",
    )(qkv, qkv)


def project_back(left, right):
    return lax.dot_general(
        left, right, (((1,), (1,)), ((), ())), preferred_element_type=jnp.float32
    )


def fast_plan(heads, own_rows, features, qkv_width, proj_rows, hidden):
    if lax.axis_size("col") != 8 or lax.axis_size("row") != 4:
        return None
    quarter = features // 4
    size = qkv_width // (3 * heads)
    whole = qkv_width // LANES * LANES
    rest = qkv_width - whole
    ok = (
        hidden == 3 * heads * LANES and own_rows % 32 == 0 and features % LANES == 0 and quarter % 32 == 0
        and hidden % LANES == 0 and 0 < rest and proj_rows == heads * size
        and proj_rows % 16 == 0 and 0 < proj_rows - LANES <= LANES // 2
        and 8 * proj_rows == features and size < LANES and whole // size == 3 * heads - 1
    )
    if not ok:
        return None
    first = 2 * quarter // LANES * LANES
    last = -(-quarter // LANES) * LANES
    middle = features - first - last
    if middle <= LANES or last <= LANES or features - last > 3 * quarter:
        return None
    if (first + middle - LANES - 2 * quarter) % 32:
        return None
    return dict(
        heads=heads, size=size, rows=own_rows, features=features, quarter=quarter, whole=whole,
        rest=rest, proj_rows=proj_rows, hidden=hidden,
        pieces=(first, middle - LANES, LANES, last - LANES, LANES),
        early=first + middle - LANES - 2 * quarter,
    )


def layer_kernel(
    plan, tok_in, g1, c1, qb, pb, g2, c2, d1, d2, wq_in, wp, w1, w2, o_ref,
    tok, wq, v1, v2, v3, v4, v5, v6, v7, v8,
    vec, x1, x2, qmain, qrest, qwide, qrow, qkv, ctx, heads_out, tails_out, heads_in, tails_in, pfull, f1, f2, resid,
    mated, sums, relay, landed,
    lsem, osem, zsend, zrecv, gsend, grecv, psend, precv, asend, arecv, ssend, srecv,
):
    heads, size, rows = plan["heads"], plan["size"], plan["rows"]
    features, quarter = plan["features"], plan["quarter"]
    whole, rest, prows = plan["whole"], plan["rest"], plan["proj_rows"]
    hidden, pieces = plan["hidden"], plan["pieces"]
    half = rows // 2
    groups = 3 * heads
    f32, bf16 = jnp.float32, jnp.bfloat16
    hid, part = qkv, x1

    row = lax.axis_index("row")
    me, mate, xn, yn, dn = neighbours()
    shift = mate - me
    pair = row // 2
    near = row + 1 - 2 * (row % 2)
    other = 2 - pair
    far = 3 - 3 * pair
    middle = jnp.logical_or(row == 1, row == 2)
    end = jnp.logical_or(row == 0, row == 3)
    lo = 2 * pair
    hi = 2 - lo

    def flipped(mask):
        bits = [(me % 2 + mask % 2) % 2, (me // 2 % 2 + mask // 2 % 2) % 2, (me // 4 + mask // 4) % 2]
        return bits[0] + 2 * bits[1] + 4 * bits[2]

    barrier = pltpu.get_barrier_semaphore()
    for step in range(1, 8):
        pl.semaphore_signal(
            barrier, inc=1, device_id={"col": flipped(step)}, device_id_type=MESH
        )
    pl.semaphore_signal(barrier, inc=1, device_id={"row": near}, device_id_type=MESH)

    @pl.when(middle)
    def _():
        pl.semaphore_signal(barrier, inc=1, device_id={"row": other}, device_id_type=MESH)


    def load(i, src, dst):
        return pltpu.make_async_copy(src, dst, lsem.at[i])

    def remote(src, dst, ssem, rsem, **to):
        return pltpu.make_async_remote_copy(
            src_ref=src, dst_ref=dst, send_sem=ssem, recv_sem=rsem,
            device_id=to, device_id_type=MESH,
        )

    def lines(b, n=rows):
        return pl.ds(pl.multiple_of(b * n, n), n)

    early = plan["early"]

    def cut(w, b):
        low = b // 2
        return {
            5: (1 - low) * LANES,
            6: low * (quarter - LANES),
            7: (1 - low) * (quarter - early),
            8: low * early,
        }[w]

    def length_of(w):
        return {5: quarter - LANES, 6: LANES, 7: early, 8: quarter - early}[w]

    def place(w, b):
        if w == 0:
            return qmain.at[lines(b, quarter)]
        if w == 1:
            return qrest.at[b]
        if w == 2:
            return pfull.at[b, lines(me, prows)]
        if w == 3:
            return f1.at[lines(b, quarter)]
        if w == 4:
            return f2.at[lines(b, quarter)]
        return f2.at[pl.ds(pl.multiple_of(b * quarter + cut(w, b), 32), length_of(w))]

    def source(w):
        if w == 0:
            return place(0, row)
        return (None, qrest.at[row], wp, w1, w2)[w]

    zwhich = (0, 1, 1, 2, 2)

    def zslot(w, which):
        return w * 3 + which if w < 5 else 10 + w

    def z_copy(w, s, b):
        return remote(
            place(w, b), place(w, b), zsend.at[min(w, 3) * 5 + s], zrecv.at[zslot(w, zwhich[s])],
            row=other if s in (1, 4) else near,
        )

    def own_copy(w, s):
        return remote(
            source(w), place(w, row), zsend.at[min(w, 3) * 5 + s], zrecv.at[zslot(w, zwhich[s])],
            row=other if s == 1 else near,
        )

    def z_wait(w, which):
        z_copy(w, (0, 2, 3)[which], (near, other, far)[which]).wait_recv()

    def z_forward(w, s):
        which = {2: 1, 3: 2, 4: 0}[s]
        z_wait(w, which)
        z_copy(w, s, (near, other, far)[which]).start()

    def z_sent(s):
        for w in (0, 1, 2):
            z_copy(w, s, row).wait_send()
        both = f1.at[pl.ds(0, 2 * quarter)]
        remote(both, both, zsend.at[15 + s], zrecv.at[0], row=near).wait_send()

    loads = [load(0, wq_in, wq), load(1, tok_in, tok)]
    for i, (src, dst) in enumerate(
        ((g1, v1), (c1, v2), (g2, v3), (c2, v4), (pb, v5), (d2, v6), (qb, v7), (d1, v8))
    ):
        loads.append(load(i + 2, src, dst))
    loads.append(load(10, wp, place(2, row)))
    loads.append(load(11, w1, place(3, row)))
    loads.append(load(12, w2, place(4, row)))
    for c in loads:
        c.start()
    loads[0].wait()
    turned = wq[...].astype(f32).T.astype(bf16)
    qmain[lines(row, quarter), :] = turned[:, :whole]
    for j in range(quarter // 32):
        qrest[row, :, j * rest : (j + 1) * rest] = turned[32 * j : 32 * (j + 1), whole:]
    for i, v in enumerate((v1, v2, v3, v4, v5, v6, v7, v8)):
        loads[i + 2].wait()
        vec[i : i + 1, : v.shape[0]] = v[...].astype(f32).reshape(1, -1)
    loads[1].wait()
    pl.semaphore_wait(barrier, 8 + row * (3 - row) // 2)
    for w in (0, 1, 2):
        own_copy(w, 0).start()

    @pl.when(middle)
    def _():
        for w in (0, 1, 2):
            own_copy(w, 1).start()

    @pl.when(end)
    def _():
        for w in (3, 4):
            own_copy(w, 0).start()

    def norm(values, g, b):
        mean = jnp.mean(values, axis=-1, keepdims=True)
        centred = values - mean
        var = jnp.mean(centred * centred, axis=-1, keepdims=True)
        return centred * lax.rsqrt(var + 1e-06) * vec[g : g + 1, :] + vec[b : b + 1, :]

    chunk = 32

    def norm1(i, c):
        at = pl.ds(pl.multiple_of(i * chunk, chunk), chunk)
        to = pl.ds(pl.multiple_of(me * rows + i * chunk, chunk), chunk)
        x1[to, :] = norm(tok[at, :].astype(f32), 0, 1).astype(bf16)
        return c

    lax.fori_loop(0, rows // chunk, norm1, 0)

    class Gather:
        wait_on = (0, 1, 2, 2, 3, 3, 4, 4, 5, 5, 5, 5, 6, 6)

        def __init__(self, x, gi):
            self.x, self.gi = x, gi

        def copy(self, i, block, h, to):
            at = self.x.at[pl.ds(pl.multiple_of(block * rows + h * half, half), half)]
            return remote(
                at, at, gsend.at[self.gi], grecv.at[self.gi, self.wait_on[i]], col=to
            )

        def arrived(self, i, count):
            at = self.x.at[pl.ds(0, count * half)]
            remote(at, at, gsend.at[self.gi], grecv.at[self.gi, i], col=mate).wait_recv()

        def start(self):
            for i, h, to in ((0, 0, xn), (1, 1, yn), (2, 1, xn), (3, 0, yn), (6, 0, mate), (7, 1, mate)):
                self.copy(i, me, h, to).start()

        def event0(self):
            self.arrived(0, 1)
            self.copy(4, xn, 0, yn).start()
            self.copy(8, xn, 0, mate).start()
            self.arrived(1, 1)
            self.copy(5, yn, 1, xn).start()
            self.copy(9, yn, 1, mate).start()

        def event1(self):
            self.arrived(2, 2)
            self.copy(10, xn, 1, mate).start()
            self.copy(11, yn, 0, mate).start()

        def event2(self):
            self.arrived(3, 2)
            self.copy(12, dn, 0, mate).start()
            self.copy(13, dn, 1, mate).start()

        def mate0(self):
            self.arrived(4, 2)

        def mate1(self):
            self.arrived(5, 4)

        def mate2(self):
            self.arrived(6, 2)

        def finish(self):
            at = self.x.at[pl.ds(0, 14 * half)]
            remote(at, at, gsend.at[self.gi], grecv.at[self.gi, 0], col=mate).wait_send()

    first = Gather(x1, 0)
    first.start()
    qrow[...] = jnp.zeros_like(qrow)
    for g in range(groups):
        qrow[:, g * LANES : g * LANES + size] = vec[6:7, g * size : (g + 1) * size]
    lane = lax.broadcasted_iota(jnp.int32, (1, LANES), 1)
    for head in range(heads):
        at = slice((3 * head + 2) * LANES, (3 * head + 3) * LANES)
        qrow[:, at] = jnp.where(lane == size, 1.0, qrow[:, at])
    for c in loads[10:]:
        c.wait()

    spare = jnp.zeros((quarter, LANES - size), bf16)
    few = jnp.zeros((32, LANES - size), bf16)

    def widen(b):
        base = b * quarter
        at = pl.ds(pl.multiple_of(base, 32), quarter)
        for g in range(groups - 1):
            qwide[at, g * LANES : (g + 1) * LANES] = jnp.concatenate(
                [qmain[at, g * size : (g + 1) * size], spare], axis=1
            )
        for j in range(quarter // 32):
            some = pl.ds(pl.multiple_of(base + 32 * j, 32), 32)
            qwide[some, (groups - 1) * LANES :] = jnp.concatenate(
                [qmain[some, (groups - 1) * size :], qrest[b, :, j * rest : (j + 1) * rest], few],
                axis=1,
            )

    widen(row)

    def q_wait(b):
        z_wait(0, b)
        z_wait(1, b)

    @pl.when(middle)
    def _():
        for w in (0, 1):
            z_forward(w, 4)
        for w in (0, 1):
            z_forward(w, 2)

    first.event0()

    @pl.when(end)
    def _():
        q_wait(0)

    widen(near)

    @pl.when(middle)
    def _():
        z_forward(2, 2)
        z_forward(2, 4)
        own_copy(3, 1).start()
        for w in (0, 1):
            z_forward(w, 3)

    first.event1()

    p_on = (0, 1, 4, 2, 3, 4, 4, 4, 4)

    def pcopy(i, r, at, count, block, to):
        ref = pfull.at[pl.ds(at, count), lines(block, prows)]
        return remote(ref, ref, psend.at[r], precv.at[r, p_on[i]], col=to)

    def punits(r, i, count):
        ref = pfull.at[pl.ds(0, 2), pl.ds(0, count // 2 * prows)]
        return remote(ref, ref, psend.at[r], precv.at[r, i], col=mate)

    def p_start(r, at):
        pcopy(0, r, at, 2, me, xn).start()
        pcopy(1, r, at, 2, me, yn).start()
        pcopy(2, r, at, 2, me, mate).start()

    def p_forward(r, at):
        pcopy(0, r, at, 2, xn, xn).wait_recv()
        pcopy(3, r, at, 1, xn, yn).start()
        pcopy(5, r, at, 2, xn, mate).start()
        pcopy(1, r, at, 2, yn, yn).wait_recv()
        pcopy(4, r, at + 1, 1, yn, xn).start()
        pcopy(6, r, at, 2, yn, mate).start()

    def p_last(r, at):
        pcopy(3, r, at, 1, dn, yn).wait_recv()
        pcopy(7, r, at, 1, dn, mate).start()
        pcopy(4, r, at + 1, 1, dn, xn).wait_recv()
        pcopy(8, r, at + 1, 1, dn, mate).start()

    def p_mates(r):
        punits(r, 4, 8).wait_recv()

    def p_finish(r):
        punits(r, 0, 14).wait_send()


    @pl.when(end)
    def _():
        z_wait(2, 0)

    p_start(0, lo)

    @pl.when(middle)
    def _():
        z_forward(2, 3)
        p_start(1, hi)
        own_copy(3, 0).start()
        z_forward(3, 4)
        own_copy(4, 1).start()

    first.event2()
    first.mate0()

    @pl.when(end)
    def _():
        q_wait(1)
        q_wait(2)

    widen(other)
    widen(far)
    first.mate1()
    first.mate2()

    factor = 1.4426950408889634 / size**0.5

    def qkv_block(i, c):
        @pl.when(jnp.logical_or(jnp.logical_and(i == 1, end), jnp.logical_and(i == 2, middle)))
        def _():
            p_forward(0, lo)

        @pl.when(jnp.logical_and(i == 2, end))
        def _():
            z_wait(2, 1)
            z_wait(2, 2)
            p_start(1, hi)

        at = lines(flipped(2 * i) // 2, 2 * rows)
        product = jnp.dot(x1[at, :], qwide[...], preferred_element_type=f32) + qrow[...]
        for g in range(groups):
            cols = slice(g * LANES, (g + 1) * LANES)
            value = product[:, cols]
            qkv[at, cols] = (value * factor if g % 3 == 0 else value).astype(bf16)
        return c

    lax.fori_loop(0, 4, qkv_block, 0)

    rest_lanes = prows - LANES

    def a_all(which):
        ref = (heads_in, tails_in)[which].at[pl.ds(0, 7)]
        return remote(ref, ref, asend.at[which], arecv.at[which], col=mate)

    def a_copies(i, core, to):
        at = lines(core)
        tail = pl.ds(pl.multiple_of(core * half, half), half)
        return (
            remote(
                heads_out.at[i, at], heads_in.at[me], asend.at[0], arecv.at[0], col=to
            ),
            remote(
                tails_out.at[i, tail], tails_in.at[me], asend.at[1], arecv.at[1], col=to
            ),
        )

    def attend_block(i, c):
        @pl.when(jnp.logical_and(i == 1, middle))
        def _():
            z_forward(3, 2)
            z_forward(4, 4)

        @pl.when(i == 2)
        def _():
            p_last(0, lo)
            p_forward(1, hi)

        chip = flipped(6 - 2 * i) // 2
        at = lines(chip, 2 * rows)
        scores = []
        for head in range(heads):
            base = head * 3 * LANES
            scores.append(
                lax.dot_general(
                    qkv[at, base : base + LANES], qkv[:, base + LANES : base + 2 * LANES],
                    (((1,), (1,)), ((), ())), preferred_element_type=f32,
                )
            )
        expos = [
            jnp.exp2(x - jnp.max(x, axis=-1, keepdims=True)).astype(bf16) for x in scores
        ]
        outs = []
        for head in range(heads):
            base = (head * 3 + 2) * LANES
            mixed = jnp.dot(
                expos[head], qkv[:, base : base + LANES], preferred_element_type=f32
            )
            outs.append(mixed[:, :size] / mixed[:, size : size + 1])
        mixed = jnp.concatenate(outs, axis=1).astype(bf16)
        gap = jnp.zeros((half, LANES // 2 - rest_lanes), bf16)
        heads_out[i] = mixed[:, :LANES]
        for core in (0, 1):
            top, low = (
                mixed[core * rows + h * half : core * rows + (h + 1) * half, LANES:]
                for h in (0, 1)
            )
            tails_out[i, core * half : (core + 1) * half, :] = jnp.concatenate(
                [top, gap, low, gap], axis=1
            )
        for core in (0, 1):
            to = 2 * chip + core

            @pl.when(to != me)
            def _():
                for c in a_copies(i, core, to):
                    c.start()

        return c

    lax.fori_loop(0, 4, attend_block, 0)
    @pl.when(middle)
    def _():
        z_forward(3, 3)
        own_copy(4, 0).start()

    p_last(1, hi)
    first.finish()
    heads_in[me] = heads_out[3, lines(me % 2), :]
    tails_in[me] = tails_out[3, lines(me % 2, half), :]
    p_mates(0)
    p_mates(1)
    a_all(0).wait_recv()
    a_all(1).wait_recv()
    for d in range(8):
        base = d * prows
        ctx[:, base : base + LANES] = heads_in[d]
        for h in (0, 1):
            ctx[h * half : (h + 1) * half, base + LANES : base + prows] = tails_in[
                d, :, h * (LANES // 2) : h * (LANES // 2) + rest_lanes
            ]

    for b in range(4):
        resid[:, b * quarter : (b + 1) * quarter] = jnp.dot(
            ctx[...], pfull[b], preferred_element_type=f32
        )

    def norm2(i, c):
        at = pl.ds(pl.multiple_of(i * chunk, chunk), chunk)
        to = pl.ds(pl.multiple_of(me * rows + i * chunk, chunk), chunk)
        value = tok[at, :].astype(f32) + resid[at, :] + vec[4:5, :]
        resid[at, :] = value
        x2[to, :] = norm(value, 2, 3).astype(bf16)
        return c

    lax.fori_loop(0, rows // chunk, norm2, 0)
    second = Gather(x2, 1)
    second.start()
    second.event0()

    @pl.when(end)
    def _():
        z_wait(3, 0)
        z_wait(3, 1)
        z_wait(3, 2)

    starts, done = [], 0
    for width in pieces:
        starts.append(done + (features - width - 2 * done) * pair)
        done += width
    targets = (dn, yn, xn, me)

    class Piece:
        def __init__(self, p):
            self.p, self.width = p, pieces[p]
            self.cols = pl.ds(pl.multiple_of(starts[p], LANES), pieces[p])

        def copy(self, i, src, dst, to):
            return remote(
                src, dst, ssend.at[self.p, min(i // 4, 1)], srecv.at[self.p, min(i, 6)], col=to
            )

        def of(self, ref, k, h):
            return ref.at[k, pl.ds(h * half, half), self.cols]

        def to_mate(self, k):
            block = flipped(6 - 2 * k + 1)
            return remote(
                part.at[lines(block), self.cols], mated.at[k, :, self.cols],
                ssend.at[self.p, 0], srecv.at[self.p, k], col=mate,
            )

        def compute(self, k):
            at = lines(flipped(6 - 2 * k) // 2, 2 * rows)
            part[at, self.cols] = project_back(hid[at, :], f2[self.cols, :]).astype(bf16)
            self.to_mate(k).start()

        def compute_all(self):
            def body(k, c):
                self.compute(k)
                return c

            lax.fori_loop(0, 4, body, 0)

        def mine(self, k, h):
            at = pl.ds(pl.multiple_of(targets[k] * rows + h * half, half), half)
            return part[at, self.cols].astype(f32) + mated[
                k, h * half : (h + 1) * half, self.cols
            ].astype(f32)

        def put(self, k, h, value):
            sums[k, h * half : (h + 1) * half, self.cols] = value.astype(bf16)

        def relays(self, h):
            return relay.at[h, :, self.cols]

        def c(self, i):
            k, h, dst, to = {
                4: (0, 0, self.relays(0), xn),
                5: (0, 1, self.relays(1), yn),
                6: (2, 0, self.of(landed, 0, 0), xn),
                7: (1, 1, self.of(landed, 1, 1), yn),
                8: (1, 0, self.of(landed, 1, 0), yn),
                9: (2, 1, self.of(landed, 0, 1), xn),
            }[i]
            return self.copy(i, self.of(sums, k, h), dst, to)

        def direct(self, k):
            h = {1: 1, 2: 0}[k]
            self.to_mate(k).wait_recv()
            self.put(k, h, self.mine(k, h))
            self.c({1: 7, 2: 6}[k]).start()

        def open_relayed(self):
            self.to_mate(0).wait_recv()
            self.put(0, 0, self.mine(0, 0))
            self.c(4).start()
            self.put(0, 1, self.mine(0, 1))
            self.c(5).start()

        def pass_on(self):
            self.c(4).wait_recv()
            self.put(1, 0, self.mine(1, 0) + relay[0, :, self.cols].astype(f32))
            self.c(8).start()
            self.c(5).wait_recv()
            self.put(2, 1, self.mine(2, 1) + relay[1, :, self.cols].astype(f32))
            self.c(9).start()

        def close(self):
            self.to_mate(3).wait_recv()
            ref = landed.at[:, :, self.cols]
            self.copy(6, ref, ref, mate).wait_recv()
            for h in (0, 1):
                at = slice(h * half, (h + 1) * half)
                total = (
                    self.mine(3, h)
                    + landed[0, at, self.cols].astype(f32)
                    + landed[1, at, self.cols].astype(f32)
                )
                resid[at, self.cols] = resid[at, self.cols] + total + vec[5:6, self.cols]
            self.out().start()

        def out(self):
            return pltpu.make_async_copy(
                resid.at[:, self.cols], o_ref.at[:, self.cols], osem.at[self.p]
            )

        def finish(self):
            self.out().wait()
            ref = mated.at[:, :, self.cols]
            self.copy(0, ref, ref, mate).wait_send()
            ref = sums.at[:, :, self.cols]
            self.copy(6, ref, ref, mate).wait_send()

    one, two, after, three, four = (Piece(p) for p in range(5))

    def fc1_block(i, c):
        @pl.when(i == 0)
        def _():
            second.mate0()

        @pl.when(i == 1)
        def _():
            second.event1()

        @pl.when(jnp.logical_and(i == 1, middle))
        def _():
            z_wait(4, 1)
            z_copy(7, 2, other).start()
            z_copy(8, 2, other).start()

        @pl.when(i == 1)
        def _():
            second.mate1()

        @pl.when(i == 3)
        def _():
            second.event2()

        @pl.when(jnp.logical_and(i == 3, middle))
        def _():
            z_wait(4, 2)
            z_copy(5, 3, far).start()
            z_copy(6, 3, far).start()

        @pl.when(i == 3)
        def _():
            one.direct(1)
            second.mate2()

        at = lines(flipped(2 * i) // 2, 2 * rows)
        for c0 in range(0, hidden, 2 * LANES):
            cols = slice(c0, c0 + 2 * LANES)
            value = jnp.dot(x2[at, :], f1[:, cols], preferred_element_type=f32) + vec[7:8, cols]
            hid[at, cols] = (
                0.5 * value * (1.0 + lax.erf(value * 0.7071067811865476))
            ).astype(bf16)

        @pl.when(jnp.logical_and(i == 1, end))
        def _():
            z_wait(4, 0)

        @pl.when(i == 2)
        def _():
            one.direct(2)

        @pl.when(i > 0)
        def _():
            one.compute(3 - i)

        return c

    lax.fori_loop(0, 4, fc1_block, 0)

    def open_all(piece):
        piece.open_relayed()
        piece.direct(2)
        piece.direct(1)

    one.compute(3)
    one.open_relayed()

    @pl.when(end)
    def _():
        z_wait(7, 1)

    two.compute_all()
    open_all(two)
    one.pass_on()

    @pl.when(end)
    def _():
        z_wait(8, 1)

    after.compute_all()
    open_all(after)
    two.pass_on()

    @pl.when(end)
    def _():
        z_wait(5, 2)

    three.compute_all()
    open_all(three)
    after.pass_on()

    @pl.when(end)
    def _():
        z_wait(6, 2)

    four.compute_all()
    open_all(four)
    three.pass_on()
    one.close()
    four.pass_on()
    two.close()
    after.close()
    three.close()
    four.close()

    for piece in (one, two, after, three, four):
        piece.finish()
    second.finish()
    p_finish(0)
    p_finish(1)
    a_all(0).wait_send()
    a_all(1).wait_send()
    z_sent(0)

    @pl.when(middle)
    def _():
        for way in range(1, 5):
            z_sent(way)


def layer_call(plan, *arrays):
    rows, features, quarter = plan["rows"], plan["features"], plan["quarter"]
    hidden = plan["hidden"]
    wide = 3 * plan["heads"] * LANES
    length = 8 * rows
    bf16, f32 = jnp.bfloat16, jnp.float32
    dma = pltpu.SemaphoreType.DMA
    return pl.pallas_call(
        functools.partial(layer_kernel, plan),
        out_shape=jax.ShapeDtypeStruct((rows, features), f32),
        in_specs=[pl.BlockSpec(memory_space=pl.ANY)] * 13,
        out_specs=pl.BlockSpec(memory_space=pl.ANY),
        scratch_shapes=[
            pltpu.VMEM((rows, features), bf16),
            pltpu.VMEM(arrays[9].shape, bf16),
            *(pltpu.VMEM(arrays[i].shape, bf16) for i in (1, 2, 5, 6, 4, 8, 3, 7)),
            pltpu.VMEM((8, features), f32),
            pltpu.VMEM((length, features), bf16),
            pltpu.VMEM((length, features), bf16),
            pltpu.VMEM((features, plan["whole"]), bf16),
            pltpu.VMEM((4, 32, quarter // 32 * plan["rest"]), bf16),
            pltpu.VMEM((features, wide), bf16),
            pltpu.VMEM((1, wide), f32),
            pltpu.VMEM((length, wide), bf16),
            pltpu.VMEM((rows, features), bf16),
            pltpu.VMEM((4, 2 * rows, LANES), bf16),
            pltpu.VMEM((4, rows, LANES), bf16),
            pltpu.VMEM((8, rows, LANES), bf16),
            pltpu.VMEM((8, rows // 2, LANES), bf16),
            pltpu.VMEM((4, features, quarter), bf16),
            pltpu.VMEM((features, hidden), bf16),
            pltpu.VMEM((features, hidden), bf16),
            pltpu.VMEM((rows, features), f32),
            pltpu.VMEM((4, rows, features), bf16),
            pltpu.VMEM((3, rows, features), bf16),
            pltpu.VMEM((2, rows // 2, features), bf16),
            pltpu.VMEM((2, rows, features), bf16),
            dma((13,)), dma((5,)),
            dma((20,)), dma((19,)),
            dma((2,)), dma((2, 7)),
            dma((2,)), dma((2, 5)),
            dma((2,)), dma((2,)),
            dma((5, 2)), dma((5, 7)),
        ],
        compiler_params=pltpu.CompilerParams(
            collective_id=3, has_side_effects=True, vmem_limit_bytes=60 * 1024 * 1024
        ),
        name="layer",
    )(*arrays)


def local(
    tokens_in,
    ln1_gain,
    ln1_bias,
    qkv_weight,
    qkv_bias,
    proj_weight,
    proj_bias,
    ln2_gain,
    ln2_bias,
    fc1_weight,
    fc1_bias,
    fc2_weight,
    fc2_bias,
):
    local_heads = HEADS // lax.axis_size("col")
    own_rows, features = tokens_in.shape
    size = qkv_weight.shape[1] // (3 * local_heads)
    padded = -(-(size + 1) // LANES) * LANES
    plan = fast_plan(
        local_heads, own_rows, features, qkv_weight.shape[1], proj_weight.shape[0],
        fc1_weight.shape[1],
    )
    if plan is not None:
        return layer_call(
            plan, tokens_in, ln1_gain, ln1_bias, qkv_bias, proj_bias, ln2_gain, ln2_bias, fc1_bias,
            fc2_bias, qkv_weight.T, proj_weight, fc1_weight, fc2_weight,
        ).astype(jnp.bfloat16)
    inputs = tokens_in.astype(jnp.float32)
    qkv_full = gather_row(qkv_weight, 0)
    proj_full = gather_row(proj_weight, 1)
    fc1_full = gather_row(fc1_weight, 0)
    fc2_full = gather_row(fc2_weight, 0)
    fc1_shift = fc1_bias.astype(jnp.float32)

    spare = padded - size
    qkv_wide = jnp.pad(
        qkv_full.reshape(features, local_heads, 3, size), ((0, 0), (0, 0), (0, 0), (0, spare))
    ).reshape(features, local_heads * 3 * padded)
    shift = jnp.pad(
        qkv_bias.astype(jnp.float32).reshape(local_heads, 3, size), ((0, 0), (0, 0), (0, spare))
    )
    shift = shift.at[:, 2, size].set(1.0).reshape(-1)
    scale = jnp.ones((local_heads, 3, padded), jnp.float32)
    scale = scale.at[:, 0].set(1.4426950408889634 / size**0.5).reshape(-1)

    ln1 = norm_local(inputs, ln1_gain, ln1_bias).astype(jnp.bfloat16)
    product = jnp.dot(gather_col(ln1, 0), qkv_wide, preferred_element_type=jnp.float32)
    qkv = ((product + shift) * scale).astype(jnp.bfloat16)
    attn = attend(qkv, local_heads, size, padded)
    proj_whole = cube_gather_col(proj_full)
    own_heads = lax.all_to_all(attn, "col", split_axis=0, concat_axis=1, tiled=True)
    attn_sum = jnp.dot(own_heads, proj_whole, preferred_element_type=jnp.float32)
    resid = inputs + attn_sum + proj_bias.astype(jnp.float32)
    ln2 = norm_local(resid, ln2_gain, ln2_bias).astype(jnp.bfloat16)
    product = jnp.dot(gather_col(ln2, 1), fc1_full, preferred_element_type=jnp.float32) + fc1_shift
    hidden = jax.nn.gelu(product, approximate=False).astype(jnp.bfloat16)
    mlp_sum = scatter_col(project_back(hidden, fc2_full).astype(jnp.bfloat16), 2)
    result = resid + mlp_sum + fc2_bias.astype(jnp.float32)
    return result.astype(jnp.bfloat16)


def solution(mesh):
    in_specs = (
        P(("row", "col"), None),
        P(),
        P(),
        P("row", "col"),
        P("col"),
        P("col", "row"),
        P(),
        P(),
        P(),
        P("row", "col"),
        P("col"),
        P("row", "col"),
        P(),
    )
    out_specs = P(("row", "col"), None)
    return jax.shard_map(local, mesh=mesh, in_specs=in_specs, out_specs=out_specs, check_vma=False)
```

```python
import functools

import jax
import jax.numpy as jnp
from jax import lax
from jax.experimental import pallas as pl
from jax.experimental.pallas import tpu as pltpu
from jax.sharding import PartitionSpec as P

HEADS = 16
LANES = 128
MESH = pl.DeviceIdType.MESH


def greet(peers):
    barrier = pltpu.get_barrier_semaphore()
    for peer in peers:
        pl.semaphore_signal(barrier, inc=1, device_id={"col": peer}, device_id_type=MESH)
    pl.semaphore_wait(barrier, len(peers))


def neighbours():
    me = lax.axis_index("col")
    core, x, y = me % 2, (me // 2) % 2, me // 4
    place = lambda y, x, core: y * 4 + x * 2 + core
    return (
        me,
        place(y, x, 1 - core),
        place(y, 1 - x, core),
        place(1 - y, x, core),
        place(1 - y, 1 - x, core),
    )


def gather_kernel(x_ref, o_ref, send, recv, local_sem):
    rows = x_ref.shape[0]
    half = rows // 2
    me, mate, xn, yn, dn = neighbours()
    greet((mate, xn, yn))

    def part(block, h):
        return o_ref.at[pl.ds(pl.multiple_of(block * rows + h * half, half), half)]

    def copy(i, src, block, h, to):
        return pltpu.make_async_remote_copy(
            src_ref=src, dst_ref=part(block, h), send_sem=send.at[i], recv_sem=recv.at[i],
            device_id={"col": to}, device_id_type=MESH,
        )

    def own(h):
        return x_ref.at[pl.ds(h * half, half)]

    def arrived(i, block, h):
        copy(i, own(0), block, h, mate).wait_recv()

    started = []

    def go(c):
        c.start()
        started.append(c)

    go(copy(0, own(0), me, 0, xn))
    go(copy(1, own(1), me, 1, yn))
    go(copy(2, own(1), me, 1, xn))
    go(copy(3, own(0), me, 0, yn))
    go(copy(6, own(0), me, 0, mate))
    go(copy(7, own(1), me, 1, mate))
    here = pltpu.make_async_copy(
        x_ref, o_ref.at[pl.ds(pl.multiple_of(me * rows, rows), rows)], local_sem
    )
    here.start()
    arrived(0, xn, 0)
    go(copy(4, part(xn, 0), xn, 0, yn))
    go(copy(8, part(xn, 0), xn, 0, mate))
    arrived(1, yn, 1)
    go(copy(5, part(yn, 1), yn, 1, xn))
    go(copy(9, part(yn, 1), yn, 1, mate))
    arrived(2, xn, 1)
    go(copy(10, part(xn, 1), xn, 1, mate))
    arrived(3, yn, 0)
    go(copy(11, part(yn, 0), yn, 0, mate))
    arrived(4, dn, 0)
    go(copy(12, part(dn, 0), dn, 0, mate))
    arrived(5, dn, 1)
    go(copy(13, part(dn, 1), dn, 1, mate))
    across = lambda block: block + mate - me
    for i, block, h in (
        (6, me, 0), (7, me, 1), (8, xn, 0), (9, yn, 1),
        (10, xn, 1), (11, yn, 0), (12, dn, 0), (13, dn, 1),
    ):
        arrived(i, across(block), h)
    for c in started:
        c.wait_send()
    here.wait()


def gather_col(x, collective_id):
    n = lax.axis_size("col")
    rows, width = x.shape
    if n != 8 or rows % 32:
        return lax.all_gather(x, "col", axis=0, tiled=True)
    return pl.pallas_call(
        gather_kernel,
        out_shape=jax.ShapeDtypeStruct((n * rows, width), x.dtype),
        in_specs=[pl.BlockSpec(memory_space=pltpu.VMEM)],
        out_specs=pl.BlockSpec(memory_space=pltpu.VMEM),
        scratch_shapes=[
            pltpu.SemaphoreType.DMA((14,)),
            pltpu.SemaphoreType.DMA((14,)),
            pltpu.SemaphoreType.DMA,
        ],
        compiler_params=pltpu.CompilerParams(
            collective_id=collective_id, has_side_effects=True, vmem_limit_bytes=24 << 20
        ),
        cost_estimate=pl.CostEstimate(
            flops=10**10, bytes_accessed=2 * n * rows * width, transcendentals=0
        ),
        name="gather_col",
    )(x)


def scatter_kernel(x_ref, o_ref, mated, sums, relay, landed, send, recv):
    rows = o_ref.shape[0]
    half = rows // 2
    me, mate, xn, yn, dn = neighbours()
    greet((mate, xn, yn))
    shift = mate - me
    targets = (dn, xn, yn, me)

    def copy(i, src, dst, to):
        return pltpu.make_async_remote_copy(
            src_ref=src, dst_ref=dst, send_sem=send.at[i], recv_sem=recv.at[i],
            device_id={"col": to}, device_id_type=MESH,
        )

    def block(j):
        return pl.ds(pl.multiple_of(j * rows, rows), rows)

    started = []

    def go(c):
        c.start()
        started.append(c)

    for k, target in enumerate(targets):
        go(copy(k, x_ref.at[block(target + shift)], mated.at[k], mate))

    def mine(k, h):
        rows_h = pl.ds(pl.multiple_of(targets[k] * rows + h * half, half), half)
        return x_ref[rows_h, :].astype(jnp.float32) + mated[k, pl.ds(h * half, half), :].astype(
            jnp.float32
        )

    def put(k, h, value):
        sums[k, pl.ds(h * half, half), :] = value.astype(jnp.bfloat16)

    def of(ref, k, h):
        return ref.at[k, pl.ds(h * half, half)]

    started[0].wait_recv()
    put(0, 0, mine(0, 0))
    go(copy(4, of(sums, 0, 0), relay.at[0], xn))
    put(0, 1, mine(0, 1))
    go(copy(5, of(sums, 0, 1), relay.at[1], yn))
    started[1].wait_recv()
    put(1, 0, mine(1, 0))
    go(copy(6, of(sums, 1, 0), of(landed, 0, 0), xn))
    started[2].wait_recv()
    put(2, 1, mine(2, 1))
    go(copy(7, of(sums, 2, 1), of(landed, 1, 1), yn))
    started[4].wait_recv()
    put(2, 0, mine(2, 0) + relay[0].astype(jnp.float32))
    go(copy(8, of(sums, 2, 0), of(landed, 1, 0), yn))
    started[5].wait_recv()
    put(1, 1, mine(1, 1) + relay[1].astype(jnp.float32))
    go(copy(9, of(sums, 1, 1), of(landed, 0, 1), xn))
    started[3].wait_recv()
    for i in (6, 7, 8, 9):
        started[i].wait_recv()
    for h in (0, 1):
        lines = pl.ds(h * half, half)
        o_ref[lines, :] = (
            mine(3, h)
            + landed[0, lines, :].astype(jnp.float32)
            + landed[1, lines, :].astype(jnp.float32)
        )
    for c in started:
        c.wait_send()


def scatter_col(x, collective_id):
    n = lax.axis_size("col")
    rows, width = x.shape[0] // n, x.shape[1]
    if n != 8 or rows % 32:
        return lax.psum_scatter(x, "col", scatter_dimension=0, tiled=True).astype(jnp.float32)
    return pl.pallas_call(
        scatter_kernel,
        out_shape=jax.ShapeDtypeStruct((rows, width), jnp.float32),
        in_specs=[pl.BlockSpec(memory_space=pltpu.VMEM)],
        out_specs=pl.BlockSpec(memory_space=pltpu.VMEM),
        scratch_shapes=[
            pltpu.VMEM((4, rows, width), x.dtype),
            pltpu.VMEM((3, rows, width), x.dtype),
            pltpu.VMEM((2, rows // 2, width), x.dtype),
            pltpu.VMEM((2, rows, width), x.dtype),
            pltpu.SemaphoreType.DMA((10,)),
            pltpu.SemaphoreType.DMA((10,)),
        ],
        compiler_params=pltpu.CompilerParams(
            collective_id=collective_id, has_side_effects=True, vmem_limit_bytes=32 << 20
        ),
        cost_estimate=pl.CostEstimate(
            flops=10**10, bytes_accessed=2 * n * rows * width, transcendentals=0
        ),
        name="scatter_col",
    )(x)


def gather_row(weight, axis):
    n = lax.axis_size("row")
    me = lax.axis_index("row")
    depth = weight.shape[axis]
    shape = list(weight.shape)
    shape[axis] *= n
    whole = jnp.zeros(shape, weight.dtype)
    for step in range(n):
        block = weight
        if step:
            block = lax.ppermute(weight, "row", [((i + step) % n, i) for i in range(n)])
        whole = lax.dynamic_update_slice_in_dim(whole, block, ((me + step) % n) * depth, axis)
    return whole


def cube_gather_col(x):
    n = lax.axis_size("col")
    if n != 8:
        return lax.all_gather(x, "col", axis=0, tiled=True)
    me = lax.axis_index("col")
    x = x[None]
    for bit, after in ((2, 1), (4, 2), (1, 4)):
        other = lax.ppermute(x, "col", [(i, i ^ bit) for i in range(n)])
        low = (me // bit) % 2 == 0
        first, second = jnp.where(low, x, other), jnp.where(low, other, x)
        x = jnp.concatenate([first, second], axis=0) if bit != 1 else jnp.stack([first, second], 1)
    return x.reshape(-1, x.shape[-1])


def norm_local(values, gain, bias):
    mean = jnp.mean(values, axis=-1, keepdims=True)
    centred = values - mean
    var = jnp.mean(centred * centred, axis=-1, keepdims=True)
    return centred * lax.rsqrt(var + 1e-06) * gain.astype(jnp.float32) + bias.astype(jnp.float32)


def attend_kernel(heads, size, padded, q_ref, kv_ref, o_ref):
    outs = []
    for head in range(heads):
        base = head * 3 * padded
        query = q_ref[:, base : base + padded]
        keys = kv_ref[:, base + padded : base + 2 * padded]
        values = kv_ref[:, base + 2 * padded : base + 3 * padded]
        scores = lax.dot_general(
            query, keys, (((1,), (1,)), ((), ())), preferred_element_type=jnp.float32
        )
        top = jnp.max(scores, axis=-1, keepdims=True)
        expo = jnp.exp2(scores - top).astype(jnp.bfloat16)
        mixed = jnp.dot(expo, values, preferred_element_type=jnp.float32)
        outs.append(mixed[:, :size] / mixed[:, size : size + 1])
    o_ref[...] = jnp.concatenate(outs, axis=1).astype(o_ref.dtype)


def attend(qkv, heads, size, padded):
    length, width = qkv.shape
    block = min(256, length)
    return pl.pallas_call(
        functools.partial(attend_kernel, heads, size, padded),
        grid=(length // block,),
        in_specs=[
            pl.BlockSpec((block, width), lambda i: (i, 0)),
            pl.BlockSpec((length, width), lambda i: (0, 0)),
        ],
        out_specs=pl.BlockSpec((block, heads * size), lambda i: (i, 0)),
        out_shape=jax.ShapeDtypeStruct((length, heads * size), jnp.bfloat16),
        compiler_params=pltpu.CompilerParams(vmem_limit_bytes=40 << 20),
        cost_estimate=pl.CostEstimate(
            flops=4 * heads * length * length * padded * 8,
            bytes_accessed=4 * length * width,
            transcendentals=heads * length * length,
        ),
        name="attend",
    )(qkv, qkv)


def project_back(left, right):
    return lax.dot_general(
        left, right, (((1,), (1,)), ((), ())), preferred_element_type=jnp.float32
    )


def fast_plan(heads, own_rows, features, qkv_width, proj_rows, hidden):
    if lax.axis_size("col") != 8 or lax.axis_size("row") != 4:
        return None
    quarter = features // 4
    size = qkv_width // (3 * heads)
    whole = qkv_width // LANES * LANES
    rest = qkv_width - whole
    ok = (
        hidden == 3 * heads * LANES and own_rows % 32 == 0 and features % LANES == 0 and quarter % 32 == 0
        and hidden % LANES == 0 and 0 < rest and proj_rows == heads * size
        and proj_rows % 16 == 0 and 0 < proj_rows - LANES <= LANES // 2
        and 8 * proj_rows == features and size < LANES and whole // size == 3 * heads - 1
    )
    if not ok:
        return None
    first = 2 * quarter // LANES * LANES
    last = -(-quarter // LANES) * LANES
    middle = features - first - last
    if middle <= LANES or last <= LANES or features - last > 3 * quarter:
        return None
    if (first + middle - LANES - 2 * quarter) % 32:
        return None
    return dict(
        heads=heads, size=size, rows=own_rows, features=features, quarter=quarter, whole=whole,
        rest=rest, proj_rows=proj_rows, hidden=hidden,
        pieces=(first, middle - LANES, LANES, last - LANES, LANES),
        early=first + middle - LANES - 2 * quarter,
    )


def layer_kernel(
    plan, tok_in, g1, c1, qb, pb, g2, c2, d1, d2, wq_in, wp, w1, w2, o_ref,
    tok, wq, v1, v2, v3, v4, v5, v6, v7, v8,
    vec, x1, x2, qmain, qrest, qwide, qrow, qkv, ctx, heads_out, tails_out, heads_in, tails_in, pfull, f1, f2, resid,
    mated, sums, relay, landed,
    lsem, zsend, zrecv, gsend, grecv, psend, precv, asend, arecv, ssend, srecv,
):
    heads, size, rows = plan["heads"], plan["size"], plan["rows"]
    features, quarter = plan["features"], plan["quarter"]
    whole, rest, prows = plan["whole"], plan["rest"], plan["proj_rows"]
    hidden, pieces = plan["hidden"], plan["pieces"]
    half = rows // 2
    groups = 3 * heads
    f32, bf16 = jnp.float32, jnp.bfloat16
    hid, part = qkv, x1

    row = lax.axis_index("row")
    me, mate, xn, yn, dn = neighbours()
    shift = mate - me
    pair = row // 2
    near = row + 1 - 2 * (row % 2)
    other = 2 - pair
    far = 3 - 3 * pair
    middle = jnp.logical_or(row == 1, row == 2)
    end = jnp.logical_or(row == 0, row == 3)
    lo = 2 * pair
    hi = 2 - lo

    def flipped(mask):
        bits = [(me % 2 + mask % 2) % 2, (me // 2 % 2 + mask // 2 % 2) % 2, (me // 4 + mask // 4) % 2]
        return bits[0] + 2 * bits[1] + 4 * bits[2]

    barrier = pltpu.get_barrier_semaphore()
    for step in range(1, 8):
        pl.semaphore_signal(
            barrier, inc=1, device_id={"col": flipped(step)}, device_id_type=MESH
        )
    pl.semaphore_signal(barrier, inc=1, device_id={"row": near}, device_id_type=MESH)

    @pl.when(middle)
    def _():
        pl.semaphore_signal(barrier, inc=1, device_id={"row": other}, device_id_type=MESH)


    def load(i, src, dst):
        return pltpu.make_async_copy(src, dst, lsem.at[i])

    def remote(src, dst, ssem, rsem, **to):
        return pltpu.make_async_remote_copy(
            src_ref=src, dst_ref=dst, send_sem=ssem, recv_sem=rsem,
            device_id=to, device_id_type=MESH,
        )

    def lines(b, n=rows):
        return pl.ds(pl.multiple_of(b * n, n), n)

    early = plan["early"]

    def cut(w, b):
        low = b // 2
        return {
            5: (1 - low) * LANES,
            6: low * (quarter - LANES),
            7: (1 - low) * (quarter - early),
            8: low * early,
        }[w]

    def length_of(w):
        return {5: quarter - LANES, 6: LANES, 7: early, 8: quarter - early}[w]

    def place(w, b):
        if w == 0:
            return qmain.at[lines(b, quarter)]
        if w == 1:
            return qrest.at[b]
        if w == 2:
            return pfull.at[b, lines(me, prows)]
        if w == 3:
            return f1.at[lines(b, quarter)]
        if w == 4:
            return f2.at[lines(b, quarter)]
        return f2.at[pl.ds(pl.multiple_of(b * quarter + cut(w, b), 32), length_of(w))]

    def source(w):
        if w == 0:
            return place(0, row)
        return (None, qrest.at[row], wp, w1, w2)[w]

    zwhich = (0, 1, 1, 2, 2)

    def zslot(w, which):
        return w * 3 + which if w < 5 else 10 + w

    def z_copy(w, s, b):
        return remote(
            place(w, b), place(w, b), zsend.at[min(w, 3) * 5 + s], zrecv.at[zslot(w, zwhich[s])],
            row=other if s in (1, 4) else near,
        )

    def own_copy(w, s):
        return remote(
            source(w), place(w, row), zsend.at[min(w, 3) * 5 + s], zrecv.at[zslot(w, zwhich[s])],
            row=other if s == 1 else near,
        )

    def z_wait(w, which):
        z_copy(w, (0, 2, 3)[which], (near, other, far)[which]).wait_recv()

    def z_forward(w, s):
        which = {2: 1, 3: 2, 4: 0}[s]
        z_wait(w, which)
        z_copy(w, s, (near, other, far)[which]).start()

    def z_sent(s):
        for w in (0, 1, 2):
            z_copy(w, s, row).wait_send()
        both = f1.at[pl.ds(0, 2 * quarter)]
        remote(both, both, zsend.at[15 + s], zrecv.at[0], row=near).wait_send()

    loads = [load(0, wq_in, wq), load(1, tok_in, tok)]
    for i, (src, dst) in enumerate(
        ((g1, v1), (c1, v2), (g2, v3), (c2, v4), (pb, v5), (d2, v6), (qb, v7), (d1, v8))
    ):
        loads.append(load(i + 2, src, dst))
    loads.append(load(10, wp, place(2, row)))
    loads.append(load(11, w1, place(3, row)))
    loads.append(load(12, w2, place(4, row)))
    for c in loads:
        c.start()
    loads[0].wait()
    turned = wq[...].astype(f32).T.astype(bf16)
    qmain[lines(row, quarter), :] = turned[:, :whole]
    for j in range(quarter // 32):
        qrest[row, :, j * rest : (j + 1) * rest] = turned[32 * j : 32 * (j + 1), whole:]
    for i, v in enumerate((v1, v2, v3, v4, v5, v6, v7, v8)):
        loads[i + 2].wait()
        vec[i : i + 1, : v.shape[0]] = v[...].astype(f32).reshape(1, -1)
    loads[1].wait()
    pl.semaphore_wait(barrier, 8 + row * (3 - row) // 2)
    for w in (0, 1, 2):
        own_copy(w, 0).start()

    @pl.when(middle)
    def _():
        for w in (0, 1, 2):
            own_copy(w, 1).start()

    @pl.when(end)
    def _():
        for w in (3, 4):
            own_copy(w, 0).start()

    def norm(values, g, b):
        mean = jnp.mean(values, axis=-1, keepdims=True)
        centred = values - mean
        var = jnp.mean(centred * centred, axis=-1, keepdims=True)
        return centred * lax.rsqrt(var + 1e-06) * vec[g : g + 1, :] + vec[b : b + 1, :]

    chunk = 32

    def norm1(i, c):
        at = pl.ds(pl.multiple_of(i * chunk, chunk), chunk)
        to = pl.ds(pl.multiple_of(me * rows + i * chunk, chunk), chunk)
        x1[to, :] = norm(tok[at, :].astype(f32), 0, 1).astype(bf16)
        return c

    lax.fori_loop(0, rows // chunk, norm1, 0)

    class Gather:
        wait_on = (0, 1, 2, 2, 3, 3, 4, 4, 5, 5, 5, 5, 6, 6)

        def __init__(self, x, gi):
            self.x, self.gi = x, gi

        def copy(self, i, block, h, to):
            at = self.x.at[pl.ds(pl.multiple_of(block * rows + h * half, half), half)]
            return remote(
                at, at, gsend.at[self.gi], grecv.at[self.gi, self.wait_on[i]], col=to
            )

        def arrived(self, i, count):
            at = self.x.at[pl.ds(0, count * half)]
            remote(at, at, gsend.at[self.gi], grecv.at[self.gi, i], col=mate).wait_recv()

        def start(self):
            for i, h, to in ((0, 0, xn), (1, 1, yn), (2, 1, xn), (3, 0, yn), (6, 0, mate), (7, 1, mate)):
                self.copy(i, me, h, to).start()

        def event0(self):
            self.arrived(0, 1)
            self.copy(4, xn, 0, yn).start()
            self.copy(8, xn, 0, mate).start()
            self.arrived(1, 1)
            self.copy(5, yn, 1, xn).start()
            self.copy(9, yn, 1, mate).start()

        def event1(self):
            self.arrived(2, 2)
            self.copy(10, xn, 1, mate).start()
            self.copy(11, yn, 0, mate).start()

        def event2(self):
            self.arrived(3, 2)
            self.copy(12, dn, 0, mate).start()
            self.copy(13, dn, 1, mate).start()

        def mate0(self):
            self.arrived(4, 2)

        def mate1(self):
            self.arrived(5, 4)

        def mate2(self):
            self.arrived(6, 2)

        def finish(self):
            at = self.x.at[pl.ds(0, 14 * half)]
            remote(at, at, gsend.at[self.gi], grecv.at[self.gi, 0], col=mate).wait_send()

    first = Gather(x1, 0)
    first.start()
    qrow[...] = jnp.zeros_like(qrow)
    for g in range(groups):
        qrow[:, g * LANES : g * LANES + size] = vec[6:7, g * size : (g + 1) * size]
    lane = lax.broadcasted_iota(jnp.int32, (1, LANES), 1)
    for head in range(heads):
        at = slice((3 * head + 2) * LANES, (3 * head + 3) * LANES)
        qrow[:, at] = jnp.where(lane == size, 1.0, qrow[:, at])
    for c in loads[10:]:
        c.wait()

    spare = jnp.zeros((quarter, LANES - size), bf16)
    few = jnp.zeros((32, LANES - size), bf16)

    def widen(b):
        base = b * quarter
        at = pl.ds(pl.multiple_of(base, 32), quarter)
        for g in range(groups - 1):
            qwide[at, g * LANES : (g + 1) * LANES] = jnp.concatenate(
                [qmain[at, g * size : (g + 1) * size], spare], axis=1
            )
        for j in range(quarter // 32):
            some = pl.ds(pl.multiple_of(base + 32 * j, 32), 32)
            qwide[some, (groups - 1) * LANES :] = jnp.concatenate(
                [qmain[some, (groups - 1) * size :], qrest[b, :, j * rest : (j + 1) * rest], few],
                axis=1,
            )

    widen(row)

    def q_wait(b):
        z_wait(0, b)
        z_wait(1, b)

    @pl.when(middle)
    def _():
        for w in (0, 1):
            z_forward(w, 4)
        for w in (0, 1):
            z_forward(w, 2)

    first.event0()

    @pl.when(end)
    def _():
        q_wait(0)

    widen(near)

    @pl.when(middle)
    def _():
        z_forward(2, 2)
        z_forward(2, 4)
        own_copy(3, 1).start()
        for w in (0, 1):
            z_forward(w, 3)

    first.event1()

    p_on = (0, 1, 4, 2, 3, 4, 4, 4, 4)

    def pcopy(i, r, at, count, block, to):
        ref = pfull.at[pl.ds(at, count), lines(block, prows)]
        return remote(ref, ref, psend.at[r], precv.at[r, p_on[i]], col=to)

    def punits(r, i, count):
        ref = pfull.at[pl.ds(0, 2), pl.ds(0, count // 2 * prows)]
        return remote(ref, ref, psend.at[r], precv.at[r, i], col=mate)

    def p_start(r, at):
        pcopy(0, r, at, 2, me, xn).start()
        pcopy(1, r, at, 2, me, yn).start()
        pcopy(2, r, at, 2, me, mate).start()

    def p_forward(r, at):
        pcopy(0, r, at, 2, xn, xn).wait_recv()
        pcopy(3, r, at, 1, xn, yn).start()
        pcopy(5, r, at, 2, xn, mate).start()
        pcopy(1, r, at, 2, yn, yn).wait_recv()
        pcopy(4, r, at + 1, 1, yn, xn).start()
        pcopy(6, r, at, 2, yn, mate).start()

    def p_last(r, at):
        pcopy(3, r, at, 1, dn, yn).wait_recv()
        pcopy(7, r, at, 1, dn, mate).start()
        pcopy(4, r, at + 1, 1, dn, xn).wait_recv()
        pcopy(8, r, at + 1, 1, dn, mate).start()

    def p_mates(r):
        punits(r, 4, 8).wait_recv()

    def p_finish(r):
        punits(r, 0, 14).wait_send()


    @pl.when(end)
    def _():
        z_wait(2, 0)

    p_start(0, lo)

    @pl.when(middle)
    def _():
        z_forward(2, 3)
        p_start(1, hi)
        own_copy(3, 0).start()
        z_forward(3, 4)
        own_copy(4, 1).start()

    first.event2()
    first.mate0()

    @pl.when(end)
    def _():
        q_wait(1)
        q_wait(2)

    widen(other)
    widen(far)
    first.mate1()
    first.mate2()

    factor = 1.4426950408889634 / size**0.5

    def qkv_block(i, c):
        @pl.when(jnp.logical_or(jnp.logical_and(i == 1, end), jnp.logical_and(i == 2, middle)))
        def _():
            p_forward(0, lo)

        @pl.when(jnp.logical_and(i == 2, end))
        def _():
            z_wait(2, 1)
            z_wait(2, 2)
            p_start(1, hi)

        at = lines(flipped(2 * i) // 2, 2 * rows)
        product = jnp.dot(x1[at, :], qwide[...], preferred_element_type=f32) + qrow[...]
        for g in range(groups):
            cols = slice(g * LANES, (g + 1) * LANES)
            value = product[:, cols]
            qkv[at, cols] = (value * factor if g % 3 == 0 else value).astype(bf16)
        return c

    lax.fori_loop(0, 4, qkv_block, 0)

    rest_lanes = prows - LANES

    def a_all(which):
        ref = (heads_in, tails_in)[which].at[pl.ds(0, 7)]
        return remote(ref, ref, asend.at[which], arecv.at[which], col=mate)

    def a_copies(i, core, to):
        at = lines(core)
        tail = pl.ds(pl.multiple_of(core * half, half), half)
        return (
            remote(
                heads_out.at[i, at], heads_in.at[me], asend.at[0], arecv.at[0], col=to
            ),
            remote(
                tails_out.at[i, tail], tails_in.at[me], asend.at[1], arecv.at[1], col=to
            ),
        )

    def attend_block(i, c):
        @pl.when(jnp.logical_and(i == 1, middle))
        def _():
            z_forward(3, 2)
            z_forward(4, 4)

        @pl.when(i == 2)
        def _():
            p_last(0, lo)
            p_forward(1, hi)

        chip = flipped(6 - 2 * i) // 2
        at = lines(chip, 2 * rows)
        scores = []
        for head in range(heads):
            base = head * 3 * LANES
            scores.append(
                lax.dot_general(
                    qkv[at, base : base + LANES], qkv[:, base + LANES : base + 2 * LANES],
                    (((1,), (1,)), ((), ())), preferred_element_type=f32,
                )
            )
        expos = [
            jnp.exp2(x - jnp.max(x, axis=-1, keepdims=True)).astype(bf16) for x in scores
        ]
        outs = []
        for head in range(heads):
            base = (head * 3 + 2) * LANES
            mixed = jnp.dot(
                expos[head], qkv[:, base : base + LANES], preferred_element_type=f32
            )
            outs.append(mixed[:, :size] / mixed[:, size : size + 1])
        mixed = jnp.concatenate(outs, axis=1).astype(bf16)
        gap = jnp.zeros((half, LANES // 2 - rest_lanes), bf16)
        heads_out[i] = mixed[:, :LANES]
        for core in (0, 1):
            top, low = (
                mixed[core * rows + h * half : core * rows + (h + 1) * half, LANES:]
                for h in (0, 1)
            )
            tails_out[i, core * half : (core + 1) * half, :] = jnp.concatenate(
                [top, gap, low, gap], axis=1
            )
        for core in (0, 1):
            to = 2 * chip + core

            @pl.when(to != me)
            def _():
                for c in a_copies(i, core, to):
                    c.start()

        return c

    lax.fori_loop(0, 4, attend_block, 0)
    @pl.when(middle)
    def _():
        z_forward(3, 3)
        own_copy(4, 0).start()

    p_last(1, hi)
    first.finish()
    heads_in[me] = heads_out[3, lines(me % 2), :]
    tails_in[me] = tails_out[3, lines(me % 2, half), :]
    p_mates(0)
    p_mates(1)
    a_all(0).wait_recv()
    a_all(1).wait_recv()
    for d in range(8):
        base = d * prows
        ctx[:, base : base + LANES] = heads_in[d]
        for h in (0, 1):
            ctx[h * half : (h + 1) * half, base + LANES : base + prows] = tails_in[
                d, :, h * (LANES // 2) : h * (LANES // 2) + rest_lanes
            ]

    for b in range(4):
        resid[:, b * quarter : (b + 1) * quarter] = jnp.dot(
            ctx[...], pfull[b], preferred_element_type=f32
        )

    def norm2(i, c):
        at = pl.ds(pl.multiple_of(i * chunk, chunk), chunk)
        to = pl.ds(pl.multiple_of(me * rows + i * chunk, chunk), chunk)
        value = tok[at, :].astype(f32) + resid[at, :] + vec[4:5, :]
        resid[at, :] = value
        x2[to, :] = norm(value, 2, 3).astype(bf16)
        return c

    lax.fori_loop(0, rows // chunk, norm2, 0)
    second = Gather(x2, 1)
    second.start()
    second.event0()

    @pl.when(end)
    def _():
        z_wait(3, 0)
        z_wait(3, 1)
        z_wait(3, 2)

    starts, done = [], 0
    for width in pieces:
        starts.append(done + (features - width - 2 * done) * pair)
        done += width
    targets = (dn, yn, xn, me)

    class Piece:
        def __init__(self, p):
            self.p, self.width = p, pieces[p]
            self.cols = pl.ds(pl.multiple_of(starts[p], LANES), pieces[p])

        def copy(self, i, src, dst, to):
            return remote(
                src, dst, ssend.at[self.p, min(i // 4, 1)], srecv.at[self.p, min(i, 6)], col=to
            )

        def of(self, ref, k, h):
            return ref.at[k, pl.ds(h * half, half), self.cols]

        def to_mate(self, k):
            block = flipped(6 - 2 * k + 1)
            return remote(
                part.at[lines(block), self.cols], mated.at[k, :, self.cols],
                ssend.at[self.p, 0], srecv.at[self.p, k], col=mate,
            )

        def compute(self, k):
            at = lines(flipped(6 - 2 * k) // 2, 2 * rows)
            part[at, self.cols] = project_back(hid[at, :], f2[self.cols, :]).astype(bf16)
            self.to_mate(k).start()

        def compute_all(self):
            def body(k, c):
                self.compute(k)
                return c

            lax.fori_loop(0, 4, body, 0)

        def mine(self, k, h):
            at = pl.ds(pl.multiple_of(targets[k] * rows + h * half, half), half)
            return part[at, self.cols].astype(f32) + mated[
                k, h * half : (h + 1) * half, self.cols
            ].astype(f32)

        def put(self, k, h, value):
            sums[k, h * half : (h + 1) * half, self.cols] = value.astype(bf16)

        def relays(self, h):
            return relay.at[h, :, self.cols]

        def c(self, i):
            k, h, dst, to = {
                4: (0, 0, self.relays(0), xn),
                5: (0, 1, self.relays(1), yn),
                6: (2, 0, self.of(landed, 0, 0), xn),
                7: (1, 1, self.of(landed, 1, 1), yn),
                8: (1, 0, self.of(landed, 1, 0), yn),
                9: (2, 1, self.of(landed, 0, 1), xn),
            }[i]
            return self.copy(i, self.of(sums, k, h), dst, to)

        def direct(self, k):
            h = {1: 1, 2: 0}[k]
            self.to_mate(k).wait_recv()
            self.put(k, h, self.mine(k, h))
            self.c({1: 7, 2: 6}[k]).start()

        def open_relayed(self):
            self.to_mate(0).wait_recv()
            self.put(0, 0, self.mine(0, 0))
            self.c(4).start()
            self.put(0, 1, self.mine(0, 1))
            self.c(5).start()

        def pass_on(self):
            self.c(4).wait_recv()
            self.put(1, 0, self.mine(1, 0) + relay[0, :, self.cols].astype(f32))
            self.c(8).start()
            self.c(5).wait_recv()
            self.put(2, 1, self.mine(2, 1) + relay[1, :, self.cols].astype(f32))
            self.c(9).start()

        def close(self):
            self.to_mate(3).wait_recv()
            ref = landed.at[:, :, self.cols]
            self.copy(6, ref, ref, mate).wait_recv()
            for h in (0, 1):
                at = slice(h * half, (h + 1) * half)
                total = (
                    self.mine(3, h)
                    + landed[0, at, self.cols].astype(f32)
                    + landed[1, at, self.cols].astype(f32)
                )
                o_ref[at, self.cols] = resid[at, self.cols] + total + vec[5:6, self.cols]

        def finish(self):
            ref = mated.at[:, :, self.cols]
            self.copy(0, ref, ref, mate).wait_send()
            ref = sums.at[:, :, self.cols]
            self.copy(6, ref, ref, mate).wait_send()

    one, two, after, three, four = (Piece(p) for p in range(5))

    def fc1_block(i, c):
        @pl.when(i == 0)
        def _():
            second.mate0()

        @pl.when(i == 1)
        def _():
            second.event1()

        @pl.when(jnp.logical_and(i == 1, middle))
        def _():
            z_wait(4, 1)
            z_copy(7, 2, other).start()
            z_copy(8, 2, other).start()

        @pl.when(i == 1)
        def _():
            second.mate1()

        @pl.when(i == 3)
        def _():
            second.event2()

        @pl.when(jnp.logical_and(i == 3, middle))
        def _():
            z_wait(4, 2)
            z_copy(5, 3, far).start()
            z_copy(6, 3, far).start()

        @pl.when(i == 3)
        def _():
            one.direct(1)
            second.mate2()

        at = lines(flipped(2 * i) // 2, 2 * rows)
        for c0 in range(0, hidden, 2 * LANES):
            cols = slice(c0, c0 + 2 * LANES)
            value = jnp.dot(x2[at, :], f1[:, cols], preferred_element_type=f32) + vec[7:8, cols]
            hid[at, cols] = (
                0.5 * value * (1.0 + lax.erf(value * 0.7071067811865476))
            ).astype(bf16)

        @pl.when(jnp.logical_and(i == 1, end))
        def _():
            z_wait(4, 0)

        @pl.when(i == 2)
        def _():
            one.direct(2)

        @pl.when(i > 0)
        def _():
            one.compute(3 - i)

        return c

    lax.fori_loop(0, 4, fc1_block, 0)

    def open_all(piece):
        piece.open_relayed()
        piece.direct(2)
        piece.direct(1)

    one.compute(3)
    one.open_relayed()

    @pl.when(end)
    def _():
        z_wait(7, 1)

    two.compute_all()
    open_all(two)
    one.pass_on()

    @pl.when(end)
    def _():
        z_wait(8, 1)

    after.compute_all()
    open_all(after)
    two.pass_on()

    @pl.when(end)
    def _():
        z_wait(5, 2)

    three.compute_all()
    open_all(three)
    after.pass_on()

    @pl.when(end)
    def _():
        z_wait(6, 2)

    four.compute_all()
    open_all(four)
    three.pass_on()
    one.close()
    four.pass_on()
    two.close()
    after.close()
    three.close()
    four.close()

    for piece in (one, two, after, three, four):
        piece.finish()
    second.finish()
    p_finish(0)
    p_finish(1)
    a_all(0).wait_send()
    a_all(1).wait_send()
    z_sent(0)

    @pl.when(middle)
    def _():
        for way in range(1, 5):
            z_sent(way)


def layer_call(plan, *arrays):
    rows, features, quarter = plan["rows"], plan["features"], plan["quarter"]
    hidden = plan["hidden"]
    wide = 3 * plan["heads"] * LANES
    length = 8 * rows
    bf16, f32 = jnp.bfloat16, jnp.float32
    dma = pltpu.SemaphoreType.DMA
    return pl.pallas_call(
        functools.partial(layer_kernel, plan),
        out_shape=pltpu.VMEM((rows, features), f32),
        in_specs=[pl.BlockSpec(memory_space=pl.ANY)] * 13,
        out_specs=pl.BlockSpec(memory_space=pltpu.VMEM),
        scratch_shapes=[
            pltpu.VMEM((rows, features), bf16),
            pltpu.VMEM(arrays[9].shape, bf16),
            *(pltpu.VMEM(arrays[i].shape, bf16) for i in (1, 2, 5, 6, 4, 8, 3, 7)),
            pltpu.VMEM((8, features), f32),
            pltpu.VMEM((length, features), bf16),
            pltpu.VMEM((length, features), bf16),
            pltpu.VMEM((features, plan["whole"]), bf16),
            pltpu.VMEM((4, 32, quarter // 32 * plan["rest"]), bf16),
            pltpu.VMEM((features, wide), bf16),
            pltpu.VMEM((1, wide), f32),
            pltpu.VMEM((length, wide), bf16),
            pltpu.VMEM((rows, features), bf16),
            pltpu.VMEM((4, 2 * rows, LANES), bf16),
            pltpu.VMEM((4, rows, LANES), bf16),
            pltpu.VMEM((8, rows, LANES), bf16),
            pltpu.VMEM((8, rows // 2, LANES), bf16),
            pltpu.VMEM((4, features, quarter), bf16),
            pltpu.VMEM((features, hidden), bf16),
            pltpu.VMEM((features, hidden), bf16),
            pltpu.VMEM((rows, features), f32),
            pltpu.VMEM((4, rows, features), bf16),
            pltpu.VMEM((3, rows, features), bf16),
            pltpu.VMEM((2, rows // 2, features), bf16),
            pltpu.VMEM((2, rows, features), bf16),
            dma((13,)),
            dma((20,)), dma((19,)),
            dma((2,)), dma((2, 7)),
            dma((2,)), dma((2, 5)),
            dma((2,)), dma((2,)),
            dma((5, 2)), dma((5, 7)),
        ],
        compiler_params=pltpu.CompilerParams(
            collective_id=3, has_side_effects=True, vmem_limit_bytes=60 * 1024 * 1024
        ),
        name="layer",
    )(*arrays)


def local(
    tokens_in,
    ln1_gain,
    ln1_bias,
    qkv_weight,
    qkv_bias,
    proj_weight,
    proj_bias,
    ln2_gain,
    ln2_bias,
    fc1_weight,
    fc1_bias,
    fc2_weight,
    fc2_bias,
):
    local_heads = HEADS // lax.axis_size("col")
    own_rows, features = tokens_in.shape
    size = qkv_weight.shape[1] // (3 * local_heads)
    padded = -(-(size + 1) // LANES) * LANES
    plan = fast_plan(
        local_heads, own_rows, features, qkv_weight.shape[1], proj_weight.shape[0],
        fc1_weight.shape[1],
    )
    if plan is not None:
        return layer_call(
            plan, tokens_in, ln1_gain, ln1_bias, qkv_bias, proj_bias, ln2_gain, ln2_bias, fc1_bias,
            fc2_bias, qkv_weight.T, proj_weight, fc1_weight, fc2_weight,
        ).astype(jnp.bfloat16)
    inputs = tokens_in.astype(jnp.float32)
    qkv_full = gather_row(qkv_weight, 0)
    proj_full = gather_row(proj_weight, 1)
    fc1_full = gather_row(fc1_weight, 0)
    fc2_full = gather_row(fc2_weight, 0)
    fc1_shift = fc1_bias.astype(jnp.float32)

    spare = padded - size
    qkv_wide = jnp.pad(
        qkv_full.reshape(features, local_heads, 3, size), ((0, 0), (0, 0), (0, 0), (0, spare))
    ).reshape(features, local_heads * 3 * padded)
    shift = jnp.pad(
        qkv_bias.astype(jnp.float32).reshape(local_heads, 3, size), ((0, 0), (0, 0), (0, spare))
    )
    shift = shift.at[:, 2, size].set(1.0).reshape(-1)
    scale = jnp.ones((local_heads, 3, padded), jnp.float32)
    scale = scale.at[:, 0].set(1.4426950408889634 / size**0.5).reshape(-1)

    ln1 = norm_local(inputs, ln1_gain, ln1_bias).astype(jnp.bfloat16)
    product = jnp.dot(gather_col(ln1, 0), qkv_wide, preferred_element_type=jnp.float32)
    qkv = ((product + shift) * scale).astype(jnp.bfloat16)
    attn = attend(qkv, local_heads, size, padded)
    proj_whole = cube_gather_col(proj_full)
    own_heads = lax.all_to_all(attn, "col", split_axis=0, concat_axis=1, tiled=True)
    attn_sum = jnp.dot(own_heads, proj_whole, preferred_element_type=jnp.float32)
    resid = inputs + attn_sum + proj_bias.astype(jnp.float32)
    ln2 = norm_local(resid, ln2_gain, ln2_bias).astype(jnp.bfloat16)
    product = jnp.dot(gather_col(ln2, 1), fc1_full, preferred_element_type=jnp.float32) + fc1_shift
    hidden = jax.nn.gelu(product, approximate=False).astype(jnp.bfloat16)
    mlp_sum = scatter_col(project_back(hidden, fc2_full).astype(jnp.bfloat16), 2)
    result = resid + mlp_sum + fc2_bias.astype(jnp.float32)
    return result.astype(jnp.bfloat16)


def solution(mesh):
    in_specs = (
        P(("row", "col"), None),
        P(),
        P(),
        P("row", "col"),
        P("col"),
        P("col", "row"),
        P(),
        P(),
        P(),
        P("row", "col"),
        P("col"),
        P("row", "col"),
        P(),
    )
    out_specs = P(("row", "col"), None)
    return jax.shard_map(local, mesh=mesh, in_specs=in_specs, out_specs=out_specs, check_vma=False)
```

```python
import functools

import jax
import jax.numpy as jnp
from jax import lax
from jax.experimental import pallas as pl
from jax.experimental.pallas import tpu as pltpu
from jax.sharding import PartitionSpec as P

HEADS = 16
LANES = 128
MESH = pl.DeviceIdType.MESH


def greet(peers):
    barrier = pltpu.get_barrier_semaphore()
    for peer in peers:
        pl.semaphore_signal(barrier, inc=1, device_id={"col": peer}, device_id_type=MESH)
    pl.semaphore_wait(barrier, len(peers))


def neighbours():
    me = lax.axis_index("col")
    core, x, y = me % 2, (me // 2) % 2, me // 4
    place = lambda y, x, core: y * 4 + x * 2 + core
    return (
        me,
        place(y, x, 1 - core),
        place(y, 1 - x, core),
        place(1 - y, x, core),
        place(1 - y, 1 - x, core),
    )


def gather_kernel(x_ref, o_ref, send, recv, local_sem):
    rows = x_ref.shape[0]
    half = rows // 2
    me, mate, xn, yn, dn = neighbours()
    greet((mate, xn, yn))

    def part(block, h):
        return o_ref.at[pl.ds(pl.multiple_of(block * rows + h * half, half), half)]

    def copy(i, src, block, h, to):
        return pltpu.make_async_remote_copy(
            src_ref=src, dst_ref=part(block, h), send_sem=send.at[i], recv_sem=recv.at[i],
            device_id={"col": to}, device_id_type=MESH,
        )

    def own(h):
        return x_ref.at[pl.ds(h * half, half)]

    def arrived(i, block, h):
        copy(i, own(0), block, h, mate).wait_recv()

    started = []

    def go(c):
        c.start()
        started.append(c)

    go(copy(0, own(0), me, 0, xn))
    go(copy(1, own(1), me, 1, yn))
    go(copy(2, own(1), me, 1, xn))
    go(copy(3, own(0), me, 0, yn))
    go(copy(6, own(0), me, 0, mate))
    go(copy(7, own(1), me, 1, mate))
    here = pltpu.make_async_copy(
        x_ref, o_ref.at[pl.ds(pl.multiple_of(me * rows, rows), rows)], local_sem
    )
    here.start()
    arrived(0, xn, 0)
    go(copy(4, part(xn, 0), xn, 0, yn))
    go(copy(8, part(xn, 0), xn, 0, mate))
    arrived(1, yn, 1)
    go(copy(5, part(yn, 1), yn, 1, xn))
    go(copy(9, part(yn, 1), yn, 1, mate))
    arrived(2, xn, 1)
    go(copy(10, part(xn, 1), xn, 1, mate))
    arrived(3, yn, 0)
    go(copy(11, part(yn, 0), yn, 0, mate))
    arrived(4, dn, 0)
    go(copy(12, part(dn, 0), dn, 0, mate))
    arrived(5, dn, 1)
    go(copy(13, part(dn, 1), dn, 1, mate))
    across = lambda block: block + mate - me
    for i, block, h in (
        (6, me, 0), (7, me, 1), (8, xn, 0), (9, yn, 1),
        (10, xn, 1), (11, yn, 0), (12, dn, 0), (13, dn, 1),
    ):
        arrived(i, across(block), h)
    for c in started:
        c.wait_send()
    here.wait()


def gather_col(x, collective_id):
    n = lax.axis_size("col")
    rows, width = x.shape
    if n != 8 or rows % 32:
        return lax.all_gather(x, "col", axis=0, tiled=True)
    return pl.pallas_call(
        gather_kernel,
        out_shape=jax.ShapeDtypeStruct((n * rows, width), x.dtype),
        in_specs=[pl.BlockSpec(memory_space=pltpu.VMEM)],
        out_specs=pl.BlockSpec(memory_space=pltpu.VMEM),
        scratch_shapes=[
            pltpu.SemaphoreType.DMA((14,)),
            pltpu.SemaphoreType.DMA((14,)),
            pltpu.SemaphoreType.DMA,
        ],
        compiler_params=pltpu.CompilerParams(
            collective_id=collective_id, has_side_effects=True, vmem_limit_bytes=24 << 20
        ),
        cost_estimate=pl.CostEstimate(
            flops=10**10, bytes_accessed=2 * n * rows * width, transcendentals=0
        ),
        name="gather_col",
    )(x)


def scatter_kernel(x_ref, o_ref, mated, sums, relay, landed, send, recv):
    rows = o_ref.shape[0]
    half = rows // 2
    me, mate, xn, yn, dn = neighbours()
    greet((mate, xn, yn))
    shift = mate - me
    targets = (dn, xn, yn, me)

    def copy(i, src, dst, to):
        return pltpu.make_async_remote_copy(
            src_ref=src, dst_ref=dst, send_sem=send.at[i], recv_sem=recv.at[i],
            device_id={"col": to}, device_id_type=MESH,
        )

    def block(j):
        return pl.ds(pl.multiple_of(j * rows, rows), rows)

    started = []

    def go(c):
        c.start()
        started.append(c)

    for k, target in enumerate(targets):
        go(copy(k, x_ref.at[block(target + shift)], mated.at[k], mate))

    def mine(k, h):
        rows_h = pl.ds(pl.multiple_of(targets[k] * rows + h * half, half), half)
        return x_ref[rows_h, :].astype(jnp.float32) + mated[k, pl.ds(h * half, half), :].astype(
            jnp.float32
        )

    def put(k, h, value):
        sums[k, pl.ds(h * half, half), :] = value.astype(jnp.bfloat16)

    def of(ref, k, h):
        return ref.at[k, pl.ds(h * half, half)]

    started[0].wait_recv()
    put(0, 0, mine(0, 0))
    go(copy(4, of(sums, 0, 0), relay.at[0], xn))
    put(0, 1, mine(0, 1))
    go(copy(5, of(sums, 0, 1), relay.at[1], yn))
    started[1].wait_recv()
    put(1, 0, mine(1, 0))
    go(copy(6, of(sums, 1, 0), of(landed, 0, 0), xn))
    started[2].wait_recv()
    put(2, 1, mine(2, 1))
    go(copy(7, of(sums, 2, 1), of(landed, 1, 1), yn))
    started[4].wait_recv()
    put(2, 0, mine(2, 0) + relay[0].astype(jnp.float32))
    go(copy(8, of(sums, 2, 0), of(landed, 1, 0), yn))
    started[5].wait_recv()
    put(1, 1, mine(1, 1) + relay[1].astype(jnp.float32))
    go(copy(9, of(sums, 1, 1), of(landed, 0, 1), xn))
    started[3].wait_recv()
    for i in (6, 7, 8, 9):
        started[i].wait_recv()
    for h in (0, 1):
        lines = pl.ds(h * half, half)
        o_ref[lines, :] = (
            mine(3, h)
            + landed[0, lines, :].astype(jnp.float32)
            + landed[1, lines, :].astype(jnp.float32)
        )
    for c in started:
        c.wait_send()


def scatter_col(x, collective_id):
    n = lax.axis_size("col")
    rows, width = x.shape[0] // n, x.shape[1]
    if n != 8 or rows % 32:
        return lax.psum_scatter(x, "col", scatter_dimension=0, tiled=True).astype(jnp.float32)
    return pl.pallas_call(
        scatter_kernel,
        out_shape=jax.ShapeDtypeStruct((rows, width), jnp.float32),
        in_specs=[pl.BlockSpec(memory_space=pltpu.VMEM)],
        out_specs=pl.BlockSpec(memory_space=pltpu.VMEM),
        scratch_shapes=[
            pltpu.VMEM((4, rows, width), x.dtype),
            pltpu.VMEM((3, rows, width), x.dtype),
            pltpu.VMEM((2, rows // 2, width), x.dtype),
            pltpu.VMEM((2, rows, width), x.dtype),
            pltpu.SemaphoreType.DMA((10,)),
            pltpu.SemaphoreType.DMA((10,)),
        ],
        compiler_params=pltpu.CompilerParams(
            collective_id=collective_id, has_side_effects=True, vmem_limit_bytes=32 << 20
        ),
        cost_estimate=pl.CostEstimate(
            flops=10**10, bytes_accessed=2 * n * rows * width, transcendentals=0
        ),
        name="scatter_col",
    )(x)


def gather_row(weight, axis):
    n = lax.axis_size("row")
    me = lax.axis_index("row")
    depth = weight.shape[axis]
    shape = list(weight.shape)
    shape[axis] *= n
    whole = jnp.zeros(shape, weight.dtype)
    for step in range(n):
        block = weight
        if step:
            block = lax.ppermute(weight, "row", [((i + step) % n, i) for i in range(n)])
        whole = lax.dynamic_update_slice_in_dim(whole, block, ((me + step) % n) * depth, axis)
    return whole


def cube_gather_col(x):
    n = lax.axis_size("col")
    if n != 8:
        return lax.all_gather(x, "col", axis=0, tiled=True)
    me = lax.axis_index("col")
    x = x[None]
    for bit, after in ((2, 1), (4, 2), (1, 4)):
        other = lax.ppermute(x, "col", [(i, i ^ bit) for i in range(n)])
        low = (me // bit) % 2 == 0
        first, second = jnp.where(low, x, other), jnp.where(low, other, x)
        x = jnp.concatenate([first, second], axis=0) if bit != 1 else jnp.stack([first, second], 1)
    return x.reshape(-1, x.shape[-1])


def norm_local(values, gain, bias):
    mean = jnp.mean(values, axis=-1, keepdims=True)
    centred = values - mean
    var = jnp.mean(centred * centred, axis=-1, keepdims=True)
    return centred * lax.rsqrt(var + 1e-06) * gain.astype(jnp.float32) + bias.astype(jnp.float32)


def attend_kernel(heads, size, padded, q_ref, kv_ref, o_ref):
    outs = []
    for head in range(heads):
        base = head * 3 * padded
        query = q_ref[:, base : base + padded]
        keys = kv_ref[:, base + padded : base + 2 * padded]
        values = kv_ref[:, base + 2 * padded : base + 3 * padded]
        scores = lax.dot_general(
            query, keys, (((1,), (1,)), ((), ())), preferred_element_type=jnp.float32
        )
        top = jnp.max(scores, axis=-1, keepdims=True)
        expo = jnp.exp2(scores - top).astype(jnp.bfloat16)
        mixed = jnp.dot(expo, values, preferred_element_type=jnp.float32)
        outs.append(mixed[:, :size] / mixed[:, size : size + 1])
    o_ref[...] = jnp.concatenate(outs, axis=1).astype(o_ref.dtype)


def attend(qkv, heads, size, padded):
    length, width = qkv.shape
    block = min(256, length)
    return pl.pallas_call(
        functools.partial(attend_kernel, heads, size, padded),
        grid=(length // block,),
        in_specs=[
            pl.BlockSpec((block, width), lambda i: (i, 0)),
            pl.BlockSpec((length, width), lambda i: (0, 0)),
        ],
        out_specs=pl.BlockSpec((block, heads * size), lambda i: (i, 0)),
        out_shape=jax.ShapeDtypeStruct((length, heads * size), jnp.bfloat16),
        compiler_params=pltpu.CompilerParams(vmem_limit_bytes=40 << 20),
        cost_estimate=pl.CostEstimate(
            flops=4 * heads * length * length * padded * 8,
            bytes_accessed=4 * length * width,
            transcendentals=heads * length * length,
        ),
        name="attend",
    )(qkv, qkv)


def project_back(left, right):
    return lax.dot_general(
        left, right, (((1,), (1,)), ((), ())), preferred_element_type=jnp.float32
    )


def fast_plan(heads, own_rows, features, qkv_width, proj_rows, hidden):
    if lax.axis_size("col") != 8 or lax.axis_size("row") != 4:
        return None
    quarter = features // 4
    size = qkv_width // (3 * heads)
    whole = qkv_width // LANES * LANES
    rest = qkv_width - whole
    ok = (
        hidden == 3 * heads * LANES and own_rows % 128 == 0 and features % LANES == 0 and quarter % 32 == 0
        and hidden % LANES == 0 and 0 < rest and proj_rows == heads * size
        and proj_rows % 16 == 0 and 0 < proj_rows - LANES <= LANES // 2
        and 8 * proj_rows == features and size < LANES and whole // size == 3 * heads - 1
    )
    if not ok:
        return None
    first = 2 * quarter // LANES * LANES
    last = -(-quarter // LANES) * LANES
    middle = features - first - last
    if middle <= LANES or last <= LANES or features - last > 3 * quarter:
        return None
    if (first + middle - LANES - 2 * quarter) % 32:
        return None
    return dict(
        heads=heads, size=size, rows=own_rows, features=features, quarter=quarter, whole=whole,
        rest=rest, proj_rows=proj_rows, hidden=hidden,
        pieces=(first, middle - LANES, LANES, last - LANES, LANES),
        early=first + middle - LANES - 2 * quarter,
    )


def layer_kernel(
    plan, tok_in, g1, c1, qb, pb, g2, c2, d1, d2, wq_in, wp, w1, w2, o_ref,
    tok, wq, v1, v2, v3, v4, v5, v6, v7, v8,
    vec, x1, x2, qmain, qrest, qwide, qrow, qkv, ctx, heads_out, tails_out, heads_in, tails_in, pfull, f1, f2, resid,
    mated, sums, relay, landed,
    lsem, zsend, zrecv, gsend, grecv, psend, precv, asend, arecv, ssend, srecv,
):
    heads, size, rows = plan["heads"], plan["size"], plan["rows"]
    features, quarter = plan["features"], plan["quarter"]
    whole, rest, prows = plan["whole"], plan["rest"], plan["proj_rows"]
    hidden, pieces = plan["hidden"], plan["pieces"]
    half = rows // 2
    groups = 3 * heads
    f32, bf16 = jnp.float32, jnp.bfloat16
    hid, part = qkv, x1

    row = lax.axis_index("row")
    me, mate, xn, yn, dn = neighbours()
    shift = mate - me
    pair = row // 2
    near = row + 1 - 2 * (row % 2)
    other = 2 - pair
    far = 3 - 3 * pair
    middle = jnp.logical_or(row == 1, row == 2)
    end = jnp.logical_or(row == 0, row == 3)
    lo = 2 * pair
    hi = 2 - lo

    def flipped(mask):
        bits = [(me % 2 + mask % 2) % 2, (me // 2 % 2 + mask // 2 % 2) % 2, (me // 4 + mask // 4) % 2]
        return bits[0] + 2 * bits[1] + 4 * bits[2]

    barrier = pltpu.get_barrier_semaphore()
    for step in range(1, 6):
        pl.semaphore_signal(
            barrier, inc=1, device_id={"col": flipped(step)}, device_id_type=MESH
        )
    pl.semaphore_signal(barrier, inc=1, device_id={"row": near}, device_id_type=MESH)

    @pl.when(middle)
    def _():
        pl.semaphore_signal(barrier, inc=1, device_id={"row": other}, device_id_type=MESH)


    def load(i, src, dst):
        return pltpu.make_async_copy(src, dst, lsem.at[i])

    def remote(src, dst, ssem, rsem, **to):
        return pltpu.make_async_remote_copy(
            src_ref=src, dst_ref=dst, send_sem=ssem, recv_sem=rsem,
            device_id=to, device_id_type=MESH,
        )

    def lines(b, n=rows):
        return pl.ds(pl.multiple_of(b * n, n), n)

    early = plan["early"]

    def cut(w, b):
        low = b // 2
        return {
            5: (1 - low) * LANES,
            6: low * (quarter - LANES),
            7: (1 - low) * (quarter - early),
            8: low * early,
        }[w]

    def length_of(w):
        return {5: quarter - LANES, 6: LANES, 7: early, 8: quarter - early}[w]

    def place(w, b):
        if w == 0:
            return qmain.at[lines(b, quarter)]
        if w == 1:
            return qrest.at[b]
        if w == 2:
            return pfull.at[b, lines(me, prows)]
        if w == 3:
            return f1.at[lines(b, quarter)]
        if w == 4:
            return f2.at[lines(b, quarter)]
        return f2.at[pl.ds(pl.multiple_of(b * quarter + cut(w, b), 32), length_of(w))]

    def source(w):
        if w == 0:
            return place(0, row)
        return (None, qrest.at[row], wp, w1, w2)[w]

    zwhich = (0, 1, 1, 2, 2)

    def zslot(w, which):
        return w * 3 + which if w < 5 else 10 + w

    def z_copy(w, s, b):
        return remote(
            place(w, b), place(w, b), zsend.at[min(w, 3) * 5 + s], zrecv.at[zslot(w, zwhich[s])],
            row=other if s in (1, 4) else near,
        )

    def own_copy(w, s):
        return remote(
            source(w), place(w, row), zsend.at[min(w, 3) * 5 + s], zrecv.at[zslot(w, zwhich[s])],
            row=other if s == 1 else near,
        )

    def z_wait(w, which):
        z_copy(w, (0, 2, 3)[which], (near, other, far)[which]).wait_recv()

    def z_forward(w, s):
        which = {2: 1, 3: 2, 4: 0}[s]
        z_wait(w, which)
        z_copy(w, s, (near, other, far)[which]).start()

    def z_sent(s):
        for w in (0, 1, 2):
            z_copy(w, s, row).wait_send()
        both = f1.at[pl.ds(0, 2 * quarter)]
        remote(both, both, zsend.at[15 + s], zrecv.at[0], row=near).wait_send()

    loads = [load(0, wq_in, wq), load(1, tok_in, tok)]
    for i, (src, dst) in enumerate(
        ((g1, v1), (c1, v2), (g2, v3), (c2, v4), (pb, v5), (d2, v6), (qb, v7), (d1, v8))
    ):
        loads.append(load(i + 2, src, dst))
    loads.append(load(10, wp, place(2, row)))
    loads.append(load(11, w1, place(3, row)))
    loads.append(load(12, w2, place(4, row)))
    for c in loads:
        c.start()
    loads[0].wait()
    turned = wq[...].astype(f32).T.astype(bf16)
    qmain[lines(row, quarter), :] = turned[:, :whole]
    for j in range(quarter // 32):
        qrest[row, :, j * rest : (j + 1) * rest] = turned[32 * j : 32 * (j + 1), whole:]
    pl.semaphore_wait(barrier, 6 + row * (3 - row) // 2)
    for w in (0, 1, 2):
        own_copy(w, 0).start()

    @pl.when(middle)
    def _():
        for w in (0, 1, 2):
            own_copy(w, 1).start()

    @pl.when(end)
    def _():
        for w in (3, 4):
            own_copy(w, 0).start()

    for i, v in enumerate((v1, v2, v3, v4, v5, v6, v7, v8)):
        loads[i + 2].wait()
        vec[i : i + 1, : v.shape[0]] = v[...].astype(f32).reshape(1, -1)
    loads[1].wait()

    def norm(values, g, b):
        mean = jnp.mean(values, axis=-1, keepdims=True)
        centred = values - mean
        var = jnp.mean(centred * centred, axis=-1, keepdims=True)
        return centred * lax.rsqrt(var + 1e-06) * vec[g : g + 1, :] + vec[b : b + 1, :]

    chunk = 32

    def norm1(i):
        at = pl.ds(pl.multiple_of(i * chunk, chunk), chunk)
        to = pl.ds(pl.multiple_of(me * rows + i * chunk, chunk), chunk)
        x1[to, :] = norm(tok[at, :].astype(f32), 0, 1).astype(bf16)

    some = half // chunk // 2

    def two_steps(body, gather):
        for part in (0, 1):
            def step(t, c):
                body(t % some + t // some * 2 * some + part * some)
                return c

            lax.fori_loop(0, 2 * some, step, 0)
            gather.start(part)

    class Gather:
        wait_on = (0, 1, 2, 2, 3, 3, 4, 4, 5, 5, 5, 5, 6, 6)

        def __init__(self, x, gi):
            self.x, self.gi = x, gi

        def copy(self, i, block, h, to):
            at = self.x.at[pl.ds(pl.multiple_of(block * rows + h * half, half), half)]
            return remote(
                at, at, gsend.at[self.gi], grecv.at[self.gi, self.wait_on[i]], col=to
            )

        def arrived(self, i, count):
            at = self.x.at[pl.ds(0, count * half)]
            remote(at, at, gsend.at[self.gi], grecv.at[self.gi, i], col=mate).wait_recv()

        def start(self, part):
            for i, to in ((0, xn), (1, yn)):
                at = self.x.at[
                    pl.ds(pl.multiple_of(me * rows + i * half + part * half // 2, half // 2), half // 2)
                ]
                remote(at, at, gsend.at[self.gi], grecv.at[self.gi, i], col=to).start()
            if part:
                for i, h, to in ((2, 1, xn), (3, 0, yn), (6, 0, mate), (7, 1, mate)):
                    self.copy(i, me, h, to).start()

        def event0(self):
            self.arrived(0, 1)
            self.copy(4, xn, 0, yn).start()
            self.copy(8, xn, 0, mate).start()
            self.arrived(1, 1)
            self.copy(5, yn, 1, xn).start()
            self.copy(9, yn, 1, mate).start()

        def event1(self):
            self.arrived(2, 2)
            self.copy(10, xn, 1, mate).start()
            self.copy(11, yn, 0, mate).start()

        def event2(self):
            self.arrived(3, 2)
            self.copy(12, dn, 0, mate).start()
            self.copy(13, dn, 1, mate).start()

        def mate0(self):
            self.arrived(4, 2)

        def mate1(self):
            self.arrived(5, 4)

        def mate2(self):
            self.arrived(6, 2)

        def finish(self):
            at = self.x.at[pl.ds(0, 14 * half)]
            remote(at, at, gsend.at[self.gi], grecv.at[self.gi, 0], col=mate).wait_send()

    first = Gather(x1, 0)
    two_steps(norm1, first)
    qrow[...] = jnp.zeros_like(qrow)
    for g in range(groups):
        qrow[:, g * LANES : g * LANES + size] = vec[6:7, g * size : (g + 1) * size]
    lane = lax.broadcasted_iota(jnp.int32, (1, LANES), 1)
    for head in range(heads):
        at = slice((3 * head + 2) * LANES, (3 * head + 3) * LANES)
        qrow[:, at] = jnp.where(lane == size, 1.0, qrow[:, at])
    for c in loads[10:]:
        c.wait()

    spare = jnp.zeros((quarter, LANES - size), bf16)
    few = jnp.zeros((32, LANES - size), bf16)

    def widen(b):
        base = b * quarter
        at = pl.ds(pl.multiple_of(base, 32), quarter)
        for g in range(groups - 1):
            qwide[at, g * LANES : (g + 1) * LANES] = jnp.concatenate(
                [qmain[at, g * size : (g + 1) * size], spare], axis=1
            )
        for j in range(quarter // 32):
            some = pl.ds(pl.multiple_of(base + 32 * j, 32), 32)
            qwide[some, (groups - 1) * LANES :] = jnp.concatenate(
                [qmain[some, (groups - 1) * size :], qrest[b, :, j * rest : (j + 1) * rest], few],
                axis=1,
            )

    widen(row)

    def q_wait(b):
        z_wait(0, b)
        z_wait(1, b)

    @pl.when(middle)
    def _():
        for w in (0, 1):
            z_forward(w, 4)
        for w in (0, 1):
            z_forward(w, 2)

    first.event0()

    @pl.when(end)
    def _():
        q_wait(0)

    widen(near)

    @pl.when(middle)
    def _():
        z_forward(2, 2)
        z_forward(2, 4)
        own_copy(3, 1).start()
        for w in (0, 1):
            z_forward(w, 3)

    first.event1()

    p_on = (0, 1, 4, 2, 3, 4, 4, 4, 4)

    def pcopy(i, r, at, count, block, to):
        ref = pfull.at[pl.ds(at, count), lines(block, prows)]
        return remote(ref, ref, psend.at[r], precv.at[r, p_on[i]], col=to)

    def punits(r, i, count):
        ref = pfull.at[pl.ds(0, 2), pl.ds(0, count // 2 * prows)]
        return remote(ref, ref, psend.at[r], precv.at[r, i], col=mate)

    def p_start(r, at):
        pcopy(0, r, at, 2, me, xn).start()
        pcopy(1, r, at, 2, me, yn).start()
        pcopy(2, r, at, 2, me, mate).start()

    def p_forward(r, at):
        pcopy(0, r, at, 2, xn, xn).wait_recv()
        pcopy(3, r, at, 1, xn, yn).start()
        pcopy(5, r, at, 2, xn, mate).start()
        pcopy(1, r, at, 2, yn, yn).wait_recv()
        pcopy(4, r, at + 1, 1, yn, xn).start()
        pcopy(6, r, at, 2, yn, mate).start()

    def p_last(r, at):
        pcopy(3, r, at, 1, dn, yn).wait_recv()
        pcopy(7, r, at, 1, dn, mate).start()
        pcopy(4, r, at + 1, 1, dn, xn).wait_recv()
        pcopy(8, r, at + 1, 1, dn, mate).start()

    def p_mates(r):
        punits(r, 4, 8).wait_recv()

    def p_finish(r):
        punits(r, 0, 14).wait_send()


    @pl.when(end)
    def _():
        z_wait(2, 0)

    p_start(0, lo)

    @pl.when(middle)
    def _():
        z_forward(2, 3)
        p_start(1, hi)
        own_copy(3, 0).start()
        z_forward(3, 4)
        own_copy(4, 1).start()

    first.event2()
    first.mate0()

    @pl.when(end)
    def _():
        q_wait(1)
        q_wait(2)

    widen(other)
    widen(far)
    first.mate1()
    first.mate2()

    factor = 1.4426950408889634 / size**0.5

    def qkv_block(i, c):
        @pl.when(jnp.logical_or(jnp.logical_and(i == 1, end), jnp.logical_and(i == 2, middle)))
        def _():
            p_forward(0, lo)

        @pl.when(jnp.logical_and(i == 2, end))
        def _():
            z_wait(2, 1)
            z_wait(2, 2)
            p_start(1, hi)

        at = lines(flipped(2 * i) // 2, 2 * rows)
        product = jnp.dot(x1[at, :], qwide[...], preferred_element_type=f32) + qrow[...]
        for g in range(groups):
            cols = slice(g * LANES, (g + 1) * LANES)
            value = product[:, cols]
            qkv[at, cols] = (value * factor if g % 3 == 0 else value).astype(bf16)
        return c

    lax.fori_loop(0, 4, qkv_block, 0)

    rest_lanes = prows - LANES

    def a_all(which):
        ref = (heads_in, tails_in)[which].at[pl.ds(0, 7)]
        return remote(ref, ref, asend.at[which], arecv.at[which], col=mate)

    def a_copies(i, core, to):
        at = lines(core)
        tail = pl.ds(pl.multiple_of(core * half, half), half)
        return (
            remote(
                heads_out.at[i, at], heads_in.at[me], asend.at[0], arecv.at[0], col=to
            ),
            remote(
                tails_out.at[i, tail], tails_in.at[me], asend.at[1], arecv.at[1], col=to
            ),
        )

    def attend_block(i, c):
        @pl.when(jnp.logical_and(i == 1, middle))
        def _():
            z_forward(3, 2)
            z_forward(4, 4)

        @pl.when(i == 2)
        def _():
            p_last(0, lo)
            p_forward(1, hi)

        chip = flipped(6 - 2 * i) // 2
        at = lines(chip, 2 * rows)
        scores = []
        for head in range(heads):
            base = head * 3 * LANES
            scores.append(
                lax.dot_general(
                    qkv[at, base : base + LANES], qkv[:, base + LANES : base + 2 * LANES],
                    (((1,), (1,)), ((), ())), preferred_element_type=f32,
                )
            )
        expos = [
            jnp.exp2(x - jnp.max(x, axis=-1, keepdims=True)).astype(bf16) for x in scores
        ]
        outs = []
        for head in range(heads):
            base = (head * 3 + 2) * LANES
            mixed = jnp.dot(
                expos[head], qkv[:, base : base + LANES], preferred_element_type=f32
            )
            outs.append(mixed[:, :size] / mixed[:, size : size + 1])
        mixed = jnp.concatenate(outs, axis=1).astype(bf16)
        gap = jnp.zeros((half, LANES // 2 - rest_lanes), bf16)
        heads_out[i] = mixed[:, :LANES]
        for core in (0, 1):
            top, low = (
                mixed[core * rows + h * half : core * rows + (h + 1) * half, LANES:]
                for h in (0, 1)
            )
            tails_out[i, core * half : (core + 1) * half, :] = jnp.concatenate(
                [top, gap, low, gap], axis=1
            )
        for core in (0, 1):
            to = 2 * chip + core

            @pl.when(to != me)
            def _():
                for c in a_copies(i, core, to):
                    c.start()

        return c

    lax.fori_loop(0, 4, attend_block, 0)
    @pl.when(middle)
    def _():
        z_forward(3, 3)
        own_copy(4, 0).start()

    p_last(1, hi)
    first.finish()
    heads_in[me] = heads_out[3, lines(me % 2), :]
    tails_in[me] = tails_out[3, lines(me % 2, half), :]
    p_mates(0)
    p_mates(1)
    a_all(0).wait_recv()
    a_all(1).wait_recv()
    for d in range(8):
        base = d * prows
        ctx[:, base : base + LANES] = heads_in[d]
        for h in (0, 1):
            ctx[h * half : (h + 1) * half, base + LANES : base + prows] = tails_in[
                d, :, h * (LANES // 2) : h * (LANES // 2) + rest_lanes
            ]

    for b in range(4):
        resid[:, b * quarter : (b + 1) * quarter] = jnp.dot(
            ctx[...], pfull[b], preferred_element_type=f32
        )

    def norm2(i):
        at = pl.ds(pl.multiple_of(i * chunk, chunk), chunk)
        to = pl.ds(pl.multiple_of(me * rows + i * chunk, chunk), chunk)
        value = tok[at, :].astype(f32) + resid[at, :] + vec[4:5, :]
        resid[at, :] = value
        x2[to, :] = norm(value, 2, 3).astype(bf16)

    second = Gather(x2, 1)
    two_steps(norm2, second)
    second.event0()

    @pl.when(end)
    def _():
        z_wait(3, 0)
        z_wait(3, 1)
        z_wait(3, 2)

    starts, done = [], 0
    for width in pieces:
        starts.append(done + (features - width - 2 * done) * pair)
        done += width
    targets = (dn, yn, xn, me)

    class Piece:
        def __init__(self, p):
            self.p, self.width = p, pieces[p]
            self.cols = pl.ds(pl.multiple_of(starts[p], LANES), pieces[p])

        def copy(self, i, src, dst, to):
            return remote(
                src, dst, ssend.at[self.p, min(i // 4, 1)], srecv.at[self.p, min(i, 6)], col=to
            )

        def of(self, ref, k, h):
            return ref.at[k, pl.ds(h * half, half), self.cols]

        def to_mate(self, k):
            block = flipped(6 - 2 * k + 1)
            return remote(
                part.at[lines(block), self.cols], mated.at[k, :, self.cols],
                ssend.at[self.p, 0], srecv.at[self.p, k], col=mate,
            )

        def compute(self, k):
            at = lines(flipped(6 - 2 * k) // 2, 2 * rows)
            part[at, self.cols] = project_back(hid[at, :], f2[self.cols, :]).astype(bf16)
            self.to_mate(k).start()

        def compute_all(self):
            def body(k, c):
                self.compute(k)
                return c

            lax.fori_loop(0, 4, body, 0)

        def mine(self, k, h):
            at = pl.ds(pl.multiple_of(targets[k] * rows + h * half, half), half)
            return part[at, self.cols].astype(f32) + mated[
                k, h * half : (h + 1) * half, self.cols
            ].astype(f32)

        def put(self, k, h, value):
            sums[k, h * half : (h + 1) * half, self.cols] = value.astype(bf16)

        def relays(self, h):
            return relay.at[h, :, self.cols]

        def c(self, i):
            k, h, dst, to = {
                4: (0, 0, self.relays(0), xn),
                5: (0, 1, self.relays(1), yn),
                6: (2, 0, self.of(landed, 0, 0), xn),
                7: (1, 1, self.of(landed, 1, 1), yn),
                8: (1, 0, self.of(landed, 1, 0), yn),
                9: (2, 1, self.of(landed, 0, 1), xn),
            }[i]
            return self.copy(i, self.of(sums, k, h), dst, to)

        def direct(self, k):
            h = {1: 1, 2: 0}[k]
            self.to_mate(k).wait_recv()
            self.put(k, h, self.mine(k, h))
            self.c({1: 7, 2: 6}[k]).start()

        def open_relayed(self):
            self.to_mate(0).wait_recv()
            self.put(0, 0, self.mine(0, 0))
            self.c(4).start()
            self.put(0, 1, self.mine(0, 1))
            self.c(5).start()

        def pass_on(self):
            self.c(4).wait_recv()
            self.put(1, 0, self.mine(1, 0) + relay[0, :, self.cols].astype(f32))
            self.c(8).start()
            self.c(5).wait_recv()
            self.put(2, 1, self.mine(2, 1) + relay[1, :, self.cols].astype(f32))
            self.c(9).start()

        def close(self):
            self.to_mate(3).wait_recv()
            ref = landed.at[:, :, self.cols]
            self.copy(6, ref, ref, mate).wait_recv()
            for h in (0, 1):
                at = slice(h * half, (h + 1) * half)
                total = (
                    self.mine(3, h)
                    + landed[0, at, self.cols].astype(f32)
                    + landed[1, at, self.cols].astype(f32)
                )
                value = resid[at, self.cols] + total + vec[5:6, self.cols]
                o_ref[at, self.cols] = value.astype(bf16)

        def finish(self):
            ref = mated.at[:, :, self.cols]
            self.copy(0, ref, ref, mate).wait_send()
            ref = sums.at[:, :, self.cols]
            self.copy(6, ref, ref, mate).wait_send()

    one, two, after, three, four = (Piece(p) for p in range(5))

    def fc1_block(i, c):
        @pl.when(i == 0)
        def _():
            second.mate0()

        @pl.when(i == 1)
        def _():
            second.event1()

        @pl.when(jnp.logical_and(i == 1, middle))
        def _():
            z_wait(4, 1)
            z_copy(7, 2, other).start()
            z_copy(8, 2, other).start()

        @pl.when(i == 1)
        def _():
            second.mate1()

        @pl.when(i == 3)
        def _():
            second.event2()

        @pl.when(jnp.logical_and(i == 3, middle))
        def _():
            z_wait(4, 2)
            z_copy(5, 3, far).start()
            z_copy(6, 3, far).start()

        @pl.when(i == 3)
        def _():
            one.direct(1)
            second.mate2()

        at = lines(flipped(2 * i) // 2, 2 * rows)
        for c0 in range(0, hidden, 2 * LANES):
            cols = slice(c0, c0 + 2 * LANES)
            value = jnp.dot(x2[at, :], f1[:, cols], preferred_element_type=f32) + vec[7:8, cols]
            hid[at, cols] = (
                0.5 * value * (1.0 + lax.erf(value * 0.7071067811865476))
            ).astype(bf16)

        @pl.when(jnp.logical_and(i == 1, end))
        def _():
            z_wait(4, 0)

        @pl.when(i == 2)
        def _():
            one.direct(2)

        @pl.when(i > 0)
        def _():
            one.compute(3 - i)

        return c

    lax.fori_loop(0, 4, fc1_block, 0)

    def open_all(piece):
        piece.open_relayed()
        piece.direct(2)
        piece.direct(1)

    one.compute(3)
    one.open_relayed()

    @pl.when(end)
    def _():
        z_wait(7, 1)

    two.compute_all()
    open_all(two)
    one.pass_on()

    @pl.when(end)
    def _():
        z_wait(8, 1)

    after.compute_all()
    open_all(after)
    two.pass_on()

    @pl.when(end)
    def _():
        z_wait(5, 2)

    three.compute_all()
    open_all(three)
    after.pass_on()

    @pl.when(end)
    def _():
        z_wait(6, 2)

    four.compute_all()
    open_all(four)
    three.pass_on()
    one.close()
    four.pass_on()
    two.close()
    after.close()
    three.close()
    four.close()

    for piece in (one, two, after, three, four):
        piece.finish()
    second.finish()
    p_finish(0)
    p_finish(1)
    a_all(0).wait_send()
    a_all(1).wait_send()
    z_sent(0)

    @pl.when(middle)
    def _():
        for way in range(1, 5):
            z_sent(way)


def layer_call(plan, *arrays):
    rows, features, quarter = plan["rows"], plan["features"], plan["quarter"]
    hidden = plan["hidden"]
    wide = 3 * plan["heads"] * LANES
    length = 8 * rows
    bf16, f32 = jnp.bfloat16, jnp.float32
    dma = pltpu.SemaphoreType.DMA
    return pl.pallas_call(
        functools.partial(layer_kernel, plan),
        out_shape=pltpu.VMEM((rows, features), bf16),
        in_specs=[pl.BlockSpec(memory_space=pl.ANY)] * 13,
        out_specs=pl.BlockSpec(memory_space=pltpu.VMEM),
        scratch_shapes=[
            pltpu.VMEM((rows, features), bf16),
            pltpu.VMEM(arrays[9].shape, bf16),
            *(pltpu.VMEM(arrays[i].shape, bf16) for i in (1, 2, 5, 6, 4, 8, 3, 7)),
            pltpu.VMEM((8, features), f32),
            pltpu.VMEM((length, features), bf16),
            pltpu.VMEM((length, features), bf16),
            pltpu.VMEM((features, plan["whole"]), bf16),
            pltpu.VMEM((4, 32, quarter // 32 * plan["rest"]), bf16),
            pltpu.VMEM((features, wide), bf16),
            pltpu.VMEM((1, wide), f32),
            pltpu.VMEM((length, wide), bf16),
            pltpu.VMEM((rows, features), bf16),
            pltpu.VMEM((4, 2 * rows, LANES), bf16),
            pltpu.VMEM((4, rows, LANES), bf16),
            pltpu.VMEM((8, rows, LANES), bf16),
            pltpu.VMEM((8, rows // 2, LANES), bf16),
            pltpu.VMEM((4, features, quarter), bf16),
            pltpu.VMEM((features, hidden), bf16),
            pltpu.VMEM((features, hidden), bf16),
            pltpu.VMEM((rows, features), f32),
            pltpu.VMEM((4, rows, features), bf16),
            pltpu.VMEM((3, rows, features), bf16),
            pltpu.VMEM((2, rows // 2, features), bf16),
            pltpu.VMEM((2, rows, features), bf16),
            dma((13,)),
            dma((20,)), dma((19,)),
            dma((2,)), dma((2, 7)),
            dma((2,)), dma((2, 5)),
            dma((2,)), dma((2,)),
            dma((5, 2)), dma((5, 7)),
        ],
        compiler_params=pltpu.CompilerParams(
            collective_id=3, has_side_effects=True, vmem_limit_bytes=60 * 1024 * 1024
        ),
        name="layer",
    )(*arrays)


def local(
    tokens_in,
    ln1_gain,
    ln1_bias,
    qkv_weight,
    qkv_bias,
    proj_weight,
    proj_bias,
    ln2_gain,
    ln2_bias,
    fc1_weight,
    fc1_bias,
    fc2_weight,
    fc2_bias,
):
    local_heads = HEADS // lax.axis_size("col")
    own_rows, features = tokens_in.shape
    size = qkv_weight.shape[1] // (3 * local_heads)
    padded = -(-(size + 1) // LANES) * LANES
    plan = fast_plan(
        local_heads, own_rows, features, qkv_weight.shape[1], proj_weight.shape[0],
        fc1_weight.shape[1],
    )
    if plan is not None:
        return layer_call(
            plan, tokens_in, ln1_gain, ln1_bias, qkv_bias, proj_bias, ln2_gain, ln2_bias, fc1_bias,
            fc2_bias, qkv_weight.T, proj_weight, fc1_weight, fc2_weight,
        )
    inputs = tokens_in.astype(jnp.float32)
    qkv_full = gather_row(qkv_weight, 0)
    proj_full = gather_row(proj_weight, 1)
    fc1_full = gather_row(fc1_weight, 0)
    fc2_full = gather_row(fc2_weight, 0)
    fc1_shift = fc1_bias.astype(jnp.float32)

    spare = padded - size
    qkv_wide = jnp.pad(
        qkv_full.reshape(features, local_heads, 3, size), ((0, 0), (0, 0), (0, 0), (0, spare))
    ).reshape(features, local_heads * 3 * padded)
    shift = jnp.pad(
        qkv_bias.astype(jnp.float32).reshape(local_heads, 3, size), ((0, 0), (0, 0), (0, spare))
    )
    shift = shift.at[:, 2, size].set(1.0).reshape(-1)
    scale = jnp.ones((local_heads, 3, padded), jnp.float32)
    scale = scale.at[:, 0].set(1.4426950408889634 / size**0.5).reshape(-1)

    ln1 = norm_local(inputs, ln1_gain, ln1_bias).astype(jnp.bfloat16)
    product = jnp.dot(gather_col(ln1, 0), qkv_wide, preferred_element_type=jnp.float32)
    qkv = ((product + shift) * scale).astype(jnp.bfloat16)
    attn = attend(qkv, local_heads, size, padded)
    proj_whole = cube_gather_col(proj_full)
    own_heads = lax.all_to_all(attn, "col", split_axis=0, concat_axis=1, tiled=True)
    attn_sum = jnp.dot(own_heads, proj_whole, preferred_element_type=jnp.float32)
    resid = inputs + attn_sum + proj_bias.astype(jnp.float32)
    ln2 = norm_local(resid, ln2_gain, ln2_bias).astype(jnp.bfloat16)
    product = jnp.dot(gather_col(ln2, 1), fc1_full, preferred_element_type=jnp.float32) + fc1_shift
    hidden = jax.nn.gelu(product, approximate=False).astype(jnp.bfloat16)
    mlp_sum = scatter_col(project_back(hidden, fc2_full).astype(jnp.bfloat16), 2)
    result = resid + mlp_sum + fc2_bias.astype(jnp.float32)
    return result.astype(jnp.bfloat16)


def solution(mesh):
    in_specs = (
        P(("row", "col"), None),
        P(),
        P(),
        P("row", "col"),
        P("col"),
        P("col", "row"),
        P(),
        P(),
        P(),
        P("row", "col"),
        P("col"),
        P("row", "col"),
        P(),
    )
    out_specs = P(("row", "col"), None)
    return jax.shard_map(local, mesh=mesh, in_specs=in_specs, out_specs=out_specs, check_vma=False)
```

```python
import functools

import jax
import jax.numpy as jnp
from jax import lax
from jax.experimental import pallas as pl
from jax.experimental.pallas import tpu as pltpu
from jax.sharding import PartitionSpec as P

HEADS = 16
LANES = 128
MESH = pl.DeviceIdType.MESH


def greet(peers):
    barrier = pltpu.get_barrier_semaphore()
    for peer in peers:
        pl.semaphore_signal(barrier, inc=1, device_id={"col": peer}, device_id_type=MESH)
    pl.semaphore_wait(barrier, len(peers))


def neighbours():
    me = lax.axis_index("col")
    core, x, y = me % 2, (me // 2) % 2, me // 4
    place = lambda y, x, core: y * 4 + x * 2 + core
    return (
        me,
        place(y, x, 1 - core),
        place(y, 1 - x, core),
        place(1 - y, x, core),
        place(1 - y, 1 - x, core),
    )


def gather_kernel(x_ref, o_ref, send, recv, local_sem):
    rows = x_ref.shape[0]
    half = rows // 2
    me, mate, xn, yn, dn = neighbours()
    greet((mate, xn, yn))

    def part(block, h):
        return o_ref.at[pl.ds(pl.multiple_of(block * rows + h * half, half), half)]

    def copy(i, src, block, h, to):
        return pltpu.make_async_remote_copy(
            src_ref=src, dst_ref=part(block, h), send_sem=send.at[i], recv_sem=recv.at[i],
            device_id={"col": to}, device_id_type=MESH,
        )

    def own(h):
        return x_ref.at[pl.ds(h * half, half)]

    def arrived(i, block, h):
        copy(i, own(0), block, h, mate).wait_recv()

    started = []

    def go(c):
        c.start()
        started.append(c)

    go(copy(0, own(0), me, 0, xn))
    go(copy(1, own(1), me, 1, yn))
    go(copy(2, own(1), me, 1, xn))
    go(copy(3, own(0), me, 0, yn))
    go(copy(6, own(0), me, 0, mate))
    go(copy(7, own(1), me, 1, mate))
    here = pltpu.make_async_copy(
        x_ref, o_ref.at[pl.ds(pl.multiple_of(me * rows, rows), rows)], local_sem
    )
    here.start()
    arrived(0, xn, 0)
    go(copy(4, part(xn, 0), xn, 0, yn))
    go(copy(8, part(xn, 0), xn, 0, mate))
    arrived(1, yn, 1)
    go(copy(5, part(yn, 1), yn, 1, xn))
    go(copy(9, part(yn, 1), yn, 1, mate))
    arrived(2, xn, 1)
    go(copy(10, part(xn, 1), xn, 1, mate))
    arrived(3, yn, 0)
    go(copy(11, part(yn, 0), yn, 0, mate))
    arrived(4, dn, 0)
    go(copy(12, part(dn, 0), dn, 0, mate))
    arrived(5, dn, 1)
    go(copy(13, part(dn, 1), dn, 1, mate))
    across = lambda block: block + mate - me
    for i, block, h in (
        (6, me, 0), (7, me, 1), (8, xn, 0), (9, yn, 1),
        (10, xn, 1), (11, yn, 0), (12, dn, 0), (13, dn, 1),
    ):
        arrived(i, across(block), h)
    for c in started:
        c.wait_send()
    here.wait()


def gather_col(x, collective_id):
    n = lax.axis_size("col")
    rows, width = x.shape
    if n != 8 or rows % 32:
        return lax.all_gather(x, "col", axis=0, tiled=True)
    return pl.pallas_call(
        gather_kernel,
        out_shape=jax.ShapeDtypeStruct((n * rows, width), x.dtype),
        in_specs=[pl.BlockSpec(memory_space=pltpu.VMEM)],
        out_specs=pl.BlockSpec(memory_space=pltpu.VMEM),
        scratch_shapes=[
            pltpu.SemaphoreType.DMA((14,)),
            pltpu.SemaphoreType.DMA((14,)),
            pltpu.SemaphoreType.DMA,
        ],
        compiler_params=pltpu.CompilerParams(
            collective_id=collective_id, has_side_effects=True, vmem_limit_bytes=24 << 20
        ),
        cost_estimate=pl.CostEstimate(
            flops=10**10, bytes_accessed=2 * n * rows * width, transcendentals=0
        ),
        name="gather_col",
    )(x)


def scatter_kernel(x_ref, o_ref, mated, sums, relay, landed, send, recv):
    rows = o_ref.shape[0]
    half = rows // 2
    me, mate, xn, yn, dn = neighbours()
    greet((mate, xn, yn))
    shift = mate - me
    targets = (dn, xn, yn, me)

    def copy(i, src, dst, to):
        return pltpu.make_async_remote_copy(
            src_ref=src, dst_ref=dst, send_sem=send.at[i], recv_sem=recv.at[i],
            device_id={"col": to}, device_id_type=MESH,
        )

    def block(j):
        return pl.ds(pl.multiple_of(j * rows, rows), rows)

    started = []

    def go(c):
        c.start()
        started.append(c)

    for k, target in enumerate(targets):
        go(copy(k, x_ref.at[block(target + shift)], mated.at[k], mate))

    def mine(k, h):
        rows_h = pl.ds(pl.multiple_of(targets[k] * rows + h * half, half), half)
        return x_ref[rows_h, :].astype(jnp.float32) + mated[k, pl.ds(h * half, half), :].astype(
            jnp.float32
        )

    def put(k, h, value):
        sums[k, pl.ds(h * half, half), :] = value.astype(jnp.bfloat16)

    def of(ref, k, h):
        return ref.at[k, pl.ds(h * half, half)]

    started[0].wait_recv()
    put(0, 0, mine(0, 0))
    go(copy(4, of(sums, 0, 0), relay.at[0], xn))
    put(0, 1, mine(0, 1))
    go(copy(5, of(sums, 0, 1), relay.at[1], yn))
    started[1].wait_recv()
    put(1, 0, mine(1, 0))
    go(copy(6, of(sums, 1, 0), of(landed, 0, 0), xn))
    started[2].wait_recv()
    put(2, 1, mine(2, 1))
    go(copy(7, of(sums, 2, 1), of(landed, 1, 1), yn))
    started[4].wait_recv()
    put(2, 0, mine(2, 0) + relay[0].astype(jnp.float32))
    go(copy(8, of(sums, 2, 0), of(landed, 1, 0), yn))
    started[5].wait_recv()
    put(1, 1, mine(1, 1) + relay[1].astype(jnp.float32))
    go(copy(9, of(sums, 1, 1), of(landed, 0, 1), xn))
    started[3].wait_recv()
    for i in (6, 7, 8, 9):
        started[i].wait_recv()
    for h in (0, 1):
        lines = pl.ds(h * half, half)
        o_ref[lines, :] = (
            mine(3, h)
            + landed[0, lines, :].astype(jnp.float32)
            + landed[1, lines, :].astype(jnp.float32)
        )
    for c in started:
        c.wait_send()


def scatter_col(x, collective_id):
    n = lax.axis_size("col")
    rows, width = x.shape[0] // n, x.shape[1]
    if n != 8 or rows % 32:
        return lax.psum_scatter(x, "col", scatter_dimension=0, tiled=True).astype(jnp.float32)
    return pl.pallas_call(
        scatter_kernel,
        out_shape=jax.ShapeDtypeStruct((rows, width), jnp.float32),
        in_specs=[pl.BlockSpec(memory_space=pltpu.VMEM)],
        out_specs=pl.BlockSpec(memory_space=pltpu.VMEM),
        scratch_shapes=[
            pltpu.VMEM((4, rows, width), x.dtype),
            pltpu.VMEM((3, rows, width), x.dtype),
            pltpu.VMEM((2, rows // 2, width), x.dtype),
            pltpu.VMEM((2, rows, width), x.dtype),
            pltpu.SemaphoreType.DMA((10,)),
            pltpu.SemaphoreType.DMA((10,)),
        ],
        compiler_params=pltpu.CompilerParams(
            collective_id=collective_id, has_side_effects=True, vmem_limit_bytes=32 << 20
        ),
        cost_estimate=pl.CostEstimate(
            flops=10**10, bytes_accessed=2 * n * rows * width, transcendentals=0
        ),
        name="scatter_col",
    )(x)


def gather_row(weight, axis):
    n = lax.axis_size("row")
    me = lax.axis_index("row")
    depth = weight.shape[axis]
    shape = list(weight.shape)
    shape[axis] *= n
    whole = jnp.zeros(shape, weight.dtype)
    for step in range(n):
        block = weight
        if step:
            block = lax.ppermute(weight, "row", [((i + step) % n, i) for i in range(n)])
        whole = lax.dynamic_update_slice_in_dim(whole, block, ((me + step) % n) * depth, axis)
    return whole


def cube_gather_col(x):
    n = lax.axis_size("col")
    if n != 8:
        return lax.all_gather(x, "col", axis=0, tiled=True)
    me = lax.axis_index("col")
    x = x[None]
    for bit, after in ((2, 1), (4, 2), (1, 4)):
        other = lax.ppermute(x, "col", [(i, i ^ bit) for i in range(n)])
        low = (me // bit) % 2 == 0
        first, second = jnp.where(low, x, other), jnp.where(low, other, x)
        x = jnp.concatenate([first, second], axis=0) if bit != 1 else jnp.stack([first, second], 1)
    return x.reshape(-1, x.shape[-1])


def norm_local(values, gain, bias):
    mean = jnp.mean(values, axis=-1, keepdims=True)
    centred = values - mean
    var = jnp.mean(centred * centred, axis=-1, keepdims=True)
    return centred * lax.rsqrt(var + 1e-06) * gain.astype(jnp.float32) + bias.astype(jnp.float32)


def attend_kernel(heads, size, padded, q_ref, kv_ref, o_ref):
    outs = []
    for head in range(heads):
        base = head * 3 * padded
        query = q_ref[:, base : base + padded]
        keys = kv_ref[:, base + padded : base + 2 * padded]
        values = kv_ref[:, base + 2 * padded : base + 3 * padded]
        scores = lax.dot_general(
            query, keys, (((1,), (1,)), ((), ())), preferred_element_type=jnp.float32
        )
        top = jnp.max(scores, axis=-1, keepdims=True)
        expo = jnp.exp2(scores - top).astype(jnp.bfloat16)
        mixed = jnp.dot(expo, values, preferred_element_type=jnp.float32)
        outs.append(mixed[:, :size] / mixed[:, size : size + 1])
    o_ref[...] = jnp.concatenate(outs, axis=1).astype(o_ref.dtype)


def attend(qkv, heads, size, padded):
    length, width = qkv.shape
    block = min(256, length)
    return pl.pallas_call(
        functools.partial(attend_kernel, heads, size, padded),
        grid=(length // block,),
        in_specs=[
            pl.BlockSpec((block, width), lambda i: (i, 0)),
            pl.BlockSpec((length, width), lambda i: (0, 0)),
        ],
        out_specs=pl.BlockSpec((block, heads * size), lambda i: (i, 0)),
        out_shape=jax.ShapeDtypeStruct((length, heads * size), jnp.bfloat16),
        compiler_params=pltpu.CompilerParams(vmem_limit_bytes=40 << 20),
        cost_estimate=pl.CostEstimate(
            flops=4 * heads * length * length * padded * 8,
            bytes_accessed=4 * length * width,
            transcendentals=heads * length * length,
        ),
        name="attend",
    )(qkv, qkv)


def project_back(left, right):
    return lax.dot_general(
        left, right, (((1,), (1,)), ((), ())), preferred_element_type=jnp.float32
    )


def fast_plan(heads, own_rows, features, qkv_width, proj_rows, hidden):
    if lax.axis_size("col") != 8 or lax.axis_size("row") != 4:
        return None
    quarter = features // 4
    size = qkv_width // (3 * heads)
    whole = qkv_width // LANES * LANES
    rest = qkv_width - whole
    ok = (
        hidden == 3 * heads * LANES and own_rows % 128 == 0 and features % LANES == 0 and quarter % 32 == 0
        and hidden % LANES == 0 and 0 < rest and proj_rows == heads * size
        and proj_rows % 16 == 0 and 0 < proj_rows - LANES <= LANES // 2
        and 8 * proj_rows == features and size < LANES and whole // size == 3 * heads - 1
    )
    if not ok:
        return None
    first = 2 * quarter // LANES * LANES
    last = -(-quarter // LANES) * LANES
    middle = features - first - last
    if middle <= LANES or last <= LANES or features - last > 3 * quarter:
        return None
    if (first + middle - LANES - 2 * quarter) % 32:
        return None
    return dict(
        heads=heads, size=size, rows=own_rows, features=features, quarter=quarter, whole=whole,
        rest=rest, proj_rows=proj_rows, hidden=hidden,
        pieces=(first, middle - LANES, LANES, last - LANES, LANES),
        early=first + middle - LANES - 2 * quarter,
    )


def layer_kernel(
    plan, tok_in, g1, c1, qb, pb, g2, c2, d1, d2, wq_in, wp, w1, w2, o_ref,
    tok, wq, v1, v2, v3, v4, v5, v6, v7, v8,
    vec, x1, x2, qmain, qrest, qwide, qrow, qkv, ctx, heads_out, tails_out, heads_in, tails_in, pfull, f1, f2, resid,
    mated, sums, relay, landed,
    lsem, zsend, zrecv, gsend, grecv, psend, precv, asend, arecv, ssend, srecv,
):
    heads, size, rows = plan["heads"], plan["size"], plan["rows"]
    features, quarter = plan["features"], plan["quarter"]
    whole, rest, prows = plan["whole"], plan["rest"], plan["proj_rows"]
    hidden, pieces = plan["hidden"], plan["pieces"]
    half = rows // 2
    groups = 3 * heads
    f32, bf16 = jnp.float32, jnp.bfloat16
    hid, part = qkv, x1

    row = lax.axis_index("row")
    me, mate, xn, yn, dn = neighbours()
    shift = mate - me
    pair = row // 2
    near = row + 1 - 2 * (row % 2)
    other = 2 - pair
    far = 3 - 3 * pair
    middle = jnp.logical_or(row == 1, row == 2)
    end = jnp.logical_or(row == 0, row == 3)
    lo = 2 * pair
    hi = 2 - lo

    def flipped(mask):
        bits = [(me % 2 + mask % 2) % 2, (me // 2 % 2 + mask // 2 % 2) % 2, (me // 4 + mask // 4) % 2]
        return bits[0] + 2 * bits[1] + 4 * bits[2]

    barrier = pltpu.get_barrier_semaphore()
    for step in range(1, 6):
        pl.semaphore_signal(
            barrier, inc=1, device_id={"col": flipped(step)}, device_id_type=MESH
        )
    pl.semaphore_signal(barrier, inc=1, device_id={"row": near}, device_id_type=MESH)

    @pl.when(middle)
    def _():
        pl.semaphore_signal(barrier, inc=1, device_id={"row": other}, device_id_type=MESH)


    def load(i, src, dst):
        return pltpu.make_async_copy(src, dst, lsem.at[i])

    def remote(src, dst, ssem, rsem, **to):
        return pltpu.make_async_remote_copy(
            src_ref=src, dst_ref=dst, send_sem=ssem, recv_sem=rsem,
            device_id=to, device_id_type=MESH,
        )

    def lines(b, n=rows):
        return pl.ds(pl.multiple_of(b * n, n), n)

    early = plan["early"]

    def cut(w, b):
        low = b // 2
        return {
            5: (1 - low) * LANES,
            6: low * (quarter - LANES),
            7: (1 - low) * (quarter - early),
            8: low * early,
        }[w]

    def length_of(w):
        return {5: quarter - LANES, 6: LANES, 7: early, 8: quarter - early}[w]

    def place(w, b):
        if w == 0:
            return qmain.at[lines(b, quarter)]
        if w == 1:
            return qrest.at[b]
        if w == 2:
            return pfull.at[b, lines(me, prows)]
        if w == 3:
            return f1.at[lines(b, quarter)]
        if w == 4:
            return f2.at[lines(b, quarter)]
        return f2.at[pl.ds(pl.multiple_of(b * quarter + cut(w, b), 32), length_of(w))]

    def source(w):
        if w == 0:
            return place(0, row)
        return (None, qrest.at[row], wp, w1, w2)[w]

    zwhich = (0, 1, 1, 2, 2)

    def zslot(w, which):
        return w * 3 + which if w < 5 else 10 + w

    def z_copy(w, s, b):
        return remote(
            place(w, b), place(w, b), zsend.at[min(w, 3) * 5 + s], zrecv.at[zslot(w, zwhich[s])],
            row=other if s in (1, 4) else near,
        )

    def own_copy(w, s):
        return remote(
            source(w), place(w, row), zsend.at[min(w, 3) * 5 + s], zrecv.at[zslot(w, zwhich[s])],
            row=other if s == 1 else near,
        )

    def z_wait(w, which):
        z_copy(w, (0, 2, 3)[which], (near, other, far)[which]).wait_recv()

    def z_forward(w, s):
        which = {2: 1, 3: 2, 4: 0}[s]
        z_wait(w, which)
        z_copy(w, s, (near, other, far)[which]).start()

    def z_sent(s):
        for w in (0, 1, 2):
            z_copy(w, s, row).wait_send()
        both = f1.at[pl.ds(0, 2 * quarter)]
        remote(both, both, zsend.at[15 + s], zrecv.at[0], row=near).wait_send()

    loads = [load(0, wq_in, wq), load(1, tok_in, tok)]
    for i, (src, dst) in enumerate(
        ((g1, v1), (c1, v2), (g2, v3), (c2, v4), (pb, v5), (d2, v6), (qb, v7), (d1, v8))
    ):
        loads.append(load(i + 2, src, dst))
    loads.append(load(10, wp, place(2, row)))
    loads.append(load(11, w1, place(3, row)))
    loads.append(load(12, w2, place(4, row)))
    for c in loads:
        c.start()
    loads[0].wait()
    turned = wq[...].astype(f32).T.astype(bf16)
    qmain[lines(row, quarter), :] = turned[:, :whole]
    for j in range(quarter // 32):
        qrest[row, :, j * rest : (j + 1) * rest] = turned[32 * j : 32 * (j + 1), whole:]
    pl.semaphore_wait(barrier, 6 + row * (3 - row) // 2)
    for w in (0, 1, 2):
        own_copy(w, 0).start()

    @pl.when(middle)
    def _():
        for w in (0, 1, 2):
            own_copy(w, 1).start()

    @pl.when(end)
    def _():
        for w in (3, 4):
            own_copy(w, 0).start()

    for i, v in enumerate((v1, v2, v3, v4, v5, v6, v7, v8)):
        loads[i + 2].wait()
        vec[i : i + 1, : v.shape[0]] = v[...].astype(f32).reshape(1, -1)
    loads[1].wait()

    def norm(values, g, b):
        mean = jnp.mean(values, axis=-1, keepdims=True)
        centred = values - mean
        var = jnp.mean(centred * centred, axis=-1, keepdims=True)
        return centred * lax.rsqrt(var + 1e-06) * vec[g : g + 1, :] + vec[b : b + 1, :]

    chunk = 32

    def norm1(i):
        at = pl.ds(pl.multiple_of(i * chunk, chunk), chunk)
        to = pl.ds(pl.multiple_of(me * rows + i * chunk, chunk), chunk)
        x1[to, :] = norm(tok[at, :].astype(f32), 0, 1).astype(bf16)

    some = half // chunk // 2

    def two_steps(body, gather):
        for part in (0, 1):
            def step(t, c):
                body(t % some + t // some * 2 * some + part * some)
                return c

            lax.fori_loop(0, 2 * some, step, 0)
            gather.start(part)

    class Gather:
        wait_on = (0, 1, 2, 2, 3, 3, 4, 4, 5, 5, 5, 5, 6, 6)

        def __init__(self, x, gi):
            self.x, self.gi = x, gi

        def copy(self, i, block, h, to):
            at = self.x.at[pl.ds(pl.multiple_of(block * rows + h * half, half), half)]
            return remote(
                at, at, gsend.at[self.gi], grecv.at[self.gi, self.wait_on[i]], col=to
            )

        def arrived(self, i, count):
            at = self.x.at[pl.ds(0, count * half)]
            remote(at, at, gsend.at[self.gi], grecv.at[self.gi, i], col=mate).wait_recv()

        def start(self, part):
            for i, to in ((0, xn), (1, yn)):
                at = self.x.at[
                    pl.ds(pl.multiple_of(me * rows + i * half + part * half // 2, half // 2), half // 2)
                ]
                remote(at, at, gsend.at[self.gi], grecv.at[self.gi, i], col=to).start()
            if part:
                for i, h, to in ((2, 1, xn), (3, 0, yn), (6, 0, mate), (7, 1, mate)):
                    self.copy(i, me, h, to).start()

        def event0(self):
            self.arrived(0, 1)
            self.copy(4, xn, 0, yn).start()
            self.copy(8, xn, 0, mate).start()
            self.arrived(1, 1)
            self.copy(5, yn, 1, xn).start()
            self.copy(9, yn, 1, mate).start()

        def event1(self):
            self.arrived(2, 2)
            self.copy(10, xn, 1, mate).start()
            self.copy(11, yn, 0, mate).start()

        def event2(self):
            self.arrived(3, 2)
            self.copy(12, dn, 0, mate).start()
            self.copy(13, dn, 1, mate).start()

        def mate0(self):
            self.arrived(4, 2)

        def mate1(self):
            self.arrived(5, 4)

        def mate2(self):
            self.arrived(6, 2)

        def finish(self):
            at = self.x.at[pl.ds(0, 14 * half)]
            remote(at, at, gsend.at[self.gi], grecv.at[self.gi, 0], col=mate).wait_send()

    first = Gather(x1, 0)
    two_steps(norm1, first)
    qrow[...] = jnp.zeros_like(qrow)
    for g in range(groups):
        qrow[:, g * LANES : g * LANES + size] = vec[6:7, g * size : (g + 1) * size]
    lane = lax.broadcasted_iota(jnp.int32, (1, LANES), 1)
    for head in range(heads):
        at = slice((3 * head + 2) * LANES, (3 * head + 3) * LANES)
        qrow[:, at] = jnp.where(lane == size, 1.0, qrow[:, at])
    for c in loads[10:]:
        c.wait()

    spare = jnp.zeros((quarter, LANES - size), bf16)
    few = jnp.zeros((32, LANES - size), bf16)

    def widen(b):
        base = b * quarter
        at = pl.ds(pl.multiple_of(base, 32), quarter)
        for g in range(groups - 1):
            qwide[at, g * LANES : (g + 1) * LANES] = jnp.concatenate(
                [qmain[at, g * size : (g + 1) * size], spare], axis=1
            )
        for j in range(quarter // 32):
            some = pl.ds(pl.multiple_of(base + 32 * j, 32), 32)
            qwide[some, (groups - 1) * LANES :] = jnp.concatenate(
                [qmain[some, (groups - 1) * size :], qrest[b, :, j * rest : (j + 1) * rest], few],
                axis=1,
            )

    widen(row)

    def q_wait(b):
        z_wait(0, b)
        z_wait(1, b)

    @pl.when(middle)
    def _():
        for w in (0, 1):
            z_forward(w, 4)
        for w in (0, 1):
            z_forward(w, 2)

    first.event0()

    @pl.when(end)
    def _():
        q_wait(0)

    widen(near)

    @pl.when(middle)
    def _():
        z_forward(2, 2)
        z_forward(2, 4)
        own_copy(3, 1).start()
        for w in (0, 1):
            z_forward(w, 3)

    first.event1()

    p_on = (0, 1, 4, 2, 3, 4, 4, 4, 4)

    def pcopy(i, r, at, count, block, to):
        ref = pfull.at[pl.ds(at, count), lines(block, prows)]
        return remote(ref, ref, psend.at[r], precv.at[r, p_on[i]], col=to)

    def punits(r, i, count):
        ref = pfull.at[pl.ds(0, 2), pl.ds(0, count // 2 * prows)]
        return remote(ref, ref, psend.at[r], precv.at[r, i], col=mate)

    def p_start(r, at):
        pcopy(0, r, at, 2, me, xn).start()
        pcopy(1, r, at, 2, me, yn).start()
        pcopy(2, r, at, 2, me, mate).start()

    def p_forward(r, at):
        pcopy(0, r, at, 2, xn, xn).wait_recv()
        pcopy(3, r, at, 1, xn, yn).start()
        pcopy(5, r, at, 2, xn, mate).start()
        pcopy(1, r, at, 2, yn, yn).wait_recv()
        pcopy(4, r, at + 1, 1, yn, xn).start()
        pcopy(6, r, at, 2, yn, mate).start()

    def p_last(r, at):
        pcopy(3, r, at, 1, dn, yn).wait_recv()
        pcopy(7, r, at, 1, dn, mate).start()
        pcopy(4, r, at + 1, 1, dn, xn).wait_recv()
        pcopy(8, r, at + 1, 1, dn, mate).start()

    def p_mates(r):
        punits(r, 4, 8).wait_recv()

    def p_finish(r):
        punits(r, 0, 14).wait_send()


    @pl.when(end)
    def _():
        z_wait(2, 0)

    p_start(0, lo)

    @pl.when(middle)
    def _():
        z_forward(2, 3)
        p_start(1, hi)
        own_copy(3, 0).start()
        z_forward(3, 4)
        own_copy(4, 1).start()

    first.event2()
    first.mate0()

    @pl.when(end)
    def _():
        q_wait(1)
        q_wait(2)

    widen(other)
    widen(far)
    first.mate1()
    first.mate2()

    factor = 1.4426950408889634 / size**0.5

    def qkv_block(i, c):
        @pl.when(jnp.logical_or(jnp.logical_and(i == 1, end), jnp.logical_and(i == 2, middle)))
        def _():
            p_forward(0, lo)

        @pl.when(jnp.logical_and(i == 2, end))
        def _():
            z_wait(2, 1)
            z_wait(2, 2)
            p_start(1, hi)

        at = lines(flipped(2 * i) // 2, 2 * rows)
        product = jnp.dot(x1[at, :], qwide[...], preferred_element_type=f32) + qrow[...]
        for g in range(groups):
            cols = slice(g * LANES, (g + 1) * LANES)
            value = product[:, cols]
            qkv[at, cols] = (value * factor if g % 3 == 0 else value).astype(bf16)
        return c

    lax.fori_loop(0, 4, qkv_block, 0)

    rest_lanes = prows - LANES

    def a_all(which):
        ref = (heads_in, tails_in)[which].at[pl.ds(0, 7)]
        return remote(ref, ref, asend.at[which], arecv.at[which], col=mate)

    def a_copies(i, core, to):
        at = lines(core)
        tail = pl.ds(pl.multiple_of(core * half, half), half)
        return (
            remote(
                heads_out.at[i, at], heads_in.at[me], asend.at[0], arecv.at[0], col=to
            ),
            remote(
                tails_out.at[i, tail], tails_in.at[me], asend.at[1], arecv.at[1], col=to
            ),
        )

    def attend_block(i, c):
        @pl.when(jnp.logical_and(i == 1, middle))
        def _():
            z_forward(3, 2)
            z_forward(4, 4)

        @pl.when(i == 2)
        def _():
            p_last(0, lo)
            p_forward(1, hi)

        chip = flipped(6 - 2 * i) // 2
        at = lines(chip, 2 * rows)
        scores = []
        for head in range(heads):
            base = head * 3 * LANES
            scores.append(
                lax.dot_general(
                    qkv[at, base : base + LANES], qkv[:, base + LANES : base + 2 * LANES],
                    (((1,), (1,)), ((), ())), preferred_element_type=f32,
                )
            )
        expos = [
            jnp.exp2(x - jnp.max(x, axis=-1, keepdims=True)).astype(bf16) for x in scores
        ]
        outs = []
        for head in range(heads):
            base = (head * 3 + 2) * LANES
            mixed = jnp.dot(
                expos[head], qkv[:, base : base + LANES], preferred_element_type=f32
            )
            outs.append(mixed[:, :size] / mixed[:, size : size + 1])
        mixed = jnp.concatenate(outs, axis=1).astype(bf16)
        gap = jnp.zeros((half, LANES // 2 - rest_lanes), bf16)
        heads_out[i] = mixed[:, :LANES]
        for core in (0, 1):
            top, low = (
                mixed[core * rows + h * half : core * rows + (h + 1) * half, LANES:]
                for h in (0, 1)
            )
            tails_out[i, core * half : (core + 1) * half, :] = jnp.concatenate(
                [top, gap, low, gap], axis=1
            )
        for core in (0, 1):
            to = 2 * chip + core

            @pl.when(to != me)
            def _():
                for c in a_copies(i, core, to):
                    c.start()

        return c

    lax.fori_loop(0, 4, attend_block, 0)
    @pl.when(middle)
    def _():
        z_forward(3, 3)
        own_copy(4, 0).start()

    p_last(1, hi)
    first.finish()
    heads_in[me] = heads_out[3, lines(me % 2), :]
    tails_in[me] = tails_out[3, lines(me % 2, half), :]
    p_mates(0)
    p_mates(1)
    a_all(0).wait_recv()
    a_all(1).wait_recv()
    for d in range(8):
        base = d * prows
        ctx[:, base : base + LANES] = heads_in[d]
        for h in (0, 1):
            ctx[h * half : (h + 1) * half, base + LANES : base + prows] = tails_in[
                d, :, h * (LANES // 2) : h * (LANES // 2) + rest_lanes
            ]

    for b in range(4):
        resid[:, b * quarter : (b + 1) * quarter] = jnp.dot(
            ctx[...], pfull[b], preferred_element_type=f32
        )

    def norm2(i):
        at = pl.ds(pl.multiple_of(i * chunk, chunk), chunk)
        to = pl.ds(pl.multiple_of(me * rows + i * chunk, chunk), chunk)
        value = tok[at, :].astype(f32) + resid[at, :] + vec[4:5, :]
        resid[at, :] = value
        x2[to, :] = norm(value, 2, 3).astype(bf16)

    second = Gather(x2, 1)
    two_steps(norm2, second)
    second.event0()

    @pl.when(end)
    def _():
        z_wait(3, 0)
        z_wait(3, 1)
        z_wait(3, 2)

    starts, done = [], 0
    for width in pieces:
        starts.append(done + (features - width - 2 * done) * pair)
        done += width
    targets = (dn, yn, xn, me)

    class Piece:
        def __init__(self, p):
            self.p, self.width = p, pieces[p]
            self.cols = pl.ds(pl.multiple_of(starts[p], LANES), pieces[p])

        def copy(self, i, src, dst, to):
            return remote(
                src, dst, ssend.at[self.p, min(i // 4, 1)], srecv.at[self.p, min(i, 6)], col=to
            )

        def of(self, ref, k, h):
            return ref.at[k, pl.ds(h * half, half), self.cols]

        def to_mate(self, k):
            block = flipped(6 - 2 * k + 1)
            return remote(
                part.at[lines(block), self.cols], mated.at[k, :, self.cols],
                ssend.at[self.p, 0], srecv.at[self.p, k], col=mate,
            )

        def compute(self, k):
            at = lines(flipped(6 - 2 * k) // 2, 2 * rows)
            part[at, self.cols] = project_back(hid[at, :], f2[self.cols, :]).astype(bf16)
            self.to_mate(k).start()

        def compute_all(self):
            def body(k, c):
                self.compute(k)
                return c

            lax.fori_loop(0, 4, body, 0)

        def mine(self, k, h):
            at = pl.ds(pl.multiple_of(targets[k] * rows + h * half, half), half)
            return part[at, self.cols].astype(f32) + mated[
                k, h * half : (h + 1) * half, self.cols
            ].astype(f32)

        def put(self, k, h, value):
            sums[k, h * half : (h + 1) * half, self.cols] = value.astype(bf16)

        def relays(self, h):
            return relay.at[h, :, self.cols]

        def c(self, i):
            k, h, dst, to = {
                4: (0, 0, self.relays(0), xn),
                5: (0, 1, self.relays(1), yn),
                6: (2, 0, self.of(landed, 0, 0), xn),
                7: (1, 1, self.of(landed, 1, 1), yn),
                8: (1, 0, self.of(landed, 1, 0), yn),
                9: (2, 1, self.of(landed, 0, 1), xn),
            }[i]
            return self.copy(i, self.of(sums, k, h), dst, to)

        def direct(self, k):
            h = {1: 1, 2: 0}[k]
            self.to_mate(k).wait_recv()
            self.put(k, h, self.mine(k, h))
            self.c({1: 7, 2: 6}[k]).start()

        def open_relayed(self):
            self.to_mate(0).wait_recv()
            self.put(0, 0, self.mine(0, 0))
            self.c(4).start()
            self.put(0, 1, self.mine(0, 1))
            self.c(5).start()

        def pass_on(self):
            self.c(4).wait_recv()
            self.put(1, 0, self.mine(1, 0) + relay[0, :, self.cols].astype(f32))
            self.c(8).start()
            self.c(5).wait_recv()
            self.put(2, 1, self.mine(2, 1) + relay[1, :, self.cols].astype(f32))
            self.c(9).start()

        def close(self):
            self.to_mate(3).wait_recv()
            ref = landed.at[:, :, self.cols]
            self.copy(6, ref, ref, mate).wait_recv()
            for h in (0, 1):
                at = slice(h * half, (h + 1) * half)
                total = (
                    self.mine(3, h)
                    + landed[0, at, self.cols].astype(f32)
                    + landed[1, at, self.cols].astype(f32)
                )
                value = resid[at, self.cols] + total + vec[5:6, self.cols]
                o_ref[at, self.cols] = value.astype(bf16)

        def finish(self):
            ref = mated.at[:, :, self.cols]
            self.copy(0, ref, ref, mate).wait_send()
            ref = sums.at[:, :, self.cols]
            self.copy(6, ref, ref, mate).wait_send()

    one, two, after, three, four = (Piece(p) for p in range(5))

    def fc1_block(i, c):
        @pl.when(i == 0)
        def _():
            second.mate0()

        @pl.when(i == 1)
        def _():
            second.event1()

        @pl.when(jnp.logical_and(i == 1, middle))
        def _():
            z_wait(4, 1)
            z_copy(7, 2, other).start()
            z_copy(8, 2, other).start()

        @pl.when(i == 1)
        def _():
            second.mate1()

        @pl.when(i == 3)
        def _():
            second.event2()

        @pl.when(jnp.logical_and(i == 3, middle))
        def _():
            z_wait(4, 2)
            z_copy(5, 3, far).start()
            z_copy(6, 3, far).start()

        @pl.when(i == 3)
        def _():
            one.direct(1)
            second.mate2()

        at = lines(flipped(2 * i) // 2, 2 * rows)
        for c0 in range(0, hidden, 2 * LANES):
            cols = slice(c0, c0 + 2 * LANES)
            value = jnp.dot(x2[at, :], f1[:, cols], preferred_element_type=f32) + vec[7:8, cols]
            hid[at, cols] = (
                0.5 * value * (1.0 + lax.erf(value * 0.7071067811865476))
            ).astype(bf16)

        @pl.when(jnp.logical_and(i == 1, end))
        def _():
            z_wait(4, 0)

        @pl.when(i == 2)
        def _():
            one.direct(2)

        @pl.when(i > 0)
        def _():
            one.compute(3 - i)

        return c

    lax.fori_loop(0, 4, fc1_block, 0)

    def open_all(piece):
        piece.open_relayed()
        piece.direct(2)
        piece.direct(1)

    one.compute(3)
    one.open_relayed()

    @pl.when(end)
    def _():
        z_wait(7, 1)

    two.compute_all()
    open_all(two)

    @pl.when(end)
    def _():
        z_wait(8, 1)

    after.compute_all()
    open_all(after)
    one.pass_on()

    @pl.when(end)
    def _():
        z_wait(5, 2)

    three.compute_all()
    three.open_relayed()
    two.pass_on()
    after.pass_on()

    @pl.when(end)
    def _():
        z_wait(6, 2)

    four.compute_all()
    four.open_relayed()
    for piece in (three, four):
        piece.direct(2)
        piece.direct(1)

    three.pass_on()
    one.close()
    four.pass_on()
    two.close()
    after.close()
    three.close()
    four.close()

    for piece in (one, two, after, three, four):
        piece.finish()
    second.finish()
    p_finish(0)
    p_finish(1)
    a_all(0).wait_send()
    a_all(1).wait_send()
    z_sent(0)

    @pl.when(middle)
    def _():
        for way in range(1, 5):
            z_sent(way)


def layer_call(plan, *arrays):
    rows, features, quarter = plan["rows"], plan["features"], plan["quarter"]
    hidden = plan["hidden"]
    wide = 3 * plan["heads"] * LANES
    length = 8 * rows
    bf16, f32 = jnp.bfloat16, jnp.float32
    dma = pltpu.SemaphoreType.DMA
    return pl.pallas_call(
        functools.partial(layer_kernel, plan),
        out_shape=pltpu.VMEM((rows, features), bf16),
        in_specs=[pl.BlockSpec(memory_space=pl.ANY)] * 13,
        out_specs=pl.BlockSpec(memory_space=pltpu.VMEM),
        scratch_shapes=[
            pltpu.VMEM((rows, features), bf16),
            pltpu.VMEM(arrays[9].shape, bf16),
            *(pltpu.VMEM(arrays[i].shape, bf16) for i in (1, 2, 5, 6, 4, 8, 3, 7)),
            pltpu.VMEM((8, features), f32),
            pltpu.VMEM((length, features), bf16),
            pltpu.VMEM((length, features), bf16),
            pltpu.VMEM((features, plan["whole"]), bf16),
            pltpu.VMEM((4, 32, quarter // 32 * plan["rest"]), bf16),
            pltpu.VMEM((features, wide), bf16),
            pltpu.VMEM((1, wide), f32),
            pltpu.VMEM((length, wide), bf16),
            pltpu.VMEM((rows, features), bf16),
            pltpu.VMEM((4, 2 * rows, LANES), bf16),
            pltpu.VMEM((4, rows, LANES), bf16),
            pltpu.VMEM((8, rows, LANES), bf16),
            pltpu.VMEM((8, rows // 2, LANES), bf16),
            pltpu.VMEM((4, features, quarter), bf16),
            pltpu.VMEM((features, hidden), bf16),
            pltpu.VMEM((features, hidden), bf16),
            pltpu.VMEM((rows, features), f32),
            pltpu.VMEM((4, rows, features), bf16),
            pltpu.VMEM((3, rows, features), bf16),
            pltpu.VMEM((2, rows // 2, features), bf16),
            pltpu.VMEM((2, rows, features), bf16),
            dma((13,)),
            dma((20,)), dma((19,)),
            dma((2,)), dma((2, 7)),
            dma((2,)), dma((2, 5)),
            dma((2,)), dma((2,)),
            dma((5, 2)), dma((5, 7)),
        ],
        compiler_params=pltpu.CompilerParams(
            collective_id=3, has_side_effects=True, vmem_limit_bytes=60 * 1024 * 1024
        ),
        name="layer",
    )(*arrays)


def local(
    tokens_in,
    ln1_gain,
    ln1_bias,
    qkv_weight,
    qkv_bias,
    proj_weight,
    proj_bias,
    ln2_gain,
    ln2_bias,
    fc1_weight,
    fc1_bias,
    fc2_weight,
    fc2_bias,
):
    local_heads = HEADS // lax.axis_size("col")
    own_rows, features = tokens_in.shape
    size = qkv_weight.shape[1] // (3 * local_heads)
    padded = -(-(size + 1) // LANES) * LANES
    plan = fast_plan(
        local_heads, own_rows, features, qkv_weight.shape[1], proj_weight.shape[0],
        fc1_weight.shape[1],
    )
    if plan is not None:
        return layer_call(
            plan, tokens_in, ln1_gain, ln1_bias, qkv_bias, proj_bias, ln2_gain, ln2_bias, fc1_bias,
            fc2_bias, qkv_weight.T, proj_weight, fc1_weight, fc2_weight,
        )
    inputs = tokens_in.astype(jnp.float32)
    qkv_full = gather_row(qkv_weight, 0)
    proj_full = gather_row(proj_weight, 1)
    fc1_full = gather_row(fc1_weight, 0)
    fc2_full = gather_row(fc2_weight, 0)
    fc1_shift = fc1_bias.astype(jnp.float32)

    spare = padded - size
    qkv_wide = jnp.pad(
        qkv_full.reshape(features, local_heads, 3, size), ((0, 0), (0, 0), (0, 0), (0, spare))
    ).reshape(features, local_heads * 3 * padded)
    shift = jnp.pad(
        qkv_bias.astype(jnp.float32).reshape(local_heads, 3, size), ((0, 0), (0, 0), (0, spare))
    )
    shift = shift.at[:, 2, size].set(1.0).reshape(-1)
    scale = jnp.ones((local_heads, 3, padded), jnp.float32)
    scale = scale.at[:, 0].set(1.4426950408889634 / size**0.5).reshape(-1)

    ln1 = norm_local(inputs, ln1_gain, ln1_bias).astype(jnp.bfloat16)
    product = jnp.dot(gather_col(ln1, 0), qkv_wide, preferred_element_type=jnp.float32)
    qkv = ((product + shift) * scale).astype(jnp.bfloat16)
    attn = attend(qkv, local_heads, size, padded)
    proj_whole = cube_gather_col(proj_full)
    own_heads = lax.all_to_all(attn, "col", split_axis=0, concat_axis=1, tiled=True)
    attn_sum = jnp.dot(own_heads, proj_whole, preferred_element_type=jnp.float32)
    resid = inputs + attn_sum + proj_bias.astype(jnp.float32)
    ln2 = norm_local(resid, ln2_gain, ln2_bias).astype(jnp.bfloat16)
    product = jnp.dot(gather_col(ln2, 1), fc1_full, preferred_element_type=jnp.float32) + fc1_shift
    hidden = jax.nn.gelu(product, approximate=False).astype(jnp.bfloat16)
    mlp_sum = scatter_col(project_back(hidden, fc2_full).astype(jnp.bfloat16), 2)
    result = resid + mlp_sum + fc2_bias.astype(jnp.float32)
    return result.astype(jnp.bfloat16)


def solution(mesh):
    in_specs = (
        P(("row", "col"), None),
        P(),
        P(),
        P("row", "col"),
        P("col"),
        P("col", "row"),
        P(),
        P(),
        P(),
        P("row", "col"),
        P("col"),
        P("row", "col"),
        P(),
    )
    out_specs = P(("row", "col"), None)
    return jax.shard_map(local, mesh=mesh, in_specs=in_specs, out_specs=out_specs, check_vma=False)
```

```python
import functools

import jax
import jax.numpy as jnp
from jax import lax
from jax.experimental import pallas as pl
from jax.experimental.pallas import tpu as pltpu
from jax.sharding import PartitionSpec as P

HEADS = 16
LANES = 128
MESH = pl.DeviceIdType.MESH


def greet(peers):
    barrier = pltpu.get_barrier_semaphore()
    for peer in peers:
        pl.semaphore_signal(barrier, inc=1, device_id={"col": peer}, device_id_type=MESH)
    pl.semaphore_wait(barrier, len(peers))


def neighbours():
    me = lax.axis_index("col")
    core, x, y = me % 2, (me // 2) % 2, me // 4
    place = lambda y, x, core: y * 4 + x * 2 + core
    return (
        me,
        place(y, x, 1 - core),
        place(y, 1 - x, core),
        place(1 - y, x, core),
        place(1 - y, 1 - x, core),
    )


def gather_kernel(x_ref, o_ref, send, recv, local_sem):
    rows = x_ref.shape[0]
    half = rows // 2
    me, mate, xn, yn, dn = neighbours()
    greet((mate, xn, yn))

    def part(block, h):
        return o_ref.at[pl.ds(pl.multiple_of(block * rows + h * half, half), half)]

    def copy(i, src, block, h, to):
        return pltpu.make_async_remote_copy(
            src_ref=src, dst_ref=part(block, h), send_sem=send.at[i], recv_sem=recv.at[i],
            device_id={"col": to}, device_id_type=MESH,
        )

    def own(h):
        return x_ref.at[pl.ds(h * half, half)]

    def arrived(i, block, h):
        copy(i, own(0), block, h, mate).wait_recv()

    started = []

    def go(c):
        c.start()
        started.append(c)

    go(copy(0, own(0), me, 0, xn))
    go(copy(1, own(1), me, 1, yn))
    go(copy(2, own(1), me, 1, xn))
    go(copy(3, own(0), me, 0, yn))
    go(copy(6, own(0), me, 0, mate))
    go(copy(7, own(1), me, 1, mate))
    here = pltpu.make_async_copy(
        x_ref, o_ref.at[pl.ds(pl.multiple_of(me * rows, rows), rows)], local_sem
    )
    here.start()
    arrived(0, xn, 0)
    go(copy(4, part(xn, 0), xn, 0, yn))
    go(copy(8, part(xn, 0), xn, 0, mate))
    arrived(1, yn, 1)
    go(copy(5, part(yn, 1), yn, 1, xn))
    go(copy(9, part(yn, 1), yn, 1, mate))
    arrived(2, xn, 1)
    go(copy(10, part(xn, 1), xn, 1, mate))
    arrived(3, yn, 0)
    go(copy(11, part(yn, 0), yn, 0, mate))
    arrived(4, dn, 0)
    go(copy(12, part(dn, 0), dn, 0, mate))
    arrived(5, dn, 1)
    go(copy(13, part(dn, 1), dn, 1, mate))
    across = lambda block: block + mate - me
    for i, block, h in (
        (6, me, 0), (7, me, 1), (8, xn, 0), (9, yn, 1),
        (10, xn, 1), (11, yn, 0), (12, dn, 0), (13, dn, 1),
    ):
        arrived(i, across(block), h)
    for c in started:
        c.wait_send()
    here.wait()


def gather_col(x, collective_id):
    n = lax.axis_size("col")
    rows, width = x.shape
    if n != 8 or rows % 32:
        return lax.all_gather(x, "col", axis=0, tiled=True)
    return pl.pallas_call(
        gather_kernel,
        out_shape=jax.ShapeDtypeStruct((n * rows, width), x.dtype),
        in_specs=[pl.BlockSpec(memory_space=pltpu.VMEM)],
        out_specs=pl.BlockSpec(memory_space=pltpu.VMEM),
        scratch_shapes=[
            pltpu.SemaphoreType.DMA((14,)),
            pltpu.SemaphoreType.DMA((14,)),
            pltpu.SemaphoreType.DMA,
        ],
        compiler_params=pltpu.CompilerParams(
            collective_id=collective_id, has_side_effects=True, vmem_limit_bytes=24 << 20
        ),
        cost_estimate=pl.CostEstimate(
            flops=10**10, bytes_accessed=2 * n * rows * width, transcendentals=0
        ),
        name="gather_col",
    )(x)


def scatter_kernel(x_ref, o_ref, mated, sums, relay, landed, send, recv):
    rows = o_ref.shape[0]
    half = rows // 2
    me, mate, xn, yn, dn = neighbours()
    greet((mate, xn, yn))
    shift = mate - me
    targets = (dn, xn, yn, me)

    def copy(i, src, dst, to):
        return pltpu.make_async_remote_copy(
            src_ref=src, dst_ref=dst, send_sem=send.at[i], recv_sem=recv.at[i],
            device_id={"col": to}, device_id_type=MESH,
        )

    def block(j):
        return pl.ds(pl.multiple_of(j * rows, rows), rows)

    started = []

    def go(c):
        c.start()
        started.append(c)

    for k, target in enumerate(targets):
        go(copy(k, x_ref.at[block(target + shift)], mated.at[k], mate))

    def mine(k, h):
        rows_h = pl.ds(pl.multiple_of(targets[k] * rows + h * half, half), half)
        return x_ref[rows_h, :].astype(jnp.float32) + mated[k, pl.ds(h * half, half), :].astype(
            jnp.float32
        )

    def put(k, h, value):
        sums[k, pl.ds(h * half, half), :] = value.astype(jnp.bfloat16)

    def of(ref, k, h):
        return ref.at[k, pl.ds(h * half, half)]

    started[0].wait_recv()
    put(0, 0, mine(0, 0))
    go(copy(4, of(sums, 0, 0), relay.at[0], xn))
    put(0, 1, mine(0, 1))
    go(copy(5, of(sums, 0, 1), relay.at[1], yn))
    started[1].wait_recv()
    put(1, 0, mine(1, 0))
    go(copy(6, of(sums, 1, 0), of(landed, 0, 0), xn))
    started[2].wait_recv()
    put(2, 1, mine(2, 1))
    go(copy(7, of(sums, 2, 1), of(landed, 1, 1), yn))
    started[4].wait_recv()
    put(2, 0, mine(2, 0) + relay[0].astype(jnp.float32))
    go(copy(8, of(sums, 2, 0), of(landed, 1, 0), yn))
    started[5].wait_recv()
    put(1, 1, mine(1, 1) + relay[1].astype(jnp.float32))
    go(copy(9, of(sums, 1, 1), of(landed, 0, 1), xn))
    started[3].wait_recv()
    for i in (6, 7, 8, 9):
        started[i].wait_recv()
    for h in (0, 1):
        lines = pl.ds(h * half, half)
        o_ref[lines, :] = (
            mine(3, h)
            + landed[0, lines, :].astype(jnp.float32)
            + landed[1, lines, :].astype(jnp.float32)
        )
    for c in started:
        c.wait_send()


def scatter_col(x, collective_id):
    n = lax.axis_size("col")
    rows, width = x.shape[0] // n, x.shape[1]
    if n != 8 or rows % 32:
        return lax.psum_scatter(x, "col", scatter_dimension=0, tiled=True).astype(jnp.float32)
    return pl.pallas_call(
        scatter_kernel,
        out_shape=jax.ShapeDtypeStruct((rows, width), jnp.float32),
        in_specs=[pl.BlockSpec(memory_space=pltpu.VMEM)],
        out_specs=pl.BlockSpec(memory_space=pltpu.VMEM),
        scratch_shapes=[
            pltpu.VMEM((4, rows, width), x.dtype),
            pltpu.VMEM((3, rows, width), x.dtype),
            pltpu.VMEM((2, rows // 2, width), x.dtype),
            pltpu.VMEM((2, rows, width), x.dtype),
            pltpu.SemaphoreType.DMA((10,)),
            pltpu.SemaphoreType.DMA((10,)),
        ],
        compiler_params=pltpu.CompilerParams(
            collective_id=collective_id, has_side_effects=True, vmem_limit_bytes=32 << 20
        ),
        cost_estimate=pl.CostEstimate(
            flops=10**10, bytes_accessed=2 * n * rows * width, transcendentals=0
        ),
        name="scatter_col",
    )(x)


def gather_row(weight, axis):
    n = lax.axis_size("row")
    me = lax.axis_index("row")
    depth = weight.shape[axis]
    shape = list(weight.shape)
    shape[axis] *= n
    whole = jnp.zeros(shape, weight.dtype)
    for step in range(n):
        block = weight
        if step:
            block = lax.ppermute(weight, "row", [((i + step) % n, i) for i in range(n)])
        whole = lax.dynamic_update_slice_in_dim(whole, block, ((me + step) % n) * depth, axis)
    return whole


def cube_gather_col(x):
    n = lax.axis_size("col")
    if n != 8:
        return lax.all_gather(x, "col", axis=0, tiled=True)
    me = lax.axis_index("col")
    x = x[None]
    for bit, after in ((2, 1), (4, 2), (1, 4)):
        other = lax.ppermute(x, "col", [(i, i ^ bit) for i in range(n)])
        low = (me // bit) % 2 == 0
        first, second = jnp.where(low, x, other), jnp.where(low, other, x)
        x = jnp.concatenate([first, second], axis=0) if bit != 1 else jnp.stack([first, second], 1)
    return x.reshape(-1, x.shape[-1])


def norm_local(values, gain, bias):
    mean = jnp.mean(values, axis=-1, keepdims=True)
    centred = values - mean
    var = jnp.mean(centred * centred, axis=-1, keepdims=True)
    return centred * lax.rsqrt(var + 1e-06) * gain.astype(jnp.float32) + bias.astype(jnp.float32)


def attend_kernel(heads, size, padded, q_ref, kv_ref, o_ref):
    outs = []
    for head in range(heads):
        base = head * 3 * padded
        query = q_ref[:, base : base + padded]
        keys = kv_ref[:, base + padded : base + 2 * padded]
        values = kv_ref[:, base + 2 * padded : base + 3 * padded]
        scores = lax.dot_general(
            query, keys, (((1,), (1,)), ((), ())), preferred_element_type=jnp.float32
        )
        top = jnp.max(scores, axis=-1, keepdims=True)
        expo = jnp.exp2(scores - top).astype(jnp.bfloat16)
        mixed = jnp.dot(expo, values, preferred_element_type=jnp.float32)
        outs.append(mixed[:, :size] / mixed[:, size : size + 1])
    o_ref[...] = jnp.concatenate(outs, axis=1).astype(o_ref.dtype)


def attend(qkv, heads, size, padded):
    length, width = qkv.shape
    block = min(256, length)
    return pl.pallas_call(
        functools.partial(attend_kernel, heads, size, padded),
        grid=(length // block,),
        in_specs=[
            pl.BlockSpec((block, width), lambda i: (i, 0)),
            pl.BlockSpec((length, width), lambda i: (0, 0)),
        ],
        out_specs=pl.BlockSpec((block, heads * size), lambda i: (i, 0)),
        out_shape=jax.ShapeDtypeStruct((length, heads * size), jnp.bfloat16),
        compiler_params=pltpu.CompilerParams(vmem_limit_bytes=40 << 20),
        cost_estimate=pl.CostEstimate(
            flops=4 * heads * length * length * padded * 8,
            bytes_accessed=4 * length * width,
            transcendentals=heads * length * length,
        ),
        name="attend",
    )(qkv, qkv)


def project_back(left, right):
    return lax.dot_general(
        left, right, (((1,), (1,)), ((), ())), preferred_element_type=jnp.float32
    )


def fast_plan(heads, own_rows, features, qkv_width, proj_rows, hidden):
    if lax.axis_size("col") != 8 or lax.axis_size("row") != 4:
        return None
    quarter = features // 4
    size = qkv_width // (3 * heads)
    whole = qkv_width // LANES * LANES
    rest = qkv_width - whole
    ok = (
        hidden == 3 * heads * LANES and own_rows % 128 == 0 and features % LANES == 0 and quarter % 32 == 0
        and hidden % LANES == 0 and 0 < rest and proj_rows == heads * size
        and proj_rows % 16 == 0 and 0 < proj_rows - LANES <= LANES // 2
        and 8 * proj_rows == features and size < LANES and whole // size == 3 * heads - 1
    )
    if not ok:
        return None
    first = 2 * quarter // LANES * LANES
    last = -(-quarter // LANES) * LANES
    middle = features - first - last
    if middle <= LANES or last <= LANES or features - last > 3 * quarter:
        return None
    if (first + middle - LANES - 2 * quarter) % 32:
        return None
    return dict(
        heads=heads, size=size, rows=own_rows, features=features, quarter=quarter, whole=whole,
        rest=rest, proj_rows=proj_rows, hidden=hidden,
        pieces=(first, middle - LANES, LANES, last - LANES, LANES),
        early=first + middle - LANES - 2 * quarter,
    )


def layer_kernel(
    plan, tok_in, g1, c1, qb, pb, g2, c2, d1, d2, wq_in, wp, w1, w2, o_ref,
    tok, wq, v1, v2, v3, v4, v5, v6, v7, v8,
    vec, x1, x2, qmain, qrest, qwide, qrow, qkv, ctx, heads_out, tails_out, heads_in, tails_in, pfull, f1, f2, resid,
    mated, sums, relay, landed,
    lsem, zsend, zrecv, gsend, grecv, psend, precv, asend, arecv, ssend, srecv,
):
    heads, size, rows = plan["heads"], plan["size"], plan["rows"]
    features, quarter = plan["features"], plan["quarter"]
    whole, rest, prows = plan["whole"], plan["rest"], plan["proj_rows"]
    hidden, pieces = plan["hidden"], plan["pieces"]
    half = rows // 2
    groups = 3 * heads
    f32, bf16 = jnp.float32, jnp.bfloat16
    hid, part = qkv, x1

    row = lax.axis_index("row")
    me, mate, xn, yn, dn = neighbours()
    shift = mate - me
    pair = row // 2
    near = row + 1 - 2 * (row % 2)
    other = 2 - pair
    far = 3 - 3 * pair
    middle = jnp.logical_or(row == 1, row == 2)
    end = jnp.logical_or(row == 0, row == 3)
    lo = 2 * pair
    hi = 2 - lo

    def flipped(mask):
        bits = [(me % 2 + mask % 2) % 2, (me // 2 % 2 + mask // 2 % 2) % 2, (me // 4 + mask // 4) % 2]
        return bits[0] + 2 * bits[1] + 4 * bits[2]

    barrier = pltpu.get_barrier_semaphore()
    for step in range(1, 6):
        pl.semaphore_signal(
            barrier, inc=1, device_id={"col": flipped(step)}, device_id_type=MESH
        )
    pl.semaphore_signal(barrier, inc=1, device_id={"row": near}, device_id_type=MESH)

    @pl.when(middle)
    def _():
        pl.semaphore_signal(barrier, inc=1, device_id={"row": other}, device_id_type=MESH)


    def load(i, src, dst):
        return pltpu.make_async_copy(src, dst, lsem.at[i])

    def remote(src, dst, ssem, rsem, **to):
        return pltpu.make_async_remote_copy(
            src_ref=src, dst_ref=dst, send_sem=ssem, recv_sem=rsem,
            device_id=to, device_id_type=MESH,
        )

    def lines(b, n=rows):
        return pl.ds(pl.multiple_of(b * n, n), n)

    early = plan["early"]

    def cut(w, b):
        low = b // 2
        return {
            5: (1 - low) * LANES,
            6: low * (quarter - LANES),
            7: (1 - low) * (quarter - early),
            8: low * early,
        }[w]

    def length_of(w):
        return {5: quarter - LANES, 6: LANES, 7: early, 8: quarter - early}[w]

    def place(w, b):
        if w == 0:
            return qmain.at[lines(b, quarter)]
        if w == 1:
            return qrest.at[b]
        if w == 2:
            return pfull.at[b, lines(me, prows)]
        if w == 3:
            return f1.at[lines(b, quarter)]
        if w == 4:
            return f2.at[lines(b, quarter)]
        return f2.at[pl.ds(pl.multiple_of(b * quarter + cut(w, b), 32), length_of(w))]

    def source(w):
        if w == 0:
            return place(0, row)
        return (None, qrest.at[row], wp, w1, w2)[w]

    zwhich = (0, 1, 1, 2, 2)

    def zslot(w, which):
        return w * 3 + which if w < 5 else 10 + w

    def z_copy(w, s, b):
        return remote(
            place(w, b), place(w, b), zsend.at[min(w, 3) * 5 + s], zrecv.at[zslot(w, zwhich[s])],
            row=other if s in (1, 4) else near,
        )

    def own_copy(w, s):
        return remote(
            source(w), place(w, row), zsend.at[min(w, 3) * 5 + s], zrecv.at[zslot(w, zwhich[s])],
            row=other if s == 1 else near,
        )

    def z_wait(w, which):
        z_copy(w, (0, 2, 3)[which], (near, other, far)[which]).wait_recv()

    def z_forward(w, s):
        which = {2: 1, 3: 2, 4: 0}[s]
        z_wait(w, which)
        z_copy(w, s, (near, other, far)[which]).start()

    def z_sent(s):
        for w in (0, 1, 2):
            z_copy(w, s, row).wait_send()
        both = f1.at[pl.ds(0, 2 * quarter)]
        remote(both, both, zsend.at[15 + s], zrecv.at[0], row=near).wait_send()

    loads = [load(0, wq_in, wq), load(1, tok_in, tok)]
    for i, (src, dst) in enumerate(
        ((g1, v1), (c1, v2), (g2, v3), (c2, v4), (pb, v5), (d2, v6), (qb, v7), (d1, v8))
    ):
        loads.append(load(i + 2, src, dst))
    loads.append(load(10, wp, place(2, row)))
    loads.append(load(11, w1, place(3, row)))
    loads.append(load(12, w2, place(4, row)))
    for c in loads:
        c.start()
    loads[0].wait()
    turned = wq[...].astype(f32).T.astype(bf16)
    qmain[lines(row, quarter), :] = turned[:, :whole]
    for j in range(quarter // 32):
        qrest[row, :, j * rest : (j + 1) * rest] = turned[32 * j : 32 * (j + 1), whole:]
    pl.semaphore_wait(barrier, 6 + row * (3 - row) // 2)
    for w in (0, 1, 2):
        own_copy(w, 0).start()

    @pl.when(middle)
    def _():
        for w in (0, 1, 2):
            own_copy(w, 1).start()

    @pl.when(end)
    def _():
        for w in (3, 4):
            own_copy(w, 0).start()

    for i, v in enumerate((v1, v2, v3, v4, v5, v6, v7, v8)):
        loads[i + 2].wait()
        vec[i : i + 1, : v.shape[0]] = v[...].astype(f32).reshape(1, -1)
    loads[1].wait()

    def norm(values, g, b):
        mean = jnp.mean(values, axis=-1, keepdims=True)
        centred = values - mean
        var = jnp.mean(centred * centred, axis=-1, keepdims=True)
        return centred * lax.rsqrt(var + 1e-06) * vec[g : g + 1, :] + vec[b : b + 1, :]

    chunk = 32

    def norm1(i):
        at = pl.ds(pl.multiple_of(i * chunk, chunk), chunk)
        to = pl.ds(pl.multiple_of(me * rows + i * chunk, chunk), chunk)
        x1[to, :] = norm(tok[at, :].astype(f32), 0, 1).astype(bf16)

    some = half // chunk // 2

    def two_steps(body, gather):
        for part in (0, 1):
            def step(t, c):
                body(t % some + t // some * 2 * some + part * some)
                return c

            lax.fori_loop(0, 2 * some, step, 0)
            gather.start(part)

    class Gather:
        wait_on = (0, 1, 2, 2, 3, 3, 4, 4, 5, 5, 5, 5, 6, 6)

        def __init__(self, x, gi):
            self.x, self.gi = x, gi

        def copy(self, i, block, h, to):
            at = self.x.at[pl.ds(pl.multiple_of(block * rows + h * half, half), half)]
            return remote(
                at, at, gsend.at[self.gi], grecv.at[self.gi, self.wait_on[i]], col=to
            )

        def arrived(self, i, count):
            at = self.x.at[pl.ds(0, count * half)]
            remote(at, at, gsend.at[self.gi], grecv.at[self.gi, i], col=mate).wait_recv()

        def start(self, part):
            for i, to in ((0, xn), (1, yn)):
                at = self.x.at[
                    pl.ds(pl.multiple_of(me * rows + i * half + part * half // 2, half // 2), half // 2)
                ]
                remote(at, at, gsend.at[self.gi], grecv.at[self.gi, i], col=to).start()
            if part:
                for i, h, to in ((2, 1, xn), (3, 0, yn), (6, 0, mate), (7, 1, mate)):
                    self.copy(i, me, h, to).start()

        def event0(self):
            self.arrived(0, 1)
            self.copy(4, xn, 0, yn).start()
            self.copy(8, xn, 0, mate).start()
            self.arrived(1, 1)
            self.copy(5, yn, 1, xn).start()
            self.copy(9, yn, 1, mate).start()

        def event1(self):
            self.arrived(2, 2)
            self.copy(10, xn, 1, mate).start()
            self.copy(11, yn, 0, mate).start()

        def event2(self):
            self.arrived(3, 2)
            self.copy(12, dn, 0, mate).start()
            self.copy(13, dn, 1, mate).start()

        def mate0(self):
            self.arrived(4, 2)

        def mate1(self):
            self.arrived(5, 4)

        def mate2(self):
            self.arrived(6, 2)

        def finish(self):
            at = self.x.at[pl.ds(0, 14 * half)]
            remote(at, at, gsend.at[self.gi], grecv.at[self.gi, 0], col=mate).wait_send()

    first = Gather(x1, 0)
    two_steps(norm1, first)
    qrow[...] = jnp.zeros_like(qrow)
    for g in range(groups):
        qrow[:, g * LANES : g * LANES + size] = vec[6:7, g * size : (g + 1) * size]
    lane = lax.broadcasted_iota(jnp.int32, (1, LANES), 1)
    for head in range(heads):
        at = slice((3 * head + 2) * LANES, (3 * head + 3) * LANES)
        qrow[:, at] = jnp.where(lane == size, 1.0, qrow[:, at])
    for c in loads[10:]:
        c.wait()

    spare = jnp.zeros((quarter, LANES - size), bf16)
    few = jnp.zeros((32, LANES - size), bf16)

    def widen(b):
        base = b * quarter
        at = pl.ds(pl.multiple_of(base, 32), quarter)
        for g in range(groups - 1):
            qwide[at, g * LANES : (g + 1) * LANES] = jnp.concatenate(
                [qmain[at, g * size : (g + 1) * size], spare], axis=1
            )
        for j in range(quarter // 32):
            some = pl.ds(pl.multiple_of(base + 32 * j, 32), 32)
            qwide[some, (groups - 1) * LANES :] = jnp.concatenate(
                [qmain[some, (groups - 1) * size :], qrest[b, :, j * rest : (j + 1) * rest], few],
                axis=1,
            )

    widen(row)

    def q_wait(b):
        z_wait(0, b)
        z_wait(1, b)

    @pl.when(middle)
    def _():
        for w in (0, 1):
            z_forward(w, 4)
        for w in (0, 1):
            z_forward(w, 2)

    first.event0()

    @pl.when(end)
    def _():
        q_wait(0)

    widen(near)

    @pl.when(middle)
    def _():
        z_forward(2, 2)
        z_forward(2, 4)
        own_copy(3, 1).start()
        for w in (0, 1):
            z_forward(w, 3)

    first.event1()

    p_on = (0, 1, 4, 2, 3, 4, 4, 4, 4)

    def pcopy(i, r, at, count, block, to):
        ref = pfull.at[pl.ds(at, count), lines(block, prows)]
        return remote(ref, ref, psend.at[r], precv.at[r, p_on[i]], col=to)

    def punits(r, i, count):
        ref = pfull.at[pl.ds(0, 2), pl.ds(0, count // 2 * prows)]
        return remote(ref, ref, psend.at[r], precv.at[r, i], col=mate)

    def p_start(r, at):
        pcopy(0, r, at, 2, me, xn).start()
        pcopy(1, r, at, 2, me, yn).start()
        pcopy(2, r, at, 2, me, mate).start()

    def p_forward(r, at):
        pcopy(0, r, at, 2, xn, xn).wait_recv()
        pcopy(3, r, at, 1, xn, yn).start()
        pcopy(5, r, at, 2, xn, mate).start()
        pcopy(1, r, at, 2, yn, yn).wait_recv()
        pcopy(4, r, at + 1, 1, yn, xn).start()
        pcopy(6, r, at, 2, yn, mate).start()

    def p_last(r, at):
        pcopy(3, r, at, 1, dn, yn).wait_recv()
        pcopy(7, r, at, 1, dn, mate).start()
        pcopy(4, r, at + 1, 1, dn, xn).wait_recv()
        pcopy(8, r, at + 1, 1, dn, mate).start()

    def p_mates(r):
        punits(r, 4, 8).wait_recv()

    def p_finish(r):
        punits(r, 0, 14).wait_send()


    @pl.when(end)
    def _():
        z_wait(2, 0)

    p_start(0, lo)

    @pl.when(middle)
    def _():
        z_forward(2, 3)
        p_start(1, hi)
        own_copy(3, 0).start()
        z_forward(3, 4)
        own_copy(4, 1).start()

    first.event2()
    first.mate0()

    @pl.when(end)
    def _():
        q_wait(1)
        q_wait(2)

    widen(other)
    widen(far)
    first.mate1()
    first.mate2()

    factor = 1.4426950408889634 / size**0.5

    def qkv_block(i, c):
        @pl.when(jnp.logical_or(jnp.logical_and(i == 1, end), jnp.logical_and(i == 2, middle)))
        def _():
            p_forward(0, lo)

        @pl.when(jnp.logical_and(i == 2, end))
        def _():
            z_wait(2, 1)
            z_wait(2, 2)
            p_start(1, hi)

        at = lines(flipped(2 * i) // 2, 2 * rows)
        product = jnp.dot(x1[at, :], qwide[...], preferred_element_type=f32) + qrow[...]
        for g in range(groups):
            cols = slice(g * LANES, (g + 1) * LANES)
            value = product[:, cols]
            qkv[at, cols] = (value * factor if g % 3 == 0 else value).astype(bf16)
        return c

    lax.fori_loop(0, 4, qkv_block, 0)

    rest_lanes = prows - LANES

    def a_all(which):
        ref = (heads_in, tails_in)[which].at[pl.ds(0, 7)]
        return remote(ref, ref, asend.at[which], arecv.at[which], col=mate)

    def a_copies(i, core, to):
        at = lines(core)
        tail = pl.ds(pl.multiple_of(core * half, half), half)
        return (
            remote(
                heads_out.at[i, at], heads_in.at[me], asend.at[0], arecv.at[0], col=to
            ),
            remote(
                tails_out.at[i, tail], tails_in.at[me], asend.at[1], arecv.at[1], col=to
            ),
        )

    def attend_block(i, c):
        @pl.when(jnp.logical_and(i == 1, middle))
        def _():
            z_forward(3, 2)
            z_forward(4, 4)

        @pl.when(i == 2)
        def _():
            p_last(0, lo)
            p_forward(1, hi)

        chip = flipped(6 - 2 * i) // 2
        at = lines(chip, 2 * rows)
        scores = []
        for head in range(heads):
            base = head * 3 * LANES
            scores.append(
                lax.dot_general(
                    qkv[at, base : base + LANES], qkv[:, base + LANES : base + 2 * LANES],
                    (((1,), (1,)), ((), ())), preferred_element_type=f32,
                )
            )
        expos = [
            jnp.exp2(x - jnp.max(x, axis=-1, keepdims=True)).astype(bf16) for x in scores
        ]
        outs = []
        for head in range(heads):
            base = (head * 3 + 2) * LANES
            mixed = jnp.dot(
                expos[head], qkv[:, base : base + LANES], preferred_element_type=f32
            )
            outs.append(mixed[:, :size] / mixed[:, size : size + 1])
        mixed = jnp.concatenate(outs, axis=1).astype(bf16)
        gap = jnp.zeros((half, LANES // 2 - rest_lanes), bf16)
        heads_out[i] = mixed[:, :LANES]
        for core in (0, 1):
            top, low = (
                mixed[core * rows + h * half : core * rows + (h + 1) * half, LANES:]
                for h in (0, 1)
            )
            tails_out[i, core * half : (core + 1) * half, :] = jnp.concatenate(
                [top, gap, low, gap], axis=1
            )
        for core in (0, 1):
            to = 2 * chip + core

            @pl.when(to != me)
            def _():
                for c in a_copies(i, core, to):
                    c.start()

        return c

    lax.fori_loop(0, 4, attend_block, 0)
    @pl.when(middle)
    def _():
        z_forward(3, 3)
        own_copy(4, 0).start()

    p_last(1, hi)
    first.finish()
    heads_in[me] = heads_out[3, lines(me % 2), :]
    tails_in[me] = tails_out[3, lines(me % 2, half), :]
    p_mates(0)
    p_mates(1)
    a_all(0).wait_recv()
    a_all(1).wait_recv()
    for d in range(8):
        base = d * prows
        ctx[:, base : base + LANES] = heads_in[d]
        for h in (0, 1):
            ctx[h * half : (h + 1) * half, base + LANES : base + prows] = tails_in[
                d, :, h * (LANES // 2) : h * (LANES // 2) + rest_lanes
            ]

    for b in range(4):
        resid[:, b * quarter : (b + 1) * quarter] = jnp.dot(
            ctx[...], pfull[b], preferred_element_type=f32
        )

    def norm2(i):
        at = pl.ds(pl.multiple_of(i * chunk, chunk), chunk)
        to = pl.ds(pl.multiple_of(me * rows + i * chunk, chunk), chunk)
        value = tok[at, :].astype(f32) + resid[at, :] + vec[4:5, :]
        resid[at, :] = value
        x2[to, :] = norm(value, 2, 3).astype(bf16)

    second = Gather(x2, 1)
    two_steps(norm2, second)
    second.event0()

    @pl.when(end)
    def _():
        z_wait(3, 0)
        z_wait(3, 1)
        z_wait(3, 2)

    starts, done = [], 0
    for width in pieces:
        starts.append(done + (features - width - 2 * done) * pair)
        done += width
    targets = (dn, yn, xn, me)

    class Piece:
        def __init__(self, p):
            self.p, self.width = p, pieces[p]
            self.cols = pl.ds(pl.multiple_of(starts[p], LANES), pieces[p])

        def copy(self, i, src, dst, to):
            return remote(
                src, dst, ssend.at[self.p, min(i // 4, 1)], srecv.at[self.p, min(i, 6)], col=to
            )

        def of(self, ref, k, h):
            return ref.at[k, pl.ds(h * half, half), self.cols]

        def to_mate(self, k):
            block = flipped(6 - 2 * k + 1)
            return remote(
                part.at[lines(block), self.cols], mated.at[k, :, self.cols],
                ssend.at[self.p, 0], srecv.at[self.p, k], col=mate,
            )

        def compute(self, k):
            at = lines(flipped(6 - 2 * k) // 2, 2 * rows)
            part[at, self.cols] = project_back(hid[at, :], f2[self.cols, :]).astype(bf16)
            self.to_mate(k).start()

        def compute_all(self):
            def body(k, c):
                self.compute(k)
                return c

            lax.fori_loop(0, 4, body, 0)

        def mine(self, k, h):
            at = pl.ds(pl.multiple_of(targets[k] * rows + h * half, half), half)
            return part[at, self.cols].astype(f32) + mated[
                k, h * half : (h + 1) * half, self.cols
            ].astype(f32)

        def put(self, k, h, value):
            sums[k, h * half : (h + 1) * half, self.cols] = value.astype(bf16)

        def relays(self, h):
            return relay.at[h, :, self.cols]

        def c(self, i):
            k, h, dst, to = {
                4: (0, 0, self.relays(0), xn),
                5: (0, 1, self.relays(1), yn),
                6: (2, 0, self.of(landed, 0, 0), xn),
                7: (1, 1, self.of(landed, 1, 1), yn),
                8: (1, 0, self.of(landed, 1, 0), yn),
                9: (2, 1, self.of(landed, 0, 1), xn),
            }[i]
            return self.copy(i, self.of(sums, k, h), dst, to)

        def direct(self, k):
            h = {1: 1, 2: 0}[k]
            self.to_mate(k).wait_recv()
            self.put(k, h, self.mine(k, h))
            self.c({1: 7, 2: 6}[k]).start()

        def open_relayed(self):
            self.to_mate(0).wait_recv()
            self.put(0, 0, self.mine(0, 0))
            self.c(4).start()
            self.put(0, 1, self.mine(0, 1))
            self.c(5).start()

        def pass_on(self):
            self.c(4).wait_recv()
            self.put(1, 0, self.mine(1, 0) + relay[0, :, self.cols].astype(f32))
            self.c(8).start()
            self.c(5).wait_recv()
            self.put(2, 1, self.mine(2, 1) + relay[1, :, self.cols].astype(f32))
            self.c(9).start()

        def close(self):
            self.to_mate(3).wait_recv()
            ref = landed.at[:, :, self.cols]
            self.copy(6, ref, ref, mate).wait_recv()
            for h in (0, 1):
                at = slice(h * half, (h + 1) * half)
                total = (
                    self.mine(3, h)
                    + landed[0, at, self.cols].astype(f32)
                    + landed[1, at, self.cols].astype(f32)
                )
                value = resid[at, self.cols] + total + vec[5:6, self.cols]
                o_ref[at, self.cols] = value.astype(bf16)

        def finish(self):
            ref = mated.at[:, :, self.cols]
            self.copy(0, ref, ref, mate).wait_send()
            ref = sums.at[:, :, self.cols]
            self.copy(6, ref, ref, mate).wait_send()

    one, two, after, three, four = (Piece(p) for p in range(5))

    def fc1_rows(block):
        at = lines(block)
        for c0 in range(0, hidden, 2 * LANES):
            cols = slice(c0, c0 + 2 * LANES)
            value = jnp.dot(x2[at, :], f1[:, cols], preferred_element_type=f32) + vec[7:8, cols]
            hid[at, cols] = (
                0.5 * value * (1.0 + lax.erf(value * 0.7071067811865476))
            ).astype(bf16)

    def fc1_block(i, c):
        @pl.when(i == 1)
        def _():
            second.event1()

        @pl.when(jnp.logical_and(i == 1, middle))
        def _():
            z_wait(4, 1)
            z_copy(7, 2, other).start()
            z_copy(8, 2, other).start()

        @pl.when(i == 3)
        def _():
            second.event2()

        @pl.when(jnp.logical_and(i == 3, middle))
        def _():
            z_wait(4, 2)
            z_copy(5, 3, far).start()
            z_copy(6, 3, far).start()

        fc1_rows(flipped(2 * i))

        @pl.when(i == 0)
        def _():
            second.mate0()

        @pl.when(i == 1)
        def _():
            second.mate1()

        @pl.when(i == 3)
        def _():
            one.direct(1)
            second.mate2()

        fc1_rows(flipped(2 * i + 1))

        @pl.when(jnp.logical_and(i == 1, end))
        def _():
            z_wait(4, 0)

        @pl.when(i == 2)
        def _():
            one.direct(2)

        @pl.when(i > 0)
        def _():
            one.compute(3 - i)

        return c

    lax.fori_loop(0, 4, fc1_block, 0)

    def open_all(piece):
        piece.open_relayed()
        piece.direct(2)
        piece.direct(1)

    one.compute(3)
    one.open_relayed()

    @pl.when(end)
    def _():
        z_wait(7, 1)

    two.compute_all()
    open_all(two)

    @pl.when(end)
    def _():
        z_wait(8, 1)

    after.compute_all()
    open_all(after)
    one.pass_on()

    @pl.when(end)
    def _():
        z_wait(5, 2)

    three.compute_all()
    three.open_relayed()
    two.pass_on()
    after.pass_on()

    @pl.when(end)
    def _():
        z_wait(6, 2)

    four.compute_all()
    four.open_relayed()
    for piece in (three, four):
        piece.direct(2)
        piece.direct(1)

    three.pass_on()
    one.close()
    four.pass_on()
    two.close()
    after.close()
    three.close()
    four.close()

    for piece in (one, two, after, three, four):
        piece.finish()
    second.finish()
    p_finish(0)
    p_finish(1)
    a_all(0).wait_send()
    a_all(1).wait_send()
    z_sent(0)

    @pl.when(middle)
    def _():
        for way in range(1, 5):
            z_sent(way)


def layer_call(plan, *arrays):
    rows, features, quarter = plan["rows"], plan["features"], plan["quarter"]
    hidden = plan["hidden"]
    wide = 3 * plan["heads"] * LANES
    length = 8 * rows
    bf16, f32 = jnp.bfloat16, jnp.float32
    dma = pltpu.SemaphoreType.DMA
    return pl.pallas_call(
        functools.partial(layer_kernel, plan),
        out_shape=pltpu.VMEM((rows, features), bf16),
        in_specs=[pl.BlockSpec(memory_space=pl.ANY)] * 13,
        out_specs=pl.BlockSpec(memory_space=pltpu.VMEM),
        scratch_shapes=[
            pltpu.VMEM((rows, features), bf16),
            pltpu.VMEM(arrays[9].shape, bf16),
            *(pltpu.VMEM(arrays[i].shape, bf16) for i in (1, 2, 5, 6, 4, 8, 3, 7)),
            pltpu.VMEM((8, features), f32),
            pltpu.VMEM((length, features), bf16),
            pltpu.VMEM((length, features), bf16),
            pltpu.VMEM((features, plan["whole"]), bf16),
            pltpu.VMEM((4, 32, quarter // 32 * plan["rest"]), bf16),
            pltpu.VMEM((features, wide), bf16),
            pltpu.VMEM((1, wide), f32),
            pltpu.VMEM((length, wide), bf16),
            pltpu.VMEM((rows, features), bf16),
            pltpu.VMEM((4, 2 * rows, LANES), bf16),
            pltpu.VMEM((4, rows, LANES), bf16),
            pltpu.VMEM((8, rows, LANES), bf16),
            pltpu.VMEM((8, rows // 2, LANES), bf16),
            pltpu.VMEM((4, features, quarter), bf16),
            pltpu.VMEM((features, hidden), bf16),
            pltpu.VMEM((features, hidden), bf16),
            pltpu.VMEM((rows, features), f32),
            pltpu.VMEM((4, rows, features), bf16),
            pltpu.VMEM((3, rows, features), bf16),
            pltpu.VMEM((2, rows // 2, features), bf16),
            pltpu.VMEM((2, rows, features), bf16),
            dma((13,)),
            dma((20,)), dma((19,)),
            dma((2,)), dma((2, 7)),
            dma((2,)), dma((2, 5)),
            dma((2,)), dma((2,)),
            dma((5, 2)), dma((5, 7)),
        ],
        compiler_params=pltpu.CompilerParams(
            collective_id=3, has_side_effects=True, vmem_limit_bytes=60 * 1024 * 1024
        ),
        name="layer",
    )(*arrays)


def local(
    tokens_in,
    ln1_gain,
    ln1_bias,
    qkv_weight,
    qkv_bias,
    proj_weight,
    proj_bias,
    ln2_gain,
    ln2_bias,
    fc1_weight,
    fc1_bias,
    fc2_weight,
    fc2_bias,
):
    local_heads = HEADS // lax.axis_size("col")
    own_rows, features = tokens_in.shape
    size = qkv_weight.shape[1] // (3 * local_heads)
    padded = -(-(size + 1) // LANES) * LANES
    plan = fast_plan(
        local_heads, own_rows, features, qkv_weight.shape[1], proj_weight.shape[0],
        fc1_weight.shape[1],
    )
    if plan is not None:
        return layer_call(
            plan, tokens_in, ln1_gain, ln1_bias, qkv_bias, proj_bias, ln2_gain, ln2_bias, fc1_bias,
            fc2_bias, qkv_weight.T, proj_weight, fc1_weight, fc2_weight,
        )
    inputs = tokens_in.astype(jnp.float32)
    qkv_full = gather_row(qkv_weight, 0)
    proj_full = gather_row(proj_weight, 1)
    fc1_full = gather_row(fc1_weight, 0)
    fc2_full = gather_row(fc2_weight, 0)
    fc1_shift = fc1_bias.astype(jnp.float32)

    spare = padded - size
    qkv_wide = jnp.pad(
        qkv_full.reshape(features, local_heads, 3, size), ((0, 0), (0, 0), (0, 0), (0, spare))
    ).reshape(features, local_heads * 3 * padded)
    shift = jnp.pad(
        qkv_bias.astype(jnp.float32).reshape(local_heads, 3, size), ((0, 0), (0, 0), (0, spare))
    )
    shift = shift.at[:, 2, size].set(1.0).reshape(-1)
    scale = jnp.ones((local_heads, 3, padded), jnp.float32)
    scale = scale.at[:, 0].set(1.4426950408889634 / size**0.5).reshape(-1)

    ln1 = norm_local(inputs, ln1_gain, ln1_bias).astype(jnp.bfloat16)
    product = jnp.dot(gather_col(ln1, 0), qkv_wide, preferred_element_type=jnp.float32)
    qkv = ((product + shift) * scale).astype(jnp.bfloat16)
    attn = attend(qkv, local_heads, size, padded)
    proj_whole = cube_gather_col(proj_full)
    own_heads = lax.all_to_all(attn, "col", split_axis=0, concat_axis=1, tiled=True)
    attn_sum = jnp.dot(own_heads, proj_whole, preferred_element_type=jnp.float32)
    resid = inputs + attn_sum + proj_bias.astype(jnp.float32)
    ln2 = norm_local(resid, ln2_gain, ln2_bias).astype(jnp.bfloat16)
    product = jnp.dot(gather_col(ln2, 1), fc1_full, preferred_element_type=jnp.float32) + fc1_shift
    hidden = jax.nn.gelu(product, approximate=False).astype(jnp.bfloat16)
    mlp_sum = scatter_col(project_back(hidden, fc2_full).astype(jnp.bfloat16), 2)
    result = resid + mlp_sum + fc2_bias.astype(jnp.float32)
    return result.astype(jnp.bfloat16)


def solution(mesh):
    in_specs = (
        P(("row", "col"), None),
        P(),
        P(),
        P("row", "col"),
        P("col"),
        P("col", "row"),
        P(),
        P(),
        P(),
        P("row", "col"),
        P("col"),
        P("row", "col"),
        P(),
    )
    out_specs = P(("row", "col"), None)
    return jax.shard_map(local, mesh=mesh, in_specs=in_specs, out_specs=out_specs, check_vma=False)
```
